128 devices in a mesh: gx: 32 (over y, x_hi, z), gy: 4 (over x_lo, core).
Axes of the slice: x: 4 (x_hi: 2, x_lo: 2; x = x_hi * 2 + x_lo), y: 4, z: 4, core: 2. Of those that a mesh axis runs over, the one named last changes fastest.
Arguments:
- electric: float32 [3, 512, 512, 128], P(None, 'gx', 'gy'), may hold values from -6 to 6
- magnetic: float32 [3, 512, 512, 128], P(None, 'gx', 'gy'), may hold values from -6 to 6
- retention: float32 [512, 512, 128], P('gx', 'gy'), may hold values from 0.5 to 1
- coupling: float32 [512, 512, 128], P('gx', 'gy'), may hold values from 0.1 to 0.5
- spectrum_real: float32 [4, 4, 512, 512], P(None, None, 'gx', 'gy'), may hold values from -6 to 6
- spectrum_imag: float32 [4, 4, 512, 512], P(None, None, 'gx', 'gy'), may hold values from -6 to 6
- phases: float32 [4], replicated, may hold values from -3.140625 to 3.140625
Outputs:
- next_electric: float32 [3, 512, 512, 128], P(None, 'gx', 'gy')
- next_magnetic: float32 [3, 512, 512, 128], P(None, 'gx', 'gy')
- next_real: float32 [4, 4, 512, 512], P(None, None, 'gx', 'gy')
- next_imag: float32 [4, 4, 512, 512], P(None, None, 'gx', 'gy')
- far_field: float32 [2, 4, 4, 256, 256], P(None, None, None, 'gx', 'gy')
The draws below stay inside these ranges and needn't reach their ends.
All inputs are finite; a program needn't handle non-finite values.
Results may differ from the reference program's by a relative error of at most 0.000071.
Values sent between devices are 32-bit elements; how exact they have to be, the bound alone decides.
A program may use at most 128 MiB of HBM per device.

```python
import math
import jax
import jax.numpy as jnp
from jax import lax

NZ = 128
FREQS = 4
WAVES = 256
TOP_PLANE = 111
NX = 512
NY = 512


def level_of(key, dims, split, smallest, high):
    loudness = 1.0
    for axis_at, blocks in split:
        draws = jax.random.uniform(jax.random.fold_in(jax.random.fold_in(key, 6), axis_at), (blocks,), jnp.float32, smallest / len(split), high / len(split))
        loudness = loudness * jnp.repeat(jnp.exp(draws), dims[axis_at] // blocks).reshape((-1,) + (1,) * (len(dims) - 1 - axis_at))
    return loudness


def noise(key, shape, width, most, split=(), kind=jnp.bfloat16):
    values = width * jax.random.normal(key, shape, jnp.float32)
    if split:
        values = values * level_of(key, shape, split, -0.22, 0.18)
    return jnp.clip(values, -most, most).astype(kind)


def setup_inputs(seed: int = 0) -> dict:
    key_list = jax.random.split(jax.random.key(seed), 8)
    return {
        "electric": noise(key_list[0], (3, NX, NY, NZ), 1.0, 6.0, ((1, 32), (2, 4)), jnp.float32),
        "magnetic": noise(key_list[1], (3, NX, NY, NZ), 1.0, 6.0, ((1, 32), (2, 4)), jnp.float32),
        "retention": jnp.clip(0.5 + 0.5 * jax.random.uniform(key_list[2], (NX, NY, NZ), jnp.float32) ** level_of(key_list[2], (NX, NY, NZ), ((0, 32), (1, 4)), -0.2, 0.2), 0.5, 1.0),
        "coupling": jnp.clip(jnp.exp(math.log(0.5) - 1.609438 * jax.random.uniform(key_list[3], (NX, NY, NZ), jnp.float32) ** level_of(key_list[3], (NX, NY, NZ), ((0, 32), (1, 4)), -0.2, 0.2)), 0.1, 0.5),
        "spectrum_real": noise(key_list[4], (4, FREQS, NX, NY), 1.0, 6.0, ((2, 32), (3, 4)), jnp.float32),
        "spectrum_imag": noise(key_list[5], (4, FREQS, NX, NY), 1.0, 6.0, ((2, 32), (3, 4)), jnp.float32),
        "phases": jnp.clip(jax.random.uniform(key_list[6], (FREQS,), jnp.float32, -3.140625, 3.140625), -3.140625, 3.140625),
    }


curl_step = 0.5

def forward_diff(values, along):
    padded = jnp.pad(values, [(0, 1) if which == along else (0, 0) for which in range(values.ndim)])
    return lax.slice_in_dim(padded, 1, values.shape[along] + 1, axis=along) - values

def backward_diff(values, along):
    padded = jnp.pad(values, [(1, 0) if which == along else (0, 0) for which in range(values.ndim)])
    return values - lax.slice_in_dim(padded, 0, values.shape[along], axis=along)

def tables(number, extent, offset):
    wave = 2 * jnp.arange(number, dtype=jnp.int32) + 1 - number
    places = offset + jnp.arange(extent, dtype=jnp.int32)
    folded = wave[:, None] * places[None, :] % (4 * number)
    angles = folded.astype(jnp.float32) * (math.pi / (2 * number))
    return (jnp.cos(angles), jnp.sin(angles))

def reference(electric, magnetic, retention, coupling, spectrum_real, spectrum_imag, phases):
    highest = lax.Precision.HIGHEST
    elec_x, elec_y, elec_z = (electric[0], electric[1], electric[2])
    mag_x = magnetic[0] - curl_step * (forward_diff(elec_z, 1) - forward_diff(elec_y, 2))
    mag_y = magnetic[1] - curl_step * (forward_diff(elec_x, 2) - forward_diff(elec_z, 0))
    mag_z = magnetic[2] - curl_step * (forward_diff(elec_y, 0) - forward_diff(elec_x, 1))
    new_x = retention * elec_x + coupling * (backward_diff(mag_z, 1) - backward_diff(mag_y, 2))
    new_y = retention * elec_y + coupling * (backward_diff(mag_x, 2) - backward_diff(mag_z, 0))
    new_z = retention * elec_z + coupling * (backward_diff(mag_y, 0) - backward_diff(mag_x, 1))
    tangent = jnp.stack([new_x[:, :, TOP_PLANE], new_y[:, :, TOP_PLANE], mag_x[:, :, TOP_PLANE], mag_y[:, :, TOP_PLANE]])
    next_real = spectrum_real + tangent[:, None] * jnp.cos(phases)[None, :, None, None]
    next_imag = spectrum_imag - tangent[:, None] * jnp.sin(phases)[None, :, None, None]
    cos_x, sin_x = tables(WAVES, NX, 0)
    cos_y, sin_y = tables(WAVES, NY, 0)
    part_real = jnp.einsum('cfxy,ky->cfxk', next_real, cos_y, precision=highest) + jnp.einsum('cfxy,ky->cfxk', next_imag, sin_y, precision=highest)
    part_imag = jnp.einsum('cfxy,ky->cfxk', next_imag, cos_y, precision=highest) - jnp.einsum('cfxy,ky->cfxk', next_real, sin_y, precision=highest)
    far_real = jnp.einsum('jx,cfxk->cfjk', cos_x, part_real, precision=highest) + jnp.einsum('jx,cfxk->cfjk', sin_x, part_imag, precision=highest)
    far_imag = jnp.einsum('jx,cfxk->cfjk', cos_x, part_imag, precision=highest) - jnp.einsum('jx,cfxk->cfjk', sin_x, part_real, precision=highest)
    scale = 1.0 / math.sqrt(NX * NY)
    far_field = jnp.stack([far_real, far_imag]) * scale
    next_electric = jnp.stack([new_x, new_y, new_z])
    next_magnetic = jnp.stack([mag_x, mag_y, mag_z])
    return (next_electric, next_magnetic, next_real, next_imag, far_field)
```

```python
import functools
import math

import jax
import jax.numpy as jnp
import numpy as np
from jax import lax
from jax.experimental import pallas as pl
from jax.experimental.pallas import tpu as pltpu
from jax.sharding import PartitionSpec as P

MESH = pl.DeviceIdType.MESH
WAVES = 256
PLANE = 111
GX, GY = 32, 4
F32, BF16 = jnp.float32, jnp.bfloat16


def split_np(table):
    high = table.astype(np.float32).astype(jnp.bfloat16)
    low = (table - high.astype(np.float64)).astype(np.float32).astype(jnp.bfloat16)
    return np.stack([high, low])


def angle_np(wave, place):
    return (np.multiply.outer(wave, place) % 1024) * (math.pi / 512)


@functools.cache
def tables():
    wave = 2 * np.arange(WAVES) - 255
    ang = angle_np(wave, np.arange(512)).reshape(256, 4, 128).transpose(1, 0, 2)
    tab_y = split_np(np.concatenate([np.cos(ang), np.sin(ang)], axis=2))
    ang = angle_np(2 * np.arange(32) - 255, 16 * np.arange(32))
    eye = np.eye(8)
    tab_w = split_np(np.concatenate([np.kron(np.cos(ang), eye), np.kron(np.sin(ang), eye)], axis=1))
    ang = np.repeat(angle_np(2 * np.arange(32) - 255, np.arange(16)), 8, axis=0)
    cos, sin = np.tile(np.cos(ang), (1, 8)), np.tile(np.sin(ang), (1, 8))
    sin[:, 64:] *= -1
    tab_t = np.stack([cos, sin]).astype(np.float32)
    ang = 2 * math.pi * (np.multiply.outer(np.arange(8), np.arange(16)) % 16) / 16
    eye = np.eye(4)
    blocks = [np.einsum("ai,fg->afgi", t, eye).reshape(32, 64) for t in (np.cos(ang), np.sin(ang))]
    tab_g = split_np(np.concatenate(blocks, axis=1) / 512.0)
    return tab_y, tab_w, tab_t, tab_g


def split(value):
    high = value.astype(BF16)
    return high, (value - high.astype(F32)).astype(BF16)


def dot_nt(a, b):
    return lax.dot_general(a, b, (((1,), (1,)), ((), ())), preferred_element_type=F32)


def dot_nn(a, b):
    return lax.dot_general(a, b, (((1,), (0,)), ((), ())), preferred_element_type=F32)


def plane_of(value, at):
    wide = jnp.broadcast_to(value[:, at : at + 1], (128, 128))
    rows = lax.broadcasted_iota(jnp.int32, (128, 128), 0)
    lanes = lax.broadcasted_iota(jnp.int32, (128, 128), 1)
    return jnp.sum(jnp.where(rows == lanes, wide, 0.0), axis=0, keepdims=True)


def step_kernel(
    e_hbm, h_hbm, r_hbm, c_hbm, sr_hbm, si_hbm, ph_ref, ty_hbm, tw_hbm, tt_hbm, tg_hbm,
    eo, ho, nr, ni, far,
    eb, hb, rb, cb, srv, siv, ty, tw, tt, tg,
    ye_s, yh_s, ye_l, yh_l, xe_l, xh_l, ce_l, pk_s, pk_l, t_s, t_l, al,
    bs, bl, cs, cl, rel, zz,
    ld_sem, yh_sem, pk_ss, pk_rs, a_ss, a_rs, t_ss, t_rs, x_sem, b_ss, b_rs, c_ss, c_rs,
):
    X = lax.axis_index("gx")
    Y = lax.axis_index("gy")
    xn, xp = lax.rem(X + 1, GX), lax.rem(X + GX - 1, GX)
    yn, yp = lax.rem(Y + 1, GY), lax.rem(Y + GY - 1, GY)
    has_xn, has_xp, has_yn, has_yp = X < GX - 1, X > 0, Y < GY - 1, Y > 0

    barrier = pltpu.get_barrier_semaphore()
    me = X * GY + Y

    def greet(d, carry):
        other = lax.rem(me + d, GX * GY)
        pl.semaphore_signal(barrier, inc=1, device_id=(other // GY, lax.rem(other, GY)), device_id_type=MESH)
        return carry

    lax.fori_loop(1, GX * GY, greet, 0)

    loads = []

    def load(src, dst):
        copy = pltpu.make_async_copy(src, dst, ld_sem.at[len(loads)])
        copy.start()
        loads.append(copy)
        return copy

    first = [load(e_hbm.at[i], eb.at[i]) for i in range(3)] + [load(h_hbm.at[i], hb.at[i]) for i in range(3)]
    first += [load(c_hbm, cb)]
    ret = load(r_hbm, rb)
    spec = [load(sr_hbm, srv), load(si_hbm, siv)]
    tabs = [load(ty_hbm, ty), load(tw_hbm, tw), load(tt_hbm, tt), load(tg_hbm, tg)]

    rows = lax.broadcasted_iota(jnp.int32, (128, 128), 0)
    lanes = lax.broadcasted_iota(jnp.int32, (128, 128), 1)
    row16 = lax.broadcasted_iota(jnp.int32, (16, 128), 0)
    lane16 = lax.broadcasted_iota(jnp.int32, (16, 128), 1)
    lane1 = lax.broadcasted_iota(jnp.int32, (1, 128), 1)

    def next_z(v, lane):
        return jnp.where(lane == 127, 0.0, pltpu.roll(v, 127, 1))

    def prev_z(v, lane):
        return jnp.where(lane == 0, 0.0, pltpu.roll(v, 1, 1))

    @pl.when(jnp.logical_not(has_xn))
    def _():
        xe_l[...] = jnp.zeros_like(xe_l)
        pk_l[2] = jnp.zeros_like(pk_l[2])

    @pl.when(jnp.logical_not(has_xp))
    def _():
        xh_l[...] = jnp.zeros_like(xh_l)
        pk_l[0] = jnp.zeros_like(pk_l[0])

    @pl.when(jnp.logical_not(has_yn))
    def _():
        ye_l[...] = jnp.zeros_like(ye_l)

    @pl.when(jnp.logical_not(has_yp))
    def _():
        yh_l[...] = jnp.zeros_like(yh_l)

    @pl.when(jnp.logical_not(jnp.logical_and(has_xn, has_yp)))
    def _():
        ce_l[...] = jnp.zeros_like(ce_l)

    for copy in first:
        copy.wait()
    ye_s[0] = eb[0, :, 0, :]
    ye_s[1] = eb[2, :, 0, :]
    ex, ey, ez = eb[0, :, 127, :], eb[1, :, 127, :], eb[2, :, 127, :]
    yh_s[0] = hb[0, :, 127, :] - 0.5 * (-ez - (next_z(ey, lane16) - ey))
    ey_up = jnp.where(row16 == 15, 0.0, pltpu.roll(ey, 15, 0))
    yh_s[1] = hb[2, :, 127, :] - 0.5 * (ey_up - ey + ex)

    ex15 = eb[0, 15]
    ex_up = jnp.where(rows == 127, 0.0, pltpu.roll(ex15, 127, 0))
    phz = hb[2, 15] - 0.5 * (-eb[1, 15] - (ex_up - ex15))
    pk_s[0:1] = plane_of(eb[1, 0], PLANE)
    pk_s[1:2] = plane_of(eb[2, 0], PLANE)
    pk_s[2:3] = plane_of(eb[2, 0], PLANE - 1)
    pk_s[3:4] = plane_of(phz, PLANE)
    pk_s[4:5] = plane_of(cb[0], PLANE)
    pk_s[5:6] = plane_of(cb[15], PLANE)
    pk_s[6:7] = plane_of(ex15, PLANE)
    pk_s[7:8] = jnp.zeros((1, 128), F32)
    pk_l[1, Y] = pk_s[...]
    for copy in spec:
        copy.wait()
    al[0, Y] = srv[Y]
    al[1, Y] = siv[Y]
    ret.wait()

    pl.semaphore_wait(barrier, GX * GY - 1)

    def remote(src, dst, ss, rs, x, y):
        return pltpu.make_async_remote_copy(
            src_ref=src, dst_ref=dst, send_sem=ss, recv_sem=rs, device_id=(x, y), device_id_type=MESH
        )

    ye = remote(ye_s, ye_l, yh_sem.at[0], yh_sem.at[1], X, yp)
    yh = remote(yh_s, yh_l, yh_sem.at[2], yh_sem.at[3], X, yn)
    pl.when(has_yp)(ye.start)
    pl.when(has_yn)(yh.start)

    def pack(dx, d):
        return remote(
            pk_s, pk_l.at[2 - dx, Y], pk_ss.at[dx, d], pk_rs.at[2 - dx, Y], (xp, X, xn)[dx], lax.rem(Y + d, GY)
        )

    for dx, ok in ((0, has_xp), (2, has_xn)):
        for d in range(GY):
            pl.when(ok)(pack(dx, d).start)
    for d in range(1, GY):
        pack(1, d).start()

    def spectrum(part, d):
        g = lax.rem(Y + d, GY)
        return remote((srv, siv)[part].at[g], al.at[part, Y], a_ss.at[part, d], a_rs.at[part, Y], X, g)

    for d in range(1, GY):
        for part in range(2):
            spectrum(part, d).start()

    corner = remote(eb.at[1, 0, pl.ds(120, 8)], ce_l, x_sem.at[0], x_sem.at[1], xp, yn)
    pl.when(jnp.logical_and(has_xp, has_yn))(corner.start)
    xe = remote(eb.at[pl.ds(1, 2), 0], xe_l, x_sem.at[2], x_sem.at[3], xp, Y)
    pl.when(has_xp)(xe.start)

    pl.when(has_yn)(ye.wait_recv)
    pl.when(has_yp)(yh.wait_recv)
    yh_l[0] = jnp.where(has_yp, yh_l[0] - 0.5 * ye_s[1], 0.0)
    yh_l[1] = jnp.where(has_yp, yh_l[1] + 0.5 * ye_s[0], 0.0)

    def row(x, edge_first, edge_last):
        ex, ey, ez = eb[0, x], eb[1, x], eb[2, x]
        exn = jnp.where(rows == 127, ye_l[0, pl.ds(x, 1), :], pltpu.roll(ex, 127, 0))
        ezn = jnp.where(rows == 127, ye_l[1, pl.ds(x, 1), :], pltpu.roll(ez, 127, 0))
        if edge_last:
            ey_x, ez_x = -ey, -ez
        else:
            ey_x, ez_x = eb[1, x + 1] - ey, eb[2, x + 1] - ez
        hx = hb[0, x] - 0.5 * ((ezn - ez) - (next_z(ey, lanes) - ey))
        hy = hb[1, x] - 0.5 * ((next_z(ex, lanes) - ex) - ez_x)
        hz = hb[2, x] - 0.5 * (ey_x - (exn - ex))
        ho[0, x] = hx
        ho[1, x] = hy
        ho[2, x] = hz
        hxp = jnp.where(rows == 0, yh_l[0, pl.ds(x, 1), :], pltpu.roll(hx, 1, 0))
        hzp = jnp.where(rows == 0, yh_l[1, pl.ds(x, 1), :], pltpu.roll(hz, 1, 0))
        if edge_first:
            hy_x, hz_x = hy, hz
        else:
            hy_x, hz_x = hy - ho[1, x - 1], hz - ho[2, x - 1]
        r, c = rb[x], cb[x]
        nx = r * ex + c * ((hz - hzp) - (hy - prev_z(hy, lanes)))
        ny = r * ey + c * ((hx - prev_z(hx, lanes)) - hz_x)
        nz = r * ez + c * (hy_x - (hx - hxp))
        eo[0, x] = nx
        eo[1, x] = ny
        eo[2, x] = nz
        for at, v in enumerate((nx, ny, hx, hy)):
            t_s[at, pl.ds(x, 1), :] = plane_of(v, PLANE)

    row(0, True, False)

    def inner(x, carry):
        row(x, False, False)
        return carry

    lax.fori_loop(1, 15, inner, 0)
    row(15, False, True)

    def tangent(d):
        g = lax.rem(Y + d, GY)
        return remote(t_s.at[g], t_l.at[Y], t_ss.at[d], t_rs.at[Y], X, g)

    for d in range(1, GY):
        tangent(d).start()
    t_l[Y] = t_s[Y]
    xh = remote(ho.at[pl.ds(1, 2), 15], xh_l, x_sem.at[4], x_sem.at[5], xn, Y)
    pl.when(has_xn)(xh.start)

    def from_gy(make, d):
        make(d).wait_recv()

    for d in range(1, GY):
        s = lax.rem(Y + d, GY)
        for part in range(2):
            remote(srv.at[0], al.at[part, s], a_ss.at[part, d], a_rs.at[part, s], X, s).wait_recv()
        remote(pk_s, pk_l.at[1, s], pk_ss.at[1, d], pk_rs.at[1, s], X, s).wait_recv()
        remote(t_s.at[0], t_l.at[s], t_ss.at[d], t_rs.at[s], X, s).wait_recv()
    for s in range(GY):
        pl.when(has_xn)(remote(pk_s, pk_l.at[2, s], pk_ss.at[2, s], pk_rs.at[2, s], xn, Y).wait_recv)
        pl.when(has_xp)(remote(pk_s, pk_l.at[0, s], pk_ss.at[0, s], pk_rs.at[0, s], xp, Y).wait_recv)
    for copy in tabs:
        copy.wait()

    wave_cos = [jnp.cos(jnp.full((8, 128), ph_ref[f], F32))[0:1] for f in range(4)]
    wave_sin = [jnp.sin(jnp.full((8, 128), ph_ref[f], F32))[0:1] for f in range(4)]
    total = None
    for s in range(GY):
        nxt, own, prv = pk_l[2, s], pk_l[1, s], pk_l[0, s]
        dhz = -0.5 * nxt[0:1]
        before = -0.5 * pk_l[2, s - 1][0:1, 127:128] if s else jnp.zeros((1, 1), F32)
        dhz_p = jnp.where(lane1 == 0, before, pltpu.roll(dhz, 1, 1))
        dhy = 0.5 * nxt[1:2]
        dhyd = dhy - 0.5 * nxt[2:3]
        after = 0.5 * pk_l[0, s + 1][6:7, 0:1] if s < GY - 1 else jnp.zeros((1, 1), F32)
        hzp = prv[3:4] - 0.5 * own[0:1] + jnp.where(lane1 == 127, after, 0.0)
        last = jnp.where(
            Y == 0, own[5:6] * (dhz - dhz_p - dhyd), jnp.where(Y == 1, -own[5:6] * dhz, jnp.where(Y == 3, dhy, 0.0))
        )
        head = jnp.where(jnp.logical_and(Y == 1, has_xp), own[4:5] * hzp, 0.0)
        t = t_l[s] + jnp.where(row16 == 15, last, 0.0) + jnp.where(row16 == 0, head, 0.0)
        re = jnp.concatenate([al[0, s, f] + t * wave_cos[f] for f in range(4)], axis=0)
        im = jnp.concatenate([al[1, s, f] - t * wave_sin[f] for f in range(4)], axis=0)
        data = jnp.concatenate(
            [jnp.concatenate([re, im], axis=0), jnp.concatenate([im, -re], axis=0)], axis=1
        )
        high, low = split(data)
        part = dot_nt(ty[0, s], high) + dot_nt(ty[0, s], low) + dot_nt(ty[1, s], high)
        total = part if total is None else total + part
    bs[...] = total.reshape(GX, 8, 128)

    def column(d):
        to = lax.rem(X + d, GX)
        return remote(bs.at[to], bl.at[X], b_ss.at[d], b_rs.at[X], to, Y)

    def b_start(d, carry):
        column(d).start()
        return carry

    lax.fori_loop(1, GX, b_start, 0)
    bl[X] = bs[X]

    pl.when(has_xn)(xe.wait_recv)
    pl.when(has_xp)(xh.wait_recv)
    pl.when(jnp.logical_and(has_xn, has_yp))(corner.wait_recv)
    pl.when(has_xn)(xh.wait_send)
    dhy, dhz = 0.5 * xe_l[1], -0.5 * xe_l[0]
    ho[1, 15] = ho[1, 15] + dhy
    ho[2, 15] = ho[2, 15] + dhz
    dhz_p = jnp.where(rows == 0, -0.5 * ce_l[7:8], pltpu.roll(dhz, 1, 0))
    c = cb[15]
    eo[0, 15] = eo[0, 15] + c * ((dhz - dhz_p) - (dhy - prev_z(dhy, lanes)))
    eo[1, 15] = eo[1, 15] - c * dhz
    eo[2, 15] = eo[2, 15] + c * dhy
    hyp = jnp.where(has_xp, xh_l[0] + 0.5 * eb[2, 0], 0.0)
    hzp = jnp.where(has_xp, xh_l[1] - 0.5 * eb[1, 0], 0.0)
    c = cb[0]
    eo[1, 0] = eo[1, 0] + c * hzp
    eo[2, 0] = eo[2, 0] - c * hyp
    for d in range(1, GY):
        tangent(d).wait_send()
    t_s[0, 15:16] = plane_of(eo[0, 15], PLANE)
    t_s[1, 15:16] = plane_of(eo[1, 15], PLANE)
    t_s[1, 0:1] = plane_of(eo[1, 0], PLANE)
    t_s[3, 15:16] = plane_of(ho[1, 15], PLANE)
    for at in range(4):
        t = t_s[at]
        for f in range(4):
            nr[at, f] = srv[at, f] + t * wave_cos[f]
            ni[at, f] = siv[at, f] - t * wave_sin[f]

    def b_wait(d, carry):
        src = lax.rem(X + d, GX)
        remote(bs.at[src], bl.at[src], b_ss.at[d], b_rs.at[src], src, Y).wait_recv()
        return carry

    lax.fori_loop(1, GX, b_wait, 0)

    block = bl[...].reshape(256, 128)
    sign = jnp.where(lax.broadcasted_iota(jnp.int32, (256, 128), 1) < 64, 1.0, -1.0)
    both = jnp.concatenate([block, pltpu.roll(block, 64, 1) * sign], axis=0)
    high, low = split(both)
    y = dot_nn(tw[0], high) + dot_nn(tw[0], low) + dot_nn(tw[1], high)
    y = y * tt[0] + pltpu.roll(y, 64, 1) * tt[1]
    y_sw = pltpu.roll(y, 64, 1) * sign
    pieces = []
    for b in range(4):
        pieces += [y[64 * b : 64 * b + 64], y_sw[64 * b : 64 * b + 64]]
    high, low = split(jnp.concatenate(pieces, axis=0))
    out = dot_nt(tg[0], high) + dot_nt(tg[0], low) + dot_nt(tg[1], high)
    for a in range(8):
        for b in range(4):
            cs[4 * a + b] = out[4 * a : 4 * a + 4, 128 * b : 128 * b + 128]

    home, slot = X // 8, lax.rem(X, 8)

    def finished(d):
        to = lax.rem(X + d, GX)
        return remote(cs.at[to], cl.at[Y, slot], c_ss.at[d], c_rs.at[Y, slot], to, home)

    def c_start(d, carry):
        pl.when(jnp.logical_or(d > 0, home != Y))(finished(d).start)
        return carry

    lax.fori_loop(0, GX, c_start, 0)

    @pl.when(home == Y)
    def _():
        cl[Y, slot] = cs[X]

    def c_wait(i, carry):
        g, q = i // 8, lax.rem(i, 8)
        src = 8 * Y + q

        @pl.when(jnp.logical_or(g != Y, src != X))
        def _():
            remote(cs.at[0], cl.at[g, q], c_ss.at[0], c_rs.at[g, q], src, g).wait_recv()

        return carry

    lax.fori_loop(0, 32, c_wait, 0)

    for q in range(8):
        for g in range(4):
            rel[q, 4 * g : 4 * g + 4, :] = cl[g, q]
    turned = [pltpu.roll(rel[q], 8 * q, 1) if q else rel[q] for q in range(8)]
    group = lane16 // 8
    for s in range(16):
        acc = turned[0]
        for q in range(1, 8):
            acc = jnp.where(group == (q + s) % 16, turned[q], acc)
        if s:
            acc = pltpu.roll(acc, 128 - 8 * s, 1)
        zz[:, s, :] = acc
    for g in range(4):
        for f in range(4):
            far[0, g, f] = zz[4 * g + f, 0:8, 0:64]
            far[1, g, f] = zz[4 * g + f, 8:16, 0:64]

    pl.when(has_yp)(ye.wait_send)
    pl.when(has_yn)(yh.wait_send)
    for dx, ok in ((0, has_xp), (2, has_xn)):
        for d in range(GY):
            pl.when(ok)(pack(dx, d).wait_send)
    for d in range(1, GY):
        pack(1, d).wait_send()
        for part in range(2):
            spectrum(part, d).wait_send()
    pl.when(jnp.logical_and(has_xp, has_yn))(corner.wait_send)
    pl.when(has_xp)(xe.wait_send)

    def b_sent(d, carry):
        column(d).wait_send()
        return carry

    lax.fori_loop(1, GX, b_sent, 0)

    def c_sent(d, carry):
        pl.when(jnp.logical_or(d > 0, home != Y))(finished(d).wait_send)
        return carry

    lax.fori_loop(0, GX, c_sent, 0)


def flush_kernel(*refs):
    ins, outs, sem = refs[:5], refs[5:10], refs[10]
    copies = []
    for at, (src, dst) in enumerate(zip(ins, outs)):
        if at < 2:
            copies += [(src.at[i], dst.at[i]) for i in range(3)]
        else:
            copies.append((src, dst))
    copies = [pltpu.make_async_copy(src, dst, sem.at[at]) for at, (src, dst) in enumerate(copies)]
    for copy in copies:
        copy.start()
    for copy in copies:
        copy.wait()


def per_device(electric, magnetic, retention, coupling, spectrum_real, spectrum_imag, phases):
    tab_y, tab_w, tab_t, tab_g = (jnp.asarray(t) for t in tables())
    vmem, dma = pltpu.VMEM, pltpu.SemaphoreType.DMA
    hbm = pl.BlockSpec(memory_space=pltpu.HBM)
    in_vmem = pl.BlockSpec(memory_space=pltpu.VMEM)
    shapes = [
        jax.ShapeDtypeStruct(electric.shape, F32),
        jax.ShapeDtypeStruct(magnetic.shape, F32),
        jax.ShapeDtypeStruct(spectrum_real.shape, F32),
        jax.ShapeDtypeStruct(spectrum_imag.shape, F32),
        jax.ShapeDtypeStruct((2, 4, 4, 8, 64), F32),
    ]
    held = pl.pallas_call(
        step_kernel,
        out_shape=shapes,
        in_specs=[hbm] * 6 + [pl.BlockSpec(memory_space=pltpu.SMEM)] + [hbm] * 4,
        out_specs=[in_vmem] * 5,
        scratch_shapes=[
            vmem(electric.shape, F32), vmem(magnetic.shape, F32), vmem(retention.shape, F32), vmem(coupling.shape, F32),
            vmem(spectrum_real.shape, F32), vmem(spectrum_imag.shape, F32),
            vmem(tab_y.shape, BF16), vmem(tab_w.shape, BF16), vmem(tab_t.shape, F32), vmem(tab_g.shape, BF16),
            vmem((2, 16, 128), F32), vmem((2, 16, 128), F32), vmem((2, 16, 128), F32), vmem((2, 16, 128), F32),
            vmem((2, 128, 128), F32), vmem((2, 128, 128), F32), vmem((8, 128), F32),
            vmem((8, 128), F32), vmem((3, 4, 8, 128), F32),
            vmem((4, 16, 128), F32), vmem((4, 16, 128), F32), vmem((2, 4, 4, 16, 128), F32),
            vmem((32, 8, 128), F32), vmem((32, 8, 128), F32), vmem((32, 4, 128), F32), vmem((4, 8, 4, 128), F32),
            vmem((8, 16, 128), F32), vmem((16, 16, 128), F32),
            dma((14,)), dma((4,)), dma((3, 4)), dma((3, 4)), dma((2, 4)), dma((2, 4)), dma((4,)), dma((4,)), dma((6,)),
            dma((32,)), dma((32,)), dma((32,)), dma((4, 8)),
        ],
        compiler_params=pltpu.CompilerParams(collective_id=0, has_side_effects=True, vmem_limit_bytes=40 * 2**20),
    )(electric, magnetic, retention, coupling, spectrum_real, spectrum_imag, phases, tab_y, tab_w, tab_t, tab_g)
    return pl.pallas_call(
        flush_kernel,
        out_shape=shapes,
        in_specs=[in_vmem] * 5,
        out_specs=[hbm] * 5,
        scratch_shapes=[dma((9,))],
        compiler_params=pltpu.CompilerParams(vmem_limit_bytes=16 * 2**20),
    )(*held)


def solution(mesh):
    placed = (
        P(None, "gx", "gy", None),
        P(None, "gx", "gy", None),
        P("gx", "gy", None),
        P("gx", "gy", None),
        P(None, None, "gx", "gy"),
        P(None, None, "gx", "gy"),
        P(),
    )
    return jax.shard_map(
        per_device,
        mesh=mesh,
        in_specs=placed,
        out_specs=(
            P(None, "gx", "gy", None),
            P(None, "gx", "gy", None),
            P(None, None, "gx", "gy"),
            P(None, None, "gx", "gy"),
            P(None, None, None, "gx", "gy"),
        ),
        check_vma=False,
    )
```

```python
import functools
import math

import jax
import jax.numpy as jnp
import numpy as np
from jax import lax
from jax.experimental import pallas as pl
from jax.experimental.pallas import tpu as pltpu
from jax.sharding import PartitionSpec as P

MESH = pl.DeviceIdType.MESH
WAVES = 256
PLANE = 111
GX, GY = 32, 4
F32, BF16 = jnp.float32, jnp.bfloat16


def split_np(table):
    high = table.astype(np.float32).astype(jnp.bfloat16)
    low = (table - high.astype(np.float64)).astype(np.float32).astype(jnp.bfloat16)
    return np.stack([high, low])


def angle_np(wave, place):
    return (np.multiply.outer(wave, place) % 1024) * (math.pi / 512)


@functools.cache
def tables():
    wave = 2 * np.arange(WAVES) - 255
    ang = angle_np(wave, np.arange(512)).reshape(256, 4, 128).transpose(1, 0, 2)
    tab_y = split_np(np.concatenate([np.cos(ang), np.sin(ang)], axis=2))
    ang = angle_np(2 * np.arange(32) - 255, 16 * np.arange(32))
    eye = np.eye(8)
    tab_w = split_np(np.concatenate([np.kron(np.cos(ang), eye), np.kron(np.sin(ang), eye)], axis=1))
    ang = np.repeat(angle_np(2 * np.arange(32) - 255, np.arange(16)), 8, axis=0)
    cos, sin = np.tile(np.cos(ang), (1, 8)), np.tile(np.sin(ang), (1, 8))
    sin[:, 64:] *= -1
    tab_t = np.stack([cos, sin]).astype(np.float32)
    ang = 2 * math.pi * (np.multiply.outer(np.arange(8), np.arange(16)) % 16) / 16
    eye = np.eye(4)
    blocks = [np.einsum("ai,fg->afgi", t, eye).reshape(32, 64) for t in (np.cos(ang), np.sin(ang))]
    tab_g = split_np(np.concatenate(blocks, axis=1) / 512.0)
    return tab_y, tab_w, tab_t, tab_g


def split(value):
    high = value.astype(BF16)
    return high, (value - high.astype(F32)).astype(BF16)


def dot_nt(a, b):
    return lax.dot_general(a, b, (((1,), (1,)), ((), ())), preferred_element_type=F32)


def dot_nn(a, b):
    return lax.dot_general(a, b, (((1,), (0,)), ((), ())), preferred_element_type=F32)


def plane_of(value, at):
    wide = jnp.broadcast_to(value[:, at : at + 1], (128, 128))
    rows = lax.broadcasted_iota(jnp.int32, (128, 128), 0)
    lanes = lax.broadcasted_iota(jnp.int32, (128, 128), 1)
    return jnp.sum(jnp.where(rows == lanes, wide, 0.0), axis=0, keepdims=True)


def step_kernel(
    e_hbm, h_hbm, r_hbm, c_hbm, sr_hbm, si_hbm, ph_ref, ty_hbm, tw_hbm, tt_hbm, tg_hbm,
    eo, ho, nr, ni, far,
    eb, hb, rb, cb, srv, siv, ty, tw, tt, tg,
    ye_s, yh_s, ye_l, yh_l, xe_l, xh_l, ce_l, pk_s, pk_l, t_s, t_l, al,
    bs, bl, cs, cl, rel, zz,
    ld_sem, yh_sem, pk_ss, pk_rs, a_ss, a_rs, t_ss, t_rs, x_sem, b_ss, b_rs, c_ss, c_rs,
):
    X = lax.axis_index("gx")
    Y = lax.axis_index("gy")
    xn, xp = lax.rem(X + 1, GX), lax.rem(X + GX - 1, GX)
    yn, yp = lax.rem(Y + 1, GY), lax.rem(Y + GY - 1, GY)
    has_xn, has_xp, has_yn, has_yp = X < GX - 1, X > 0, Y < GY - 1, Y > 0

    barrier = pltpu.get_barrier_semaphore()
    me = X * GY + Y

    def greet(d, carry):
        other = lax.rem(me + d, GX * GY)
        pl.semaphore_signal(barrier, inc=1, device_id=(other // GY, lax.rem(other, GY)), device_id_type=MESH)
        return carry

    lax.fori_loop(1, GX * GY, greet, 0)

    loads = []

    def load(src, dst):
        copy = pltpu.make_async_copy(src, dst, ld_sem.at[len(loads)])
        copy.start()
        loads.append(copy)
        return copy

    first = [load(e_hbm.at[i], eb.at[i]) for i in range(3)] + [load(h_hbm.at[i], hb.at[i]) for i in range(3)]
    first += [load(c_hbm, cb)]
    ret = load(r_hbm, rb)
    spec = [load(sr_hbm, srv), load(si_hbm, siv)]
    tabs = [load(ty_hbm, ty), load(tw_hbm, tw), load(tt_hbm, tt), load(tg_hbm, tg)]

    rows = lax.broadcasted_iota(jnp.int32, (128, 128), 0)
    lanes = lax.broadcasted_iota(jnp.int32, (128, 128), 1)
    row16 = lax.broadcasted_iota(jnp.int32, (16, 128), 0)
    lane16 = lax.broadcasted_iota(jnp.int32, (16, 128), 1)
    lane1 = lax.broadcasted_iota(jnp.int32, (1, 128), 1)

    def next_z(v, lane):
        return jnp.where(lane == 127, 0.0, pltpu.roll(v, 127, 1))

    def prev_z(v, lane):
        return jnp.where(lane == 0, 0.0, pltpu.roll(v, 1, 1))

    @pl.when(jnp.logical_not(has_xn))
    def _():
        xe_l[...] = jnp.zeros_like(xe_l)
        pk_l[2] = jnp.zeros_like(pk_l[2])

    @pl.when(jnp.logical_not(has_xp))
    def _():
        xh_l[...] = jnp.zeros_like(xh_l)
        pk_l[0] = jnp.zeros_like(pk_l[0])

    @pl.when(jnp.logical_not(has_yn))
    def _():
        ye_l[...] = jnp.zeros_like(ye_l)

    @pl.when(jnp.logical_not(has_yp))
    def _():
        yh_l[...] = jnp.zeros_like(yh_l)

    @pl.when(jnp.logical_not(jnp.logical_and(has_xn, has_yp)))
    def _():
        ce_l[...] = jnp.zeros_like(ce_l)

    for copy in first:
        copy.wait()
    ye_s[0] = eb[0, :, 0, :]
    ye_s[1] = eb[2, :, 0, :]
    ex, ey, ez = eb[0, :, 127, :], eb[1, :, 127, :], eb[2, :, 127, :]
    yh_s[0] = hb[0, :, 127, :] - 0.5 * (-ez - (next_z(ey, lane16) - ey))
    ey_up = jnp.where(row16 == 15, 0.0, pltpu.roll(ey, 15, 0))
    yh_s[1] = hb[2, :, 127, :] - 0.5 * (ey_up - ey + ex)

    ex15 = eb[0, 15]
    ex_up = jnp.where(rows == 127, 0.0, pltpu.roll(ex15, 127, 0))
    phz = hb[2, 15] - 0.5 * (-eb[1, 15] - (ex_up - ex15))
    pk_s[0:1] = plane_of(eb[1, 0], PLANE)
    pk_s[1:2] = plane_of(eb[2, 0], PLANE)
    pk_s[2:3] = plane_of(eb[2, 0], PLANE - 1)
    pk_s[3:4] = plane_of(phz, PLANE)
    pk_s[4:5] = plane_of(cb[0], PLANE)
    pk_s[5:6] = plane_of(cb[15], PLANE)
    pk_s[6:7] = plane_of(ex15, PLANE)
    pk_s[7:8] = jnp.zeros((1, 128), F32)
    pk_l[1, Y] = pk_s[...]
    for copy in spec:
        copy.wait()
    al[0, Y] = srv[Y]
    al[1, Y] = siv[Y]
    ret.wait()

    pl.semaphore_wait(barrier, GX * GY - 1)

    def remote(src, dst, ss, rs, x, y):
        return pltpu.make_async_remote_copy(
            src_ref=src, dst_ref=dst, send_sem=ss, recv_sem=rs, device_id=(x, y), device_id_type=MESH
        )

    ye = remote(ye_s, ye_l, yh_sem.at[0], yh_sem.at[1], X, yp)
    yh = remote(yh_s, yh_l, yh_sem.at[2], yh_sem.at[3], X, yn)
    pl.when(has_yp)(ye.start)
    pl.when(has_yn)(yh.start)

    def pack(dx, d):
        return remote(
            pk_s, pk_l.at[2 - dx, Y], pk_ss.at[dx, d], pk_rs.at[2 - dx, Y], (xp, X, xn)[dx], lax.rem(Y + d, GY)
        )

    for dx, ok in ((0, has_xp), (2, has_xn)):
        for d in range(GY):
            pl.when(ok)(pack(dx, d).start)
    for d in range(1, GY):
        pack(1, d).start()

    def spectrum(part, d):
        g = lax.rem(Y + d, GY)
        return remote((srv, siv)[part].at[g], al.at[part, Y], a_ss.at[part, d], a_rs.at[part, Y], X, g)

    for d in range(1, GY):
        for part in range(2):
            spectrum(part, d).start()

    corner = remote(eb.at[1, 0, pl.ds(120, 8)], ce_l, x_sem.at[0], x_sem.at[1], xp, yn)
    pl.when(jnp.logical_and(has_xp, has_yn))(corner.start)
    xe = remote(eb.at[pl.ds(1, 2), 0], xe_l, x_sem.at[2], x_sem.at[3], xp, Y)
    pl.when(has_xp)(xe.start)

    pl.when(has_yn)(ye.wait_recv)
    pl.when(has_yp)(yh.wait_recv)
    yh_l[0] = jnp.where(has_yp, yh_l[0] - 0.5 * ye_s[1], 0.0)
    yh_l[1] = jnp.where(has_yp, yh_l[1] + 0.5 * ye_s[0], 0.0)

    def row(x, edge_first, edge_last):
        ex, ey, ez = eb[0, x], eb[1, x], eb[2, x]
        exn = jnp.where(rows == 127, ye_l[0, pl.ds(x, 1), :], pltpu.roll(ex, 127, 0))
        ezn = jnp.where(rows == 127, ye_l[1, pl.ds(x, 1), :], pltpu.roll(ez, 127, 0))
        if edge_last:
            ey_x, ez_x = -ey, -ez
        else:
            ey_x, ez_x = eb[1, x + 1] - ey, eb[2, x + 1] - ez
        hx = hb[0, x] - 0.5 * ((ezn - ez) - (next_z(ey, lanes) - ey))
        hy = hb[1, x] - 0.5 * ((next_z(ex, lanes) - ex) - ez_x)
        hz = hb[2, x] - 0.5 * (ey_x - (exn - ex))
        ho[0, x] = hx
        ho[1, x] = hy
        ho[2, x] = hz
        hxp = jnp.where(rows == 0, yh_l[0, pl.ds(x, 1), :], pltpu.roll(hx, 1, 0))
        hzp = jnp.where(rows == 0, yh_l[1, pl.ds(x, 1), :], pltpu.roll(hz, 1, 0))
        if edge_first:
            hy_x, hz_x = hy, hz
        else:
            hy_x, hz_x = hy - ho[1, x - 1], hz - ho[2, x - 1]
        r, c = rb[x], cb[x]
        nx = r * ex + c * ((hz - hzp) - (hy - prev_z(hy, lanes)))
        ny = r * ey + c * ((hx - prev_z(hx, lanes)) - hz_x)
        nz = r * ez + c * (hy_x - (hx - hxp))
        eo[0, x] = nx
        eo[1, x] = ny
        eo[2, x] = nz
        for at, v in enumerate((nx, ny, hx, hy)):
            t_s[at, pl.ds(x, 1), :] = plane_of(v, PLANE)

    row(0, True, False)

    def inner(x, carry):
        row(x, False, False)
        return carry

    lax.fori_loop(1, 15, inner, 0)
    row(15, False, True)

    def tangent(d):
        g = lax.rem(Y + d, GY)
        return remote(t_s.at[g], t_l.at[Y], t_ss.at[d], t_rs.at[Y], X, g)

    for d in range(1, GY):
        tangent(d).start()
    t_l[Y] = t_s[Y]
    xh = remote(ho.at[pl.ds(1, 2), 15], xh_l, x_sem.at[4], x_sem.at[5], xn, Y)
    pl.when(has_xn)(xh.start)

    def from_gy(make, d):
        make(d).wait_recv()

    for d in range(1, GY):
        s = lax.rem(Y + d, GY)
        for part in range(2):
            remote(srv.at[0], al.at[part, s], a_ss.at[part, d], a_rs.at[part, s], X, s).wait_recv()
        remote(pk_s, pk_l.at[1, s], pk_ss.at[1, d], pk_rs.at[1, s], X, s).wait_recv()
        remote(t_s.at[0], t_l.at[s], t_ss.at[d], t_rs.at[s], X, s).wait_recv()
    for s in range(GY):
        pl.when(has_xn)(remote(pk_s, pk_l.at[2, s], pk_ss.at[2, s], pk_rs.at[2, s], xn, Y).wait_recv)
        pl.when(has_xp)(remote(pk_s, pk_l.at[0, s], pk_ss.at[0, s], pk_rs.at[0, s], xp, Y).wait_recv)
    for copy in tabs:
        copy.wait()

    wave_cos = [jnp.cos(jnp.full((8, 128), ph_ref[f], F32))[0:1] for f in range(4)]
    wave_sin = [jnp.sin(jnp.full((8, 128), ph_ref[f], F32))[0:1] for f in range(4)]
    total = None
    for s in range(GY):
        nxt, own, prv = pk_l[2, s], pk_l[1, s], pk_l[0, s]
        dhz = -0.5 * nxt[0:1]
        before = -0.5 * pk_l[2, s - 1][0:1, 127:128] if s else jnp.zeros((1, 1), F32)
        dhz_p = jnp.where(lane1 == 0, before, pltpu.roll(dhz, 1, 1))
        dhy = 0.5 * nxt[1:2]
        dhyd = dhy - 0.5 * nxt[2:3]
        after = 0.5 * pk_l[0, s + 1][6:7, 0:1] if s < GY - 1 else jnp.zeros((1, 1), F32)
        hzp = prv[3:4] - 0.5 * own[0:1] + jnp.where(lane1 == 127, after, 0.0)
        last = jnp.where(
            Y == 0, own[5:6] * (dhz - dhz_p - dhyd), jnp.where(Y == 1, -own[5:6] * dhz, jnp.where(Y == 3, dhy, 0.0))
        )
        head = jnp.where(jnp.logical_and(Y == 1, has_xp), own[4:5] * hzp, 0.0)
        t = t_l[s] + jnp.where(row16 == 15, last, 0.0) + jnp.where(row16 == 0, head, 0.0)
        re = jnp.concatenate([al[0, s, f] + t * wave_cos[f] for f in range(4)], axis=0)
        im = jnp.concatenate([al[1, s, f] - t * wave_sin[f] for f in range(4)], axis=0)
        data = jnp.concatenate(
            [jnp.concatenate([re, im], axis=0), jnp.concatenate([im, -re], axis=0)], axis=1
        )
        high, low = split(data)
        part = dot_nt(ty[0, s], high) + dot_nt(ty[0, s], low) + dot_nt(ty[1, s], high)
        total = part if total is None else total + part
    bs[...] = total.reshape(GX, 8, 128)

    def column(d):
        to = lax.rem(X + d, GX)
        return remote(bs.at[to], bl.at[X], b_ss.at[d], b_rs.at[X], to, Y)

    def b_start(d, carry):
        column(d).start()
        return carry

    lax.fori_loop(1, GX, b_start, 0)
    bl[X] = bs[X]

    pl.when(has_xn)(xe.wait_recv)
    pl.when(has_xp)(xh.wait_recv)
    pl.when(jnp.logical_and(has_xn, has_yp))(corner.wait_recv)
    pl.when(has_xn)(xh.wait_send)
    dhy, dhz = 0.5 * xe_l[1], -0.5 * xe_l[0]
    ho[1, 15] = ho[1, 15] + dhy
    ho[2, 15] = ho[2, 15] + dhz
    dhz_p = jnp.where(rows == 0, -0.5 * ce_l[7:8], pltpu.roll(dhz, 1, 0))
    c = cb[15]
    eo[0, 15] = eo[0, 15] + c * ((dhz - dhz_p) - (dhy - prev_z(dhy, lanes)))
    eo[1, 15] = eo[1, 15] - c * dhz
    eo[2, 15] = eo[2, 15] + c * dhy
    hyp = jnp.where(has_xp, xh_l[0] + 0.5 * eb[2, 0], 0.0)
    hzp = jnp.where(has_xp, xh_l[1] - 0.5 * eb[1, 0], 0.0)
    c = cb[0]
    eo[1, 0] = eo[1, 0] + c * hzp
    eo[2, 0] = eo[2, 0] - c * hyp
    for d in range(1, GY):
        tangent(d).wait_send()
    t_s[0, 15:16] = plane_of(eo[0, 15], PLANE)
    t_s[1, 15:16] = plane_of(eo[1, 15], PLANE)
    t_s[1, 0:1] = plane_of(eo[1, 0], PLANE)
    t_s[3, 15:16] = plane_of(ho[1, 15], PLANE)
    for at in range(4):
        t = t_s[at]
        for f in range(4):
            nr[at, f] = srv[at, f] + t * wave_cos[f]
            ni[at, f] = siv[at, f] - t * wave_sin[f]

    def b_wait(d, carry):
        src = lax.rem(X + d, GX)
        remote(bs.at[src], bl.at[src], b_ss.at[d], b_rs.at[src], src, Y).wait_recv()
        return carry

    lax.fori_loop(1, GX, b_wait, 0)

    block = bl[...].reshape(256, 128)
    sign = jnp.where(lax.broadcasted_iota(jnp.int32, (256, 128), 1) < 64, 1.0, -1.0)
    both = jnp.concatenate([block, pltpu.roll(block, 64, 1) * sign], axis=0)
    high, low = split(both)
    y = dot_nn(tw[0], high) + dot_nn(tw[0], low) + dot_nn(tw[1], high)
    y = y * tt[0] + pltpu.roll(y, 64, 1) * tt[1]
    y_sw = pltpu.roll(y, 64, 1) * sign
    pieces = []
    for b in range(4):
        pieces += [y[64 * b : 64 * b + 64], y_sw[64 * b : 64 * b + 64]]
    high, low = split(jnp.concatenate(pieces, axis=0))
    out = dot_nt(tg[0], high) + dot_nt(tg[0], low) + dot_nt(tg[1], high)
    for a in range(8):
        for b in range(4):
            cs[4 * a + b] = out[4 * a : 4 * a + 4, 128 * b : 128 * b + 128]

    home, slot = X // 8, lax.rem(X, 8)

    def finished(d):
        to = lax.rem(X + d, GX)
        return remote(cs.at[to], cl.at[Y, slot], c_ss.at[d], c_rs.at[Y, slot], to, home)

    def c_start(d, carry):
        pl.when(jnp.logical_or(d > 0, home != Y))(finished(d).start)
        return carry

    lax.fori_loop(0, GX, c_start, 0)

    @pl.when(home == Y)
    def _():
        cl[Y, slot] = cs[X]

    def c_wait(i, carry):
        g, q = i // 8, lax.rem(i, 8)
        src = 8 * Y + q

        @pl.when(jnp.logical_or(g != Y, src != X))
        def _():
            remote(cs.at[0], cl.at[g, q], c_ss.at[0], c_rs.at[g, q], src, g).wait_recv()

        return carry

    lax.fori_loop(0, 32, c_wait, 0)

    for q in range(8):
        for g in range(4):
            rel[q, 4 * g : 4 * g + 4, :] = cl[g, q]
    turned = [pltpu.roll(rel[q], 8 * q, 1) if q else rel[q] for q in range(8)]
    group = lane16 // 8
    for s in range(16):
        acc = turned[0]
        for q in range(1, 8):
            acc = jnp.where(group == (q + s) % 16, turned[q], acc)
        if s:
            acc = pltpu.roll(acc, 128 - 8 * s, 1)
        zz[:, s, :] = acc
    for g in range(4):
        for f in range(4):
            far[0, g, f] = zz[4 * g + f, 0:8, 0:64]
            far[1, g, f] = zz[4 * g + f, 8:16, 0:64]

    pl.when(has_yp)(ye.wait_send)
    pl.when(has_yn)(yh.wait_send)
    for dx, ok in ((0, has_xp), (2, has_xn)):
        for d in range(GY):
            pl.when(ok)(pack(dx, d).wait_send)
    for d in range(1, GY):
        pack(1, d).wait_send()
        for part in range(2):
            spectrum(part, d).wait_send()
    pl.when(jnp.logical_and(has_xp, has_yn))(corner.wait_send)
    pl.when(has_xp)(xe.wait_send)

    def b_sent(d, carry):
        column(d).wait_send()
        return carry

    lax.fori_loop(1, GX, b_sent, 0)

    def c_sent(d, carry):
        pl.when(jnp.logical_or(d > 0, home != Y))(finished(d).wait_send)
        return carry

    lax.fori_loop(0, GX, c_sent, 0)


def flush_kernel(*refs):
    ins, outs, sem = refs[:5], refs[5:10], refs[10]
    copies = []
    for at, (src, dst) in enumerate(zip(ins, outs)):
        if at < 2:
            copies += [(src.at[i], dst.at[i]) for i in range(3)]
        else:
            copies.append((src, dst))
    copies = [pltpu.make_async_copy(src, dst, sem.at[at]) for at, (src, dst) in enumerate(copies)]
    for copy in copies:
        copy.start()
    for copy in copies:
        copy.wait()


def per_device(electric, magnetic, retention, coupling, spectrum_real, spectrum_imag, phases):
    tab_y, tab_w, tab_t, tab_g = (jnp.asarray(t) for t in tables())
    vmem, dma = pltpu.VMEM, pltpu.SemaphoreType.DMA
    hbm = pl.BlockSpec(memory_space=pltpu.HBM)
    in_vmem = pl.BlockSpec(memory_space=pltpu.VMEM)
    shapes = [
        jax.ShapeDtypeStruct(electric.shape, F32),
        jax.ShapeDtypeStruct(magnetic.shape, F32),
        jax.ShapeDtypeStruct(spectrum_real.shape, F32),
        jax.ShapeDtypeStruct(spectrum_imag.shape, F32),
        jax.ShapeDtypeStruct((2, 4, 4, 8, 64), F32),
    ]
    fixed = [
        pltpu.with_memory_space_constraint(a, pltpu.HBM)
        for a in (electric, magnetic, retention, coupling, spectrum_real, spectrum_imag, tab_y, tab_w, tab_t, tab_g)
    ]
    held = pl.pallas_call(
        step_kernel,
        out_shape=shapes,
        in_specs=[hbm] * 6 + [pl.BlockSpec(memory_space=pltpu.SMEM)] + [hbm] * 4,
        out_specs=[in_vmem] * 5,
        scratch_shapes=[
            vmem(electric.shape, F32), vmem(magnetic.shape, F32), vmem(retention.shape, F32), vmem(coupling.shape, F32),
            vmem(spectrum_real.shape, F32), vmem(spectrum_imag.shape, F32),
            vmem(tab_y.shape, BF16), vmem(tab_w.shape, BF16), vmem(tab_t.shape, F32), vmem(tab_g.shape, BF16),
            vmem((2, 16, 128), F32), vmem((2, 16, 128), F32), vmem((2, 16, 128), F32), vmem((2, 16, 128), F32),
            vmem((2, 128, 128), F32), vmem((2, 128, 128), F32), vmem((8, 128), F32),
            vmem((8, 128), F32), vmem((3, 4, 8, 128), F32),
            vmem((4, 16, 128), F32), vmem((4, 16, 128), F32), vmem((2, 4, 4, 16, 128), F32),
            vmem((32, 8, 128), F32), vmem((32, 8, 128), F32), vmem((32, 4, 128), F32), vmem((4, 8, 4, 128), F32),
            vmem((8, 16, 128), F32), vmem((16, 16, 128), F32),
            dma((14,)), dma((4,)), dma((3, 4)), dma((3, 4)), dma((2, 4)), dma((2, 4)), dma((4,)), dma((4,)), dma((6,)),
            dma((32,)), dma((32,)), dma((32,)), dma((4, 8)),
        ],
        compiler_params=pltpu.CompilerParams(collective_id=0, has_side_effects=True, vmem_limit_bytes=40 * 2**20),
    )(*fixed[:6], pltpu.with_memory_space_constraint(phases, pltpu.HBM), *fixed[6:])
    return pl.pallas_call(
        flush_kernel,
        out_shape=shapes,
        in_specs=[in_vmem] * 5,
        out_specs=[hbm] * 5,
        scratch_shapes=[dma((9,))],
        compiler_params=pltpu.CompilerParams(vmem_limit_bytes=16 * 2**20),
    )(*held)


def solution(mesh):
    placed = (
        P(None, "gx", "gy", None),
        P(None, "gx", "gy", None),
        P("gx", "gy", None),
        P("gx", "gy", None),
        P(None, None, "gx", "gy"),
        P(None, None, "gx", "gy"),
        P(),
    )
    return jax.shard_map(
        per_device,
        mesh=mesh,
        in_specs=placed,
        out_specs=(
            P(None, "gx", "gy", None),
            P(None, "gx", "gy", None),
            P(None, None, "gx", "gy"),
            P(None, None, "gx", "gy"),
            P(None, None, None, "gx", "gy"),
        ),
        check_vma=False,
    )
```

```python
import functools
import math

import jax
import jax.numpy as jnp
import numpy as np
from jax import lax
from jax.experimental import pallas as pl
from jax.experimental.pallas import tpu as pltpu
from jax.sharding import PartitionSpec as P

MESH = pl.DeviceIdType.MESH
WAVES = 256
PLANE = 111
GX, GY = 32, 4
F32, BF16 = jnp.float32, jnp.bfloat16


def split_np(table):
    high = table.astype(np.float32).astype(jnp.bfloat16)
    low = (table - high.astype(np.float64)).astype(np.float32).astype(jnp.bfloat16)
    return np.stack([high, low])


def angle_np(wave, place):
    return (np.multiply.outer(wave, place) % 1024) * (math.pi / 512)


@functools.cache
def tables():
    wave = 2 * np.arange(WAVES) - 255
    ang = angle_np(wave, np.arange(512)).reshape(256, 4, 128).transpose(1, 0, 2)
    tab_y = split_np(np.concatenate([np.cos(ang), np.sin(ang)], axis=2))
    ang = angle_np(2 * np.arange(32) - 255, 16 * np.arange(32))
    eye = np.eye(8)
    tab_w = split_np(np.concatenate([np.kron(np.cos(ang), eye), np.kron(np.sin(ang), eye)], axis=1))
    ang = np.repeat(angle_np(2 * np.arange(32) - 255, np.arange(16)), 8, axis=0)
    cos, sin = np.tile(np.cos(ang), (1, 8)), np.tile(np.sin(ang), (1, 8))
    sin[:, 64:] *= -1
    tab_t = np.stack([cos, sin]).astype(np.float32)
    ang = 2 * math.pi * (np.multiply.outer(np.arange(8), np.arange(16)) % 16) / 16
    eye = np.eye(4)
    blocks = [np.einsum("ai,fg->afgi", t, eye).reshape(32, 64) for t in (np.cos(ang), np.sin(ang))]
    tab_g = split_np(np.concatenate(blocks, axis=1) / 512.0)
    return tab_y, tab_w, tab_t, tab_g


def split(value):
    high = value.astype(BF16)
    return high, (value - high.astype(F32)).astype(BF16)


def dot_nt(a, b):
    return lax.dot_general(a, b, (((1,), (1,)), ((), ())), preferred_element_type=F32)


def dot_nn(a, b):
    return lax.dot_general(a, b, (((1,), (0,)), ((), ())), preferred_element_type=F32)


def plane_of(value, at):
    wide = jnp.broadcast_to(value[:, at : at + 1], (128, 128))
    rows = lax.broadcasted_iota(jnp.int32, (128, 128), 0)
    lanes = lax.broadcasted_iota(jnp.int32, (128, 128), 1)
    return jnp.sum(jnp.where(rows == lanes, wide, 0.0), axis=0, keepdims=True)


def step_kernel(
    e_hbm, h_hbm, r_hbm, c_hbm, sr_hbm, si_hbm, ph_ref, ty_hbm, tw_hbm, tt_hbm, tg_hbm,
    eo, ho, nr, ni, rel,
    eb, hb, rb, cb, srv, siv, ty, tw, tt, tg,
    ye_s, yh_s, ye_l, yh_l, xe_l, xh_l, ce_l, pk_s, pk_l, t_s, t_l, al,
    bs, bl, cs, cl, xh_s, pp,
    ld_sem, yh_sem, pk_ss, pk_rs, a_ss, a_rs, t_ss, t_rs, x_sem, b_ss, b_rs, c_ss, c_rs,
):
    X = lax.axis_index("gx")
    Y = lax.axis_index("gy")
    xn, xp = lax.rem(X + 1, GX), lax.rem(X + GX - 1, GX)
    yn, yp = lax.rem(Y + 1, GY), lax.rem(Y + GY - 1, GY)
    has_xn, has_xp, has_yn, has_yp = X < GX - 1, X > 0, Y < GY - 1, Y > 0

    pending = []
    barrier = pltpu.get_barrier_semaphore()
    home, slot = X // 8, lax.rem(X, 8)

    def greet(x, y):
        pl.semaphore_signal(barrier, inc=1, device_id=(x, y), device_id_type=MESH)

    def greet_gx(d, carry):
        greet(lax.rem(X + d, GX), Y)
        return carry

    def greet_home(q, carry):
        src = 8 * Y + q
        for d in range(1, GY):
            greet(src, lax.rem(Y + d, GY))
        return carry

    for d in range(1, GY):
        for x in (xp, X, xn):
            greet(x, lax.rem(Y + d, GY))
    lax.fori_loop(1, GX, greet_gx, 0)
    lax.fori_loop(0, 8, greet_home, 0)
    greeted = 3 * (GY - 1) + (GX - 1) + jnp.where(home != Y, GX, 0)

    loads = []

    def load(src, dst):
        copy = pltpu.make_async_copy(src, dst, ld_sem.at[len(loads)])
        copy.start()
        loads.append(copy)
        return copy

    chunks = []
    for at in range(4):
        part = pl.ds(4 * at, 4)
        chunks.append(
            [
                load(e_hbm.at[:, part], eb.at[:, part]),
                load(h_hbm.at[:, part], hb.at[:, part]),
                load(c_hbm.at[part], cb.at[part]),
                load(r_hbm.at[part], rb.at[part]),
            ]
        )
    spec = [load(sr_hbm, srv), load(si_hbm, siv)]

    rows = lax.broadcasted_iota(jnp.int32, (128, 128), 0)
    lanes = lax.broadcasted_iota(jnp.int32, (128, 128), 1)
    row16 = lax.broadcasted_iota(jnp.int32, (16, 128), 0)
    lane16 = lax.broadcasted_iota(jnp.int32, (16, 128), 1)
    lane1 = lax.broadcasted_iota(jnp.int32, (1, 128), 1)

    def next_z(v, lane):
        return jnp.where(lane == 127, 0.0, pltpu.roll(v, 127, 1))

    def prev_z(v, lane):
        return jnp.where(lane == 0, 0.0, pltpu.roll(v, 1, 1))

    @pl.when(jnp.logical_not(has_xn))
    def _():
        xe_l[...] = jnp.zeros_like(xe_l)
        pk_l[2] = jnp.zeros_like(pk_l[2])

    @pl.when(jnp.logical_not(has_xp))
    def _():
        xh_l[...] = jnp.zeros_like(xh_l)
        pk_l[0] = jnp.zeros_like(pk_l[0])

    @pl.when(jnp.logical_not(has_yn))
    def _():
        ye_l[...] = jnp.zeros_like(ye_l)

    @pl.when(jnp.logical_not(has_yp))
    def _():
        yh_l[...] = jnp.zeros_like(yh_l)

    @pl.when(jnp.logical_not(jnp.logical_and(has_xn, has_yp)))
    def _():
        ce_l[...] = jnp.zeros_like(ce_l)

    picks = (
        (eb, 0, (110, 111, 112)), (eb, 1, (110, 111, 112)), (eb, 2, (110, 111)),
        (hb, 0, (110, 111)), (hb, 1, (110, 111)), (hb, 2, (111,)),
    )

    def pick(x, carry):
        at = 0
        for ref, which, planes in picks:
            v = ref[which, x]
            for z in planes:
                pp[at, pl.ds(x, 1), :] = plane_of(v, z)
                at += 1
        for ref in (rb, cb):
            pp[at, pl.ds(x, 1), :] = plane_of(ref[x], PLANE)
            at += 1
        return carry

    for at in range(4):
        for copy in chunks[at]:
            copy.wait()
        lax.fori_loop(4 * at, 4 * at + 4, pick, 0)
    tabs = [load(ty_hbm, ty), load(tw_hbm, tw), load(tt_hbm, tt), load(tg_hbm, tg)]

    ex0, ex1, ex2, ey0, ey1, ey2, ez0, ez1, hx0, hx1, hy0, hy1, hz1, r1, c1 = (pp[at] for at in range(15))

    def next_x(v):
        return jnp.where(row16 == 15, 0.0, pltpu.roll(v, 15, 0))

    def prev_x(v):
        return jnp.where(row16 == 0, 0.0, pltpu.roll(v, 1, 0))

    phx1 = hx1 - 0.5 * ((next_z(ez1, lane16) - ez1) - (ey2 - ey1))
    phx0 = hx0 - 0.5 * ((next_z(ez0, lane16) - ez0) - (ey1 - ey0))
    phy1 = hy1 - 0.5 * ((ex2 - ex1) - (next_x(ez1) - ez1))
    phy0 = hy0 - 0.5 * ((ex1 - ex0) - (next_x(ez0) - ez0))
    phz1 = hz1 - 0.5 * ((next_x(ey1) - ey1) - (next_z(ex1, lane16) - ex1))
    t_s[0, 0:16] = r1 * ex1 + c1 * ((phz1 - prev_z(phz1, lane16)) - (phy1 - phy0))
    t_s[1, 0:16] = r1 * ey1 + c1 * ((phx1 - phx0) - (phz1 - prev_x(phz1)))
    t_s[2, 0:16] = phx1
    t_s[3, 0:16] = phy1
    cols = jnp.zeros((16, 128), F32)
    for at, (v, y) in enumerate(((ex1, 0), (ez1, 0), (ez0, 0), (c1, 0), (phz1, 127), (c1, 127))):
        cols = jnp.where(lane16 == at, v[:, y : y + 1], cols)
    for g in range(GY):
        t_s[g, 16:32] = cols
    pk_s[0:1] = ey1[0:1]
    pk_s[1:2] = ez1[0:1]
    pk_s[2:3] = ez0[0:1]
    pk_s[3:4] = phz1[15:16]
    pk_s[4:5] = c1[0:1]
    pk_s[5:6] = c1[15:16]
    pk_s[6:7] = ex1[15:16]
    pk_s[7:8] = jnp.zeros((1, 128), F32)

    ye_s[0] = eb[0, :, 0, :]
    ye_s[1] = eb[2, :, 0, :]
    ex, ey, ez = eb[0, :, 127, :], eb[1, :, 127, :], eb[2, :, 127, :]
    yh_s[0] = hb[0, :, 127, :] - 0.5 * (-ez - (next_z(ey, lane16) - ey))
    ey_up = jnp.where(row16 == 15, 0.0, pltpu.roll(ey, 15, 0))
    yh_s[1] = hb[2, :, 127, :] - 0.5 * (ey_up - ey + ex)

    pk_l[1, Y] = pk_s[...]
    for copy in spec:
        copy.wait()
    al[0, Y] = srv[Y]
    al[1, Y] = siv[Y]
    t_l[Y] = t_s[Y]

    pl.semaphore_wait(barrier, greeted)

    def remote(src, dst, ss, rs, x, y):
        return pltpu.make_async_remote_copy(
            src_ref=src, dst_ref=dst, send_sem=ss, recv_sem=rs, device_id=(x, y), device_id_type=MESH
        )

    def pack(dx, d):
        return remote(
            pk_s, pk_l.at[2 - dx, Y], pk_ss.at[dx, d], pk_rs.at[2 - dx, Y], (xp, X, xn)[dx], lax.rem(Y + d, GY)
        )

    for dx, ok in ((0, has_xp), (2, has_xn)):
        for d in range(GY):
            pl.when(ok)(pack(dx, d).start)
    for d in range(1, GY):
        pack(1, d).start()

    def packs_sent():
        for dx, ok in ((0, has_xp), (2, has_xn)):
            for d in range(GY):
                pl.when(ok)(pack(dx, d).wait_send)
        for d in range(1, GY):
            pack(1, d).wait_send()

    pending.append(packs_sent)

    def tangent(d):
        g = lax.rem(Y + d, GY)
        return remote(t_s.at[g], t_l.at[Y], t_ss.at[d], t_rs.at[Y], X, g)

    for d in range(1, GY):
        tangent(d).start()
        pending.append(tangent(d).wait_send)

    def spectrum(part, d):
        g = lax.rem(Y + d, GY)
        return remote((srv, siv)[part].at[g], al.at[part, Y], a_ss.at[part, d], a_rs.at[part, Y], X, g)

    for d in range(1, GY):
        for part in range(2):
            spectrum(part, d).start()
            pending.append(spectrum(part, d).wait_send)

    ye = remote(ye_s, ye_l, yh_sem.at[0], yh_sem.at[1], X, yp)
    yh = remote(yh_s, yh_l, yh_sem.at[2], yh_sem.at[3], X, yn)
    pl.when(has_yp)(ye.start)
    pl.when(has_yn)(yh.start)
    pending.append(lambda: pl.when(has_yp)(ye.wait_send))
    pending.append(lambda: pl.when(has_yn)(yh.wait_send))

    corner = remote(eb.at[1, 0, pl.ds(120, 8)], ce_l, x_sem.at[0], x_sem.at[1], xp, yn)
    pl.when(jnp.logical_and(has_xp, has_yn))(corner.start)
    pending.append(lambda: pl.when(jnp.logical_and(has_xp, has_yn))(corner.wait_send))
    xe = remote(eb.at[pl.ds(1, 2), 0], xe_l, x_sem.at[2], x_sem.at[3], xp, Y)
    pl.when(has_xp)(xe.start)
    pending.append(lambda: pl.when(has_xp)(xe.wait_send))

    pl.when(has_yn)(ye.wait_recv)
    pl.when(has_yp)(yh.wait_recv)
    yh_l[0] = jnp.where(has_yp, yh_l[0] - 0.5 * ye_s[1], 0.0)
    yh_l[1] = jnp.where(has_yp, yh_l[1] + 0.5 * ye_s[0], 0.0)

    ex, ey, ez = eb[0, 15], eb[1, 15], eb[2, 15]
    exn = jnp.where(rows == 127, ye_l[0, 15:16, :], pltpu.roll(ex, 127, 0))
    xh_s[0] = hb[1, 15] - 0.5 * ((next_z(ex, lanes) - ex) + ez)
    xh_s[1] = hb[2, 15] - 0.5 * (-ey - (exn - ex))
    xh = remote(xh_s, xh_l, x_sem.at[4], x_sem.at[5], xn, Y)
    pl.when(has_xn)(xh.start)
    pending.append(lambda: pl.when(has_xn)(xh.wait_send))

    def from_gy(make, d):
        make(d).wait_recv()

    for d in range(1, GY):
        s = lax.rem(Y + d, GY)
        for part in range(2):
            remote(srv.at[0], al.at[part, s], a_ss.at[part, d], a_rs.at[part, s], X, s).wait_recv()
        remote(pk_s, pk_l.at[1, s], pk_ss.at[1, d], pk_rs.at[1, s], X, s).wait_recv()
        remote(t_s.at[0], t_l.at[s], t_ss.at[d], t_rs.at[s], X, s).wait_recv()
    for s in range(GY):
        pl.when(has_xn)(remote(pk_s, pk_l.at[2, s], pk_ss.at[2, s], pk_rs.at[2, s], xn, Y).wait_recv)
        pl.when(has_xp)(remote(pk_s, pk_l.at[0, s], pk_ss.at[0, s], pk_rs.at[0, s], xp, Y).wait_recv)
    for copy in tabs:
        copy.wait()

    wave_cos = [jnp.cos(jnp.full((8, 128), ph_ref[f], F32))[0:1] for f in range(4)]
    wave_sin = [jnp.sin(jnp.full((8, 128), ph_ref[f], F32))[0:1] for f in range(4)]
    total = None
    for s in range(GY):
        nxt, own, prv = pk_l[2, s], pk_l[1, s], pk_l[0, s]
        dhz = -0.5 * nxt[0:1]
        before = -0.5 * pk_l[2, s - 1][0:1, 127:128] if s else jnp.zeros((1, 1), F32)
        dhz_p = jnp.where(lane1 == 0, before, pltpu.roll(dhz, 1, 1))
        dhy = 0.5 * nxt[1:2]
        dhyd = dhy - 0.5 * nxt[2:3]
        after = 0.5 * pk_l[0, s + 1][6:7, 0:1] if s < GY - 1 else jnp.zeros((1, 1), F32)
        hzp = prv[3:4] - 0.5 * own[0:1] + jnp.where(lane1 == 127, after, 0.0)
        last = jnp.where(
            Y == 0, own[5:6] * (dhz - dhz_p - dhyd), jnp.where(Y == 1, -own[5:6] * dhz, jnp.where(Y == 3, dhy, 0.0))
        )
        head = jnp.where(jnp.logical_and(Y == 1, has_xp), own[4:5] * hzp, 0.0)
        t = t_l[s, 0:16] + jnp.where(row16 == 15, last, 0.0) + jnp.where(row16 == 0, head, 0.0)
        mine = t_l[s, 16:32]
        if s < GY - 1:
            after = t_l[s + 1, 16:32]
            exn, ez1n, ez0n, c127 = after[:, 0:1], after[:, 1:2], after[:, 2:3], mine[:, 5:6]
            exn_p = prev_x(after)[:, 0:1]
            edge = jnp.where(
                Y == 0,
                0.5 * c127 * exn,
                jnp.where(Y == 1, -0.5 * c127 * ((ez1n - ez0n) + (exn - exn_p)), jnp.where(Y == 2, -0.5 * ez1n, 0.0)),
            )
            t = t + jnp.where(lane16 == 127, edge, 0.0)
        if s > 0:
            hzp0 = t_l[s - 1, 16:32][:, 4:5] + 0.5 * mine[:, 0:1]
            t = t + jnp.where(lane16 == 0, jnp.where(Y == 0, -mine[:, 3:4] * hzp0, 0.0), 0.0)
        re = jnp.concatenate([al[0, s, f] + t * wave_cos[f] for f in range(4)], axis=0)
        im = jnp.concatenate([al[1, s, f] - t * wave_sin[f] for f in range(4)], axis=0)
        data = jnp.concatenate(
            [jnp.concatenate([re, im], axis=0), jnp.concatenate([im, -re], axis=0)], axis=1
        )
        high, low = split(data)
        part = dot_nt(ty[0, s], high) + dot_nt(ty[0, s], low) + dot_nt(ty[1, s], high)
        total = part if total is None else total + part
    bs[...] = total.reshape(GX, 8, 128)

    def column(d):
        to = lax.rem(X + d, GX)
        return remote(bs.at[to], bl.at[X], b_ss.at[d], b_rs.at[X], to, Y)

    def b_start(d, carry):
        column(d).start()
        return carry

    lax.fori_loop(1, GX, b_start, 0)

    def b_sent(d, carry):
        column(d).wait_send()
        return carry

    pending.append(lambda: lax.fori_loop(1, GX, b_sent, 0))
    bl[X] = bs[X]

    def row(x, edge_first, edge_last):
        ex, ey, ez = eb[0, x], eb[1, x], eb[2, x]
        exn = jnp.where(rows == 127, ye_l[0, pl.ds(x, 1), :], pltpu.roll(ex, 127, 0))
        ezn = jnp.where(rows == 127, ye_l[1, pl.ds(x, 1), :], pltpu.roll(ez, 127, 0))
        if edge_last:
            ey_x, ez_x = -ey, -ez
        else:
            ey_x, ez_x = eb[1, x + 1] - ey, eb[2, x + 1] - ez
        hx = hb[0, x] - 0.5 * ((ezn - ez) - (next_z(ey, lanes) - ey))
        hy = hb[1, x] - 0.5 * ((next_z(ex, lanes) - ex) - ez_x)
        hz = hb[2, x] - 0.5 * (ey_x - (exn - ex))
        ho[0, x] = hx
        ho[1, x] = hy
        ho[2, x] = hz
        hxp = jnp.where(rows == 0, yh_l[0, pl.ds(x, 1), :], pltpu.roll(hx, 1, 0))
        hzp = jnp.where(rows == 0, yh_l[1, pl.ds(x, 1), :], pltpu.roll(hz, 1, 0))
        if edge_first:
            hy_x, hz_x = hy, hz
        else:
            hy_x, hz_x = hy - ho[1, x - 1], hz - ho[2, x - 1]
        r, c = rb[x], cb[x]
        nx = r * ex + c * ((hz - hzp) - (hy - prev_z(hy, lanes)))
        ny = r * ey + c * ((hx - prev_z(hx, lanes)) - hz_x)
        nz = r * ez + c * (hy_x - (hx - hxp))
        eo[0, x] = nx
        eo[1, x] = ny
        eo[2, x] = nz
    row(0, True, False)

    def inner(x, carry):
        row(x, False, False)
        return carry

    lax.fori_loop(1, 15, inner, 0)
    row(15, False, True)

    pl.when(has_xn)(xe.wait_recv)
    pl.when(has_xp)(xh.wait_recv)
    pl.when(jnp.logical_and(has_xn, has_yp))(corner.wait_recv)
    dhy, dhz = 0.5 * xe_l[1], -0.5 * xe_l[0]
    ho[1, 15] = ho[1, 15] + dhy
    ho[2, 15] = ho[2, 15] + dhz
    dhz_p = jnp.where(rows == 0, -0.5 * ce_l[7:8], pltpu.roll(dhz, 1, 0))
    c = cb[15]
    eo[0, 15] = eo[0, 15] + c * ((dhz - dhz_p) - (dhy - prev_z(dhy, lanes)))
    eo[1, 15] = eo[1, 15] - c * dhz
    eo[2, 15] = eo[2, 15] + c * dhy
    hyp = jnp.where(has_xp, xh_l[0] + 0.5 * eb[2, 0], 0.0)
    hzp = jnp.where(has_xp, xh_l[1] - 0.5 * eb[1, 0], 0.0)
    c = cb[0]
    eo[1, 0] = eo[1, 0] + c * hzp
    eo[2, 0] = eo[2, 0] - c * hyp
    def b_wait(d, carry):
        src = lax.rem(X + d, GX)
        remote(bs.at[src], bl.at[src], b_ss.at[d], b_rs.at[src], src, Y).wait_recv()
        return carry

    lax.fori_loop(1, GX, b_wait, 0)

    block = bl[...].reshape(256, 128)
    sign = jnp.where(lax.broadcasted_iota(jnp.int32, (256, 128), 1) < 64, 1.0, -1.0)
    both = jnp.concatenate([block, pltpu.roll(block, 64, 1) * sign], axis=0)
    high, low = split(both)
    y = dot_nn(tw[0], high) + dot_nn(tw[0], low) + dot_nn(tw[1], high)
    y = y * tt[0] + pltpu.roll(y, 64, 1) * tt[1]
    y_sw = pltpu.roll(y, 64, 1) * sign
    pieces = []
    for b in range(4):
        pieces += [y[64 * b : 64 * b + 64], y_sw[64 * b : 64 * b + 64]]
    high, low = split(jnp.concatenate(pieces, axis=0))
    out = dot_nt(tg[0], high) + dot_nt(tg[0], low) + dot_nt(tg[1], high)
    for a in range(8):
        for b in range(4):
            cs[4 * a + b] = out[4 * a : 4 * a + 4, 128 * b : 128 * b + 128]

    def finished(d):
        to = lax.rem(X + d, GX)
        return remote(cs.at[to], cl.at[Y, slot], c_ss.at[d], c_rs.at[Y, slot], to, home)

    def c_start(d, carry):
        pl.when(jnp.logical_or(d > 0, home != Y))(finished(d).start)
        return carry

    lax.fori_loop(0, GX, c_start, 0)

    def c_sent(d, carry):
        pl.when(jnp.logical_or(d > 0, home != Y))(finished(d).wait_send)
        return carry

    pending.append(lambda: lax.fori_loop(0, GX, c_sent, 0))

    @pl.when(home == Y)
    def _():
        cl[Y, slot] = cs[X]

    def own_plane(x, carry):
        for at, v in enumerate((eo[0, x], eo[1, x], ho[0, x], ho[1, x])):
            pp[at, pl.ds(x, 1), :] = plane_of(v, PLANE)
        return carry

    lax.fori_loop(0, 16, own_plane, 0)
    for at in range(4):
        t = pp[at]
        for f in range(4):
            nr[at, f] = srv[at, f] + t * wave_cos[f]
            ni[at, f] = siv[at, f] - t * wave_sin[f]

    def c_wait(i, carry):
        g, q = i // 8, lax.rem(i, 8)
        src = 8 * Y + q

        @pl.when(jnp.logical_or(g != Y, src != X))
        def _():
            remote(cs.at[0], cl.at[g, q], c_ss.at[0], c_rs.at[g, q], src, g).wait_recv()

        return carry

    lax.fori_loop(0, 32, c_wait, 0)

    for q in range(8):
        for g in range(4):
            rel[q, 4 * g : 4 * g + 4, :] = cl[g, q]
    for wait in pending:
        wait()


def flush_kernel(eo, ho, nr, ni, rel, e_out, h_out, r_out, i_out, f_out, zz, fv, sem):
    copies = [(eo.at[i], e_out.at[i]) for i in range(3)] + [(ho.at[i], h_out.at[i]) for i in range(3)]
    copies += [(nr, r_out), (ni, i_out)]
    copies = [pltpu.make_async_copy(src, dst, sem.at[at]) for at, (src, dst) in enumerate(copies)]
    for copy in copies:
        copy.start()
    lane16 = lax.broadcasted_iota(jnp.int32, (16, 128), 1)
    turned = [pltpu.roll(rel[q], 8 * q, 1) if q else rel[q] for q in range(8)]
    group = lane16 // 8
    for s in range(16):
        acc = turned[0]
        for q in range(1, 8):
            acc = jnp.where(group == (q + s) % 16, turned[q], acc)
        if s:
            acc = pltpu.roll(acc, 128 - 8 * s, 1)
        zz[:, s, :] = acc
    for g in range(4):
        for f in range(4):
            fv[0, g, f] = zz[4 * g + f, 0:8, 0:64]
            fv[1, g, f] = zz[4 * g + f, 8:16, 0:64]
    copies.append(pltpu.make_async_copy(fv, f_out, sem.at[8]))
    copies[-1].start()
    for copy in copies:
        copy.wait()


def per_device(electric, magnetic, retention, coupling, spectrum_real, spectrum_imag, phases):
    tab_y, tab_w, tab_t, tab_g = (jnp.asarray(t) for t in tables())
    vmem, dma = pltpu.VMEM, pltpu.SemaphoreType.DMA
    hbm = pl.BlockSpec(memory_space=pltpu.HBM)
    in_vmem = pl.BlockSpec(memory_space=pltpu.VMEM)
    shapes = [
        jax.ShapeDtypeStruct(electric.shape, F32),
        jax.ShapeDtypeStruct(magnetic.shape, F32),
        jax.ShapeDtypeStruct(spectrum_real.shape, F32),
        jax.ShapeDtypeStruct(spectrum_imag.shape, F32),
        jax.ShapeDtypeStruct((2, 4, 4, 8, 64), F32),
    ]
    fixed = [
        pltpu.with_memory_space_constraint(a, pltpu.HBM)
        for a in (electric, magnetic, retention, coupling, spectrum_real, spectrum_imag, tab_y, tab_w, tab_t, tab_g)
    ]
    held = pl.pallas_call(
        step_kernel,
        out_shape=shapes[:4] + [jax.ShapeDtypeStruct((8, 16, 128), F32)],
        in_specs=[hbm] * 6 + [pl.BlockSpec(memory_space=pltpu.SMEM)] + [hbm] * 4,
        out_specs=[in_vmem] * 5,
        scratch_shapes=[
            vmem(electric.shape, F32), vmem(magnetic.shape, F32), vmem(retention.shape, F32), vmem(coupling.shape, F32),
            vmem(spectrum_real.shape, F32), vmem(spectrum_imag.shape, F32),
            vmem(tab_y.shape, BF16), vmem(tab_w.shape, BF16), vmem(tab_t.shape, F32), vmem(tab_g.shape, BF16),
            vmem((2, 16, 128), F32), vmem((2, 16, 128), F32), vmem((2, 16, 128), F32), vmem((2, 16, 128), F32),
            vmem((2, 128, 128), F32), vmem((2, 128, 128), F32), vmem((8, 128), F32),
            vmem((8, 128), F32), vmem((3, 4, 8, 128), F32),
            vmem((4, 32, 128), F32), vmem((4, 32, 128), F32), vmem((2, 4, 4, 16, 128), F32),
            vmem((32, 8, 128), F32), vmem((32, 8, 128), F32), vmem((32, 4, 128), F32), vmem((4, 8, 4, 128), F32),
            vmem((2, 128, 128), F32), vmem((15, 16, 128), F32),
            dma((22,)), dma((4,)), dma((3, 4)), dma((3, 4)), dma((2, 4)), dma((2, 4)), dma((4,)), dma((4,)), dma((6,)),
            dma((32,)), dma((32,)), dma((32,)), dma((4, 8)),
        ],
        compiler_params=pltpu.CompilerParams(collective_id=0, has_side_effects=True, vmem_limit_bytes=40 * 2**20),
    )(*fixed[:6], pltpu.with_memory_space_constraint(phases, pltpu.HBM), *fixed[6:])
    return pl.pallas_call(
        flush_kernel,
        out_shape=shapes,
        in_specs=[in_vmem] * 5,
        out_specs=[hbm] * 5,
        scratch_shapes=[vmem((16, 16, 128), F32), vmem((2, 4, 4, 8, 64), F32), dma((9,))],
        compiler_params=pltpu.CompilerParams(vmem_limit_bytes=16 * 2**20),
    )(*held)


def solution(mesh):
    placed = (
        P(None, "gx", "gy", None),
        P(None, "gx", "gy", None),
        P("gx", "gy", None),
        P("gx", "gy", None),
        P(None, None, "gx", "gy"),
        P(None, None, "gx", "gy"),
        P(),
    )
    return jax.shard_map(
        per_device,
        mesh=mesh,
        in_specs=placed,
        out_specs=(
            P(None, "gx", "gy", None),
            P(None, "gx", "gy", None),
            P(None, None, "gx", "gy"),
            P(None, None, "gx", "gy"),
            P(None, None, None, "gx", "gy"),
        ),
        check_vma=False,
    )
```

```python
import functools
import itertools
import math

import jax
import jax.numpy as jnp
import numpy as np
from jax import lax
from jax.experimental import pallas as pl
from jax.experimental.pallas import tpu as pltpu
from jax.sharding import PartitionSpec as P

MESH = pl.DeviceIdType.MESH
WAVES = 256
PLANE = 111
GX, GY = 32, 4
F32, BF16 = jnp.float32, jnp.bfloat16


def split_np(table):
    high = table.astype(np.float32).astype(jnp.bfloat16)
    low = (table - high.astype(np.float64)).astype(np.float32).astype(jnp.bfloat16)
    return np.stack([high, low])


def angle_np(wave, place):
    return (np.multiply.outer(wave, place) % 1024) * (math.pi / 512)


@functools.cache
def tables():
    wave = 2 * np.arange(WAVES) - 255
    ang = angle_np(wave, np.arange(512)).reshape(256, 4, 128).transpose(1, 0, 2)
    tab_y = split_np(np.concatenate([np.cos(ang), np.sin(ang)], axis=2))
    ang = angle_np(2 * np.arange(32) - 255, 16 * np.arange(32))
    eye = np.eye(8)
    ang = ang.reshape(32, 4, 2, 4).transpose(2, 0, 1, 3).reshape(2, 32, 16)
    tab_w = np.stack([np.concatenate([np.kron(np.cos(a), eye), np.kron(np.sin(a), eye)], axis=1) for a in ang])
    tab_w = split_np(tab_w)
    ang = np.repeat(angle_np(2 * np.arange(32) - 255, np.arange(16)), 8, axis=0)
    cos, sin = np.tile(np.cos(ang), (1, 8)), np.tile(np.sin(ang), (1, 8))
    sin[:, 64:] *= -1
    tab_t = np.stack([cos, sin]).astype(np.float32)
    ang = 2 * math.pi * (np.multiply.outer(np.arange(8), np.arange(16)) % 16) / 16
    eye = np.eye(4)
    blocks = [np.einsum("ai,fg->afgi", t, eye).reshape(32, 64) for t in (np.cos(ang), np.sin(ang))]
    tab_g = split_np(np.concatenate(blocks, axis=1) / 512.0)
    return tab_y, tab_w, tab_t, tab_g


def hops(o):
    return min(o[0], 4 - o[0]) + 2 * o[1] + min(o[2], 4 - o[2])


def split(value):
    high = value.astype(BF16)
    return high, (value - high.astype(F32)).astype(BF16)


def dot_nt(a, b):
    return lax.dot_general(a, b, (((1,), (1,)), ((), ())), preferred_element_type=F32)


def dot_nn(a, b):
    return lax.dot_general(a, b, (((1,), (0,)), ((), ())), preferred_element_type=F32)


def plane_of(value, at):
    wide = jnp.broadcast_to(value[:, at : at + 1], (128, 128))
    rows = lax.broadcasted_iota(jnp.int32, (128, 128), 0)
    lanes = lax.broadcasted_iota(jnp.int32, (128, 128), 1)
    return jnp.sum(jnp.where(rows == lanes, wide, 0.0), axis=0, keepdims=True)


def step_kernel(
    e_hbm, h_hbm, r_hbm, c_hbm, sr_hbm, si_hbm, ph_hbm, ty_hbm, tw_hbm, tt_hbm, tg_hbm,
    eo, ho, nr, ni, rel,
    eb, hb, rb, cb, srv, siv, ty, tw, tt, tg,
    ye_s, yh_s, ye_l, yh_l, xe_l, xh_l, ce_l, pk_s, pk_l, t_s, t_l, al,
    bs, bl, cs, cl, xh_s, pp, wv, ph_ref,
    ld_sem, yh_sem, pk_ss, pk_rs, a_ss, a_rs, t_ss, t_rs, x_sem, b_ss, b_rs, c_ss, c_rs, ph_sem,
):
    X = lax.axis_index("gx")
    Y = lax.axis_index("gy")
    xn, xp = lax.rem(X + 1, GX), lax.rem(X + GX - 1, GX)
    yn, yp = lax.rem(Y + 1, GY), lax.rem(Y + GY - 1, GY)
    has_xn, has_xp, has_yn, has_yp = X < GX - 1, X > 0, Y < GY - 1, Y > 0

    pending = []
    barrier = pltpu.get_barrier_semaphore()
    home, slot = X // 8, lax.rem(X, 8)
    offsets = sorted(itertools.product(range(4), range(2), range(4)), key=lambda o: (-hops(o), o))
    at_y = [((X // 8 + a) & 3) * 8 for a in range(4)]
    at_x = [((X // 4 + b) & 1) * 4 for b in range(2)]
    at_z = [(X + c) & 3 for c in range(4)]

    def block_at(o):
        return at_y[o[0]] + at_x[o[1]] + at_z[o[2]]

    def greet(x, y):
        pl.semaphore_signal(barrier, inc=1, device_id=(x, y), device_id_type=MESH)

    others = [lax.rem(Y + d, GY) for d in range(1, GY)]
    for o in offsets[:-1]:
        greet(block_at(o), Y)
    for x in (xp, xn, X):
        for y in others:
            greet(x, y)
    for o in sorted(itertools.product(range(2), range(4)), key=lambda o: (-hops((0,) + o), o)):
        for y in others:
            greet(8 * Y + at_x[o[0]] + at_z[o[1]], y)
    greeted = 3 * (GY - 1) + (GX - 1) + jnp.where(home != Y, GX, 0)

    loads = []

    def load(src, dst):
        copy = pltpu.make_async_copy(src, dst, ld_sem.at[len(loads)])
        copy.start()
        loads.append(copy)
        return copy

    phase = pltpu.make_async_copy(ph_hbm, ph_ref, ph_sem)
    phase.start()
    chunks = []
    for at in range(4):
        part = pl.ds(4 * at, 4)
        chunks.append(
            [
                load(e_hbm.at[:, part], eb.at[:, part]),
                load(h_hbm.at[:, part], hb.at[:, part]),
                load(c_hbm.at[part], cb.at[part]),
                load(r_hbm.at[part], rb.at[part]),
            ]
        )
    spec = [load(sr_hbm, srv), load(si_hbm, siv)]
    phase.wait()
    row8 = lax.broadcasted_iota(jnp.int32, (8, 128), 0)
    angle = jnp.zeros((8, 128), F32)
    for f in range(4):
        angle = jnp.where(lax.rem(row8, 4) == f, ph_ref[f], angle)
    wv[...] = jnp.where(row8 < 4, jnp.cos(angle), jnp.sin(angle))

    rows = lax.broadcasted_iota(jnp.int32, (128, 128), 0)
    lanes = lax.broadcasted_iota(jnp.int32, (128, 128), 1)
    row16 = lax.broadcasted_iota(jnp.int32, (16, 128), 0)
    lane16 = lax.broadcasted_iota(jnp.int32, (16, 128), 1)
    lane1 = lax.broadcasted_iota(jnp.int32, (1, 128), 1)

    def next_z(v, lane):
        return jnp.where(lane == 127, 0.0, pltpu.roll(v, 127, 1))

    def prev_z(v, lane):
        return jnp.where(lane == 0, 0.0, pltpu.roll(v, 1, 1))

    @pl.when(jnp.logical_not(has_xn))
    def _():
        xe_l[...] = jnp.zeros_like(xe_l)
        pk_l[2] = jnp.zeros_like(pk_l[2])

    @pl.when(jnp.logical_not(has_xp))
    def _():
        xh_l[...] = jnp.zeros_like(xh_l)
        pk_l[0] = jnp.zeros_like(pk_l[0])

    @pl.when(jnp.logical_not(has_yn))
    def _():
        ye_l[...] = jnp.zeros_like(ye_l)

    @pl.when(jnp.logical_not(has_yp))
    def _():
        yh_l[...] = jnp.zeros_like(yh_l)

    @pl.when(jnp.logical_not(jnp.logical_and(has_xn, has_yp)))
    def _():
        ce_l[...] = jnp.zeros_like(ce_l)

    picks = (
        (eb, 0, (110, 111, 112)), (eb, 1, (110, 111, 112)), (eb, 2, (110, 111)),
        (hb, 0, (110, 111)), (hb, 1, (110, 111)), (hb, 2, (111,)),
    )

    def pick(x, carry):
        at = 0
        for ref, which, planes in picks:
            v = ref[which, x]
            for z in planes:
                pp[at, pl.ds(x, 1), :] = plane_of(v, z)
                at += 1
        for ref in (rb, cb):
            pp[at, pl.ds(x, 1), :] = plane_of(ref[x], PLANE)
            at += 1
        return carry

    for at in range(4):
        for copy in chunks[at]:
            copy.wait()
        lax.fori_loop(4 * at, 4 * at + 4, pick, 0)
    tabs = [load(ty_hbm, ty), load(tw_hbm, tw), load(tt_hbm, tt), load(tg_hbm, tg)]

    ex0, ex1, ex2, ey0, ey1, ey2, ez0, ez1, hx0, hx1, hy0, hy1, hz1, r1, c1 = (pp[at] for at in range(15))

    def next_x(v):
        return jnp.where(row16 == 15, 0.0, pltpu.roll(v, 15, 0))

    def prev_x(v):
        return jnp.where(row16 == 0, 0.0, pltpu.roll(v, 1, 0))

    phx1 = hx1 - 0.5 * ((next_z(ez1, lane16) - ez1) - (ey2 - ey1))
    phx0 = hx0 - 0.5 * ((next_z(ez0, lane16) - ez0) - (ey1 - ey0))
    phy1 = hy1 - 0.5 * ((ex2 - ex1) - (next_x(ez1) - ez1))
    phy0 = hy0 - 0.5 * ((ex1 - ex0) - (next_x(ez0) - ez0))
    phz1 = hz1 - 0.5 * ((next_x(ey1) - ey1) - (next_z(ex1, lane16) - ex1))
    t_s[0, 0:16] = r1 * ex1 + c1 * ((phz1 - prev_z(phz1, lane16)) - (phy1 - phy0))
    t_s[1, 0:16] = r1 * ey1 + c1 * ((phx1 - phx0) - (phz1 - prev_x(phz1)))
    t_s[2, 0:16] = phx1
    t_s[3, 0:16] = phy1
    cols = jnp.zeros((16, 128), F32)
    for at, (v, y) in enumerate(((ex1, 0), (ez1, 0), (ez0, 0), (c1, 0), (phz1, 127), (c1, 127))):
        cols = jnp.where(lane16 == at, v[:, y : y + 1], cols)
    for g in range(GY):
        t_s[g, 16:32] = cols
    pk_s[0:1] = ey1[0:1]
    pk_s[1:2] = ez1[0:1]
    pk_s[2:3] = ez0[0:1]
    pk_s[3:4] = phz1[15:16]
    pk_s[4:5] = c1[0:1]
    pk_s[5:6] = c1[15:16]
    pk_s[6:7] = ex1[15:16]
    pk_s[7:8] = jnp.zeros((1, 128), F32)

    ye_s[0] = eb[0, :, 0, :]
    ye_s[1] = eb[2, :, 0, :]
    ex, ey, ez = eb[0, :, 127, :], eb[1, :, 127, :], eb[2, :, 127, :]
    yh_s[0] = hb[0, :, 127, :] - 0.5 * (-ez - (next_z(ey, lane16) - ey))
    ey_up = jnp.where(row16 == 15, 0.0, pltpu.roll(ey, 15, 0))
    yh_s[1] = hb[2, :, 127, :] - 0.5 * (ey_up - ey + ex)

    pk_l[1, Y] = pk_s[...]
    for copy in spec:
        copy.wait()
    al[0, Y] = srv[Y]
    al[1, Y] = siv[Y]
    t_l[Y] = t_s[Y]

    pl.semaphore_wait(barrier, greeted)

    def remote(src, dst, ss, rs, x, y):
        return pltpu.make_async_remote_copy(
            src_ref=src, dst_ref=dst, send_sem=ss, recv_sem=rs, device_id=(x, y), device_id_type=MESH
        )

    def pack(dx, d):
        return remote(
            pk_s, pk_l.at[2 - dx, Y], pk_ss.at[dx, d], pk_rs.at[2 - dx, Y], (xp, X, xn)[dx], lax.rem(Y + d, GY)
        )

    for dx, ok in ((0, has_xp), (2, has_xn)):
        for d in range(GY):
            pl.when(ok)(pack(dx, d).start)
    for d in range(1, GY):
        pack(1, d).start()

    def packs_sent():
        for dx, ok in ((0, has_xp), (2, has_xn)):
            for d in range(GY):
                pl.when(ok)(pack(dx, d).wait_send)
        for d in range(1, GY):
            pack(1, d).wait_send()

    pending.append(packs_sent)

    def tangent(d):
        g = lax.rem(Y + d, GY)
        return remote(t_s.at[g], t_l.at[Y], t_ss.at[d], t_rs.at[Y], X, g)

    for d in range(1, GY):
        tangent(d).start()
        pending.append(tangent(d).wait_send)

    def spectrum(part, d):
        g = lax.rem(Y + d, GY)
        return remote((srv, siv)[part].at[g], al.at[part, Y], a_ss.at[part, d], a_rs.at[part, Y], X, g)

    for d in range(1, GY):
        for part in range(2):
            spectrum(part, d).start()
            pending.append(spectrum(part, d).wait_send)

    ye = remote(ye_s, ye_l, yh_sem.at[0], yh_sem.at[1], X, yp)
    yh = remote(yh_s, yh_l, yh_sem.at[2], yh_sem.at[3], X, yn)
    pl.when(has_yp)(ye.start)
    pl.when(has_yn)(yh.start)
    pending.append(lambda: pl.when(has_yp)(ye.wait_send))
    pending.append(lambda: pl.when(has_yn)(yh.wait_send))

    corner = remote(eb.at[1, 0, pl.ds(120, 8)], ce_l, x_sem.at[0], x_sem.at[1], xp, yn)
    pl.when(jnp.logical_and(has_xp, has_yn))(corner.start)
    pending.append(lambda: pl.when(jnp.logical_and(has_xp, has_yn))(corner.wait_send))
    xe = remote(eb.at[pl.ds(1, 2), 0], xe_l, x_sem.at[2], x_sem.at[3], xp, Y)
    pl.when(has_xp)(xe.start)
    pending.append(lambda: pl.when(has_xp)(xe.wait_send))

    pl.when(has_yn)(ye.wait_recv)
    pl.when(has_yp)(yh.wait_recv)
    yh_l[0] = jnp.where(has_yp, yh_l[0] - 0.5 * ye_s[1], 0.0)
    yh_l[1] = jnp.where(has_yp, yh_l[1] + 0.5 * ye_s[0], 0.0)

    ex, ey, ez = eb[0, 15], eb[1, 15], eb[2, 15]
    exn = jnp.where(rows == 127, ye_l[0, 15:16, :], pltpu.roll(ex, 127, 0))
    xh_s[0] = hb[1, 15] - 0.5 * ((next_z(ex, lanes) - ex) + ez)
    xh_s[1] = hb[2, 15] - 0.5 * (-ey - (exn - ex))
    xh = remote(xh_s, xh_l, x_sem.at[4], x_sem.at[5], xn, Y)
    pl.when(has_xn)(xh.start)
    pending.append(lambda: pl.when(has_xn)(xh.wait_send))

    def from_gy(make, d):
        make(d).wait_recv()

    for d in range(1, GY):
        s = lax.rem(Y + d, GY)
        for part in range(2):
            remote(srv.at[0], al.at[part, s], a_ss.at[part, d], a_rs.at[part, s], X, s).wait_recv()
        remote(t_s.at[0], t_l.at[s], t_ss.at[d], t_rs.at[s], X, s).wait_recv()
    for copy in tabs:
        copy.wait()

    wave_cos, wave_sin = [wv[f : f + 1] for f in range(4)], [wv[f : f + 1] for f in range(4, 8)]
    total = None
    for s in range(GY):
        t, mine = t_l[s, 0:16], t_l[s, 16:32]
        if s < GY - 1:
            after = t_l[s + 1, 16:32]
            exn, ez1n, ez0n, c127 = after[:, 0:1], after[:, 1:2], after[:, 2:3], mine[:, 5:6]
            exn_p = prev_x(after)[:, 0:1]
            edge = jnp.where(
                Y == 0,
                0.5 * c127 * exn,
                jnp.where(Y == 1, -0.5 * c127 * ((ez1n - ez0n) + (exn - exn_p)), jnp.where(Y == 2, -0.5 * ez1n, 0.0)),
            )
            t = t + jnp.where(lane16 == 127, edge, 0.0)
        if s > 0:
            hzp0 = t_l[s - 1, 16:32][:, 4:5] + 0.5 * mine[:, 0:1]
            t = t + jnp.where(lane16 == 0, jnp.where(Y == 0, -mine[:, 3:4] * hzp0, 0.0), 0.0)
        re = jnp.concatenate([al[0, s, f] + t * wave_cos[f] for f in range(4)], axis=0)
        im = jnp.concatenate([al[1, s, f] - t * wave_sin[f] for f in range(4)], axis=0)
        data = jnp.concatenate(
            [jnp.concatenate([re, im], axis=0), jnp.concatenate([im, -re], axis=0)], axis=1
        )
        high, low = split(data)
        part = dot_nt(ty[0, s], high) + dot_nt(ty[0, s], low) + dot_nt(ty[1, s], high)
        total = part if total is None else total + part
    bs[...] = total.reshape(GX, 8, 128)

    for d in range(1, GY):
        s = lax.rem(Y + d, GY)
        remote(pk_s, pk_l.at[1, s], pk_ss.at[1, d], pk_rs.at[1, s], X, s).wait_recv()
    for s in range(GY):
        pl.when(has_xn)(remote(pk_s, pk_l.at[2, s], pk_ss.at[2, s], pk_rs.at[2, s], xn, Y).wait_recv)
        pl.when(has_xp)(remote(pk_s, pk_l.at[0, s], pk_ss.at[0, s], pk_rs.at[0, s], xp, Y).wait_recv)
    added = None
    none = jnp.zeros((1, 128), F32)
    for s in range(GY):
        nxt, own, prv = pk_l[2, s], pk_l[1, s], pk_l[0, s]
        dhz = -0.5 * nxt[0:1]
        before = -0.5 * pk_l[2, s - 1][0:1, 127:128] if s else jnp.zeros((1, 1), F32)
        dhz_p = jnp.where(lane1 == 0, before, pltpu.roll(dhz, 1, 1))
        dhy = 0.5 * nxt[1:2]
        dhyd = dhy - 0.5 * nxt[2:3]
        after = 0.5 * pk_l[0, s + 1][6:7, 0:1] if s < GY - 1 else jnp.zeros((1, 1), F32)
        hzp = prv[3:4] - 0.5 * own[0:1] + jnp.where(lane1 == 127, after, 0.0)
        last = jnp.where(
            Y == 0, own[5:6] * (dhz - dhz_p - dhyd), jnp.where(Y == 1, -own[5:6] * dhz, jnp.where(Y == 3, dhy, 0.0))
        )
        head = jnp.where(jnp.logical_and(Y == 1, has_xp), own[4:5] * hzp, 0.0)
        pair = [
            jnp.where(row8 == 0, last, 0.0) + jnp.where(row8 == 1, head, 0.0),
            jnp.where(row8 == 2, last, 0.0) + jnp.where(row8 == 3, head, 0.0),
        ]
        high, low = split(jnp.concatenate(pair, axis=1))
        rhs = jnp.concatenate([high, low], axis=0)
        part = dot_nt(ty[0, s], rhs) + dot_nt(ty[1, s], rhs)
        added = part if added is None else added + part
    added = added[:, 0:8] + added[:, 8:16]
    wc, ws = none, none
    for f in range(4):
        wc = jnp.where((lane1 // 16) % 4 == f, wave_cos[f], wc)
        ws = jnp.where((lane1 // 16) % 4 == f, wave_sin[f], ws)
    by_cos, by_sin = jnp.where(lane1 < 64, wc, -ws), jnp.where(lane1 < 64, -ws, -wc)
    is_last, is_head = lane1 % 16 == 15, lane1 % 16 == 0
    extra = added[:, 0:1] * jnp.where(is_last, by_cos, 0.0) + added[:, 1:2] * jnp.where(is_head, by_cos, 0.0)
    extra = extra + added[:, 2:3] * jnp.where(is_last, by_sin, 0.0) + added[:, 3:4] * jnp.where(is_head, by_sin, 0.0)
    bs[...] = bs[...] + extra.reshape(GX, 8, 128)

    x_hi, row_in = (X // 4) & 1, (X // 8) * 4 + (X & 3)

    def column(at):
        to = block_at(offsets[at])
        return remote(bs.at[to], bl.at[x_hi, row_in], b_ss.at[at], b_rs.at[x_hi, row_in], to, Y)

    for at in range(GX - 1):
        column(at).start()
        pending.append(column(at).wait_send)
    bl[x_hi, row_in] = bs[X]

    def row(x, edge_first, edge_last):
        ex, ey, ez = eb[0, x], eb[1, x], eb[2, x]
        exn = jnp.where(rows == 127, ye_l[0, pl.ds(x, 1), :], pltpu.roll(ex, 127, 0))
        ezn = jnp.where(rows == 127, ye_l[1, pl.ds(x, 1), :], pltpu.roll(ez, 127, 0))
        if edge_last:
            ey_x, ez_x = -ey, -ez
        else:
            ey_x, ez_x = eb[1, x + 1] - ey, eb[2, x + 1] - ez
        hx = hb[0, x] - 0.5 * ((ezn - ez) - (next_z(ey, lanes) - ey))
        hy = hb[1, x] - 0.5 * ((next_z(ex, lanes) - ex) - ez_x)
        hz = hb[2, x] - 0.5 * (ey_x - (exn - ex))
        ho[0, x] = hx
        ho[1, x] = hy
        ho[2, x] = hz
        hxp = jnp.where(rows == 0, yh_l[0, pl.ds(x, 1), :], pltpu.roll(hx, 1, 0))
        hzp = jnp.where(rows == 0, yh_l[1, pl.ds(x, 1), :], pltpu.roll(hz, 1, 0))
        if edge_first:
            hy_x, hz_x = hy, hz
        else:
            hy_x, hz_x = hy - ho[1, x - 1], hz - ho[2, x - 1]
        r, c = rb[x], cb[x]
        nx = r * ex + c * ((hz - hzp) - (hy - prev_z(hy, lanes)))
        ny = r * ey + c * ((hx - prev_z(hx, lanes)) - hz_x)
        nz = r * ez + c * (hy_x - (hx - hxp))
        eo[0, x] = nx
        eo[1, x] = ny
        eo[2, x] = nz
    row(0, True, False)

    def inner(x, carry):
        row(x, False, False)
        return carry

    lax.fori_loop(1, 15, inner, 0)
    row(15, False, True)

    pl.when(has_xn)(xe.wait_recv)
    pl.when(has_xp)(xh.wait_recv)
    pl.when(jnp.logical_and(has_xn, has_yp))(corner.wait_recv)
    dhy, dhz = 0.5 * xe_l[1], -0.5 * xe_l[0]
    ho[1, 15] = ho[1, 15] + dhy
    ho[2, 15] = ho[2, 15] + dhz
    dhz_p = jnp.where(rows == 0, -0.5 * ce_l[7:8], pltpu.roll(dhz, 1, 0))
    c = cb[15]
    eo[0, 15] = eo[0, 15] + c * ((dhz - dhz_p) - (dhy - prev_z(dhy, lanes)))
    eo[1, 15] = eo[1, 15] - c * dhz
    eo[2, 15] = eo[2, 15] + c * dhy
    hyp = jnp.where(has_xp, xh_l[0] + 0.5 * eb[2, 0], 0.0)
    hzp = jnp.where(has_xp, xh_l[1] - 0.5 * eb[1, 0], 0.0)
    c = cb[0]
    eo[1, 0] = eo[1, 0] + c * hzp
    eo[2, 0] = eo[2, 0] - c * hyp
    def b_wait(o):
        src = block_at(o)
        at = ((src // 4) & 1, (src // 8) * 4 + (src & 3))
        remote(bs.at[src], bl.at[at], b_ss.at[0], b_rs.at[at], src, Y).wait_recv()

    sign = jnp.where(lax.broadcasted_iota(jnp.int32, (128, 128), 1) < 64, 1.0, -1.0)
    y = None
    for half in range(2):
        for o in offsets[:-1]:
            if o[1] == half:
                b_wait(o)
        which = (x_hi + half) & 1
        block = bl[which].reshape(128, 128)
        high, low = split(jnp.concatenate([block, pltpu.roll(block, 64, 1) * sign], axis=0))
        part = dot_nn(tw[0, which], high) + dot_nn(tw[0, which], low) + dot_nn(tw[1, which], high)
        y = part if y is None else y + part
    y = y * tt[0] + pltpu.roll(y, 64, 1) * tt[1]
    y_sw = pltpu.roll(y, 64, 1) * jnp.concatenate([sign, sign], axis=0)
    pieces = []
    for b in range(4):
        pieces += [y[64 * b : 64 * b + 64], y_sw[64 * b : 64 * b + 64]]
    high, low = split(jnp.concatenate(pieces, axis=0))
    out = dot_nt(tg[0], high) + dot_nt(tg[0], low) + dot_nt(tg[1], high)
    for a in range(8):
        for b in range(4):
            cs[4 * a + b] = out[4 * a : 4 * a + 4, 128 * b : 128 * b + 128]

    def finished(at):
        to = block_at(offsets[at])
        return remote(cs.at[to], cl.at[Y, slot], c_ss.at[at], c_rs.at[Y, slot], to, home)

    for at in range(GX - 1):
        finished(at).start()
        pending.append(finished(at).wait_send)
    pl.when(home != Y)(finished(GX - 1).start)
    pending.append(lambda: pl.when(home != Y)(finished(GX - 1).wait_send))

    @pl.when(home == Y)
    def _():
        cl[Y, slot] = cs[X]

    def own_plane(x, carry):
        for at, v in enumerate((eo[0, x], eo[1, x], ho[0, x], ho[1, x])):
            pp[at, pl.ds(x, 1), :] = plane_of(v, PLANE)
        return carry

    lax.fori_loop(0, 16, own_plane, 0)
    for at in range(4):
        t = pp[at]
        for f in range(4):
            nr[at, f] = srv[at, f] + t * wave_cos[f]
            ni[at, f] = siv[at, f] - t * wave_sin[f]

    def c_wait(i, carry):
        g, q = i // 8, lax.rem(i, 8)
        src = 8 * Y + q

        @pl.when(jnp.logical_or(g != Y, src != X))
        def _():
            remote(cs.at[0], cl.at[g, q], c_ss.at[0], c_rs.at[g, q], src, g).wait_recv()

        return carry

    lax.fori_loop(0, 32, c_wait, 0)

    for q in range(8):
        for g in range(4):
            rel[q, 4 * g : 4 * g + 4, :] = cl[g, q]
    for wait in pending:
        wait()


def flush_kernel(eo, ho, nr, ni, rel, e_out, h_out, r_out, i_out, f_out, zz, fv, sem):
    copies = []
    for i in range(3):
        for x in range(0, 16, 4):
            part = (i, pl.ds(x, 4))
            copies += [(eo.at[part], e_out.at[part]), (ho.at[part], h_out.at[part])]
    copies += [(nr, r_out), (ni, i_out)]
    copies = [pltpu.make_async_copy(src, dst, sem.at[at]) for at, (src, dst) in enumerate(copies)]
    for copy in copies:
        copy.start()
    lane16 = lax.broadcasted_iota(jnp.int32, (16, 128), 1)
    turned = [pltpu.roll(rel[q], 8 * q, 1) if q else rel[q] for q in range(8)]
    group = lane16 // 8
    for s in range(16):
        acc = turned[0]
        for q in range(1, 8):
            acc = jnp.where(group == (q + s) % 16, turned[q], acc)
        if s:
            acc = pltpu.roll(acc, 128 - 8 * s, 1)
        zz[:, s, :] = acc
    for g in range(4):
        for f in range(4):
            fv[0, g, f] = zz[4 * g + f, 0:8, 0:64]
            fv[1, g, f] = zz[4 * g + f, 8:16, 0:64]
    copies.append(pltpu.make_async_copy(fv, f_out, sem.at[26]))
    copies[-1].start()
    for copy in copies:
        copy.wait()


def per_device(electric, magnetic, retention, coupling, spectrum_real, spectrum_imag, phases):
    tab_y, tab_w, tab_t, tab_g = (jnp.asarray(t) for t in tables())
    vmem, dma = pltpu.VMEM, pltpu.SemaphoreType.DMA
    hbm = pl.BlockSpec(memory_space=pltpu.HBM)
    in_vmem = pl.BlockSpec(memory_space=pltpu.VMEM)
    shapes = [
        jax.ShapeDtypeStruct(electric.shape, F32),
        jax.ShapeDtypeStruct(magnetic.shape, F32),
        jax.ShapeDtypeStruct(spectrum_real.shape, F32),
        jax.ShapeDtypeStruct(spectrum_imag.shape, F32),
        jax.ShapeDtypeStruct((2, 4, 4, 8, 64), F32),
    ]
    fixed = [
        pltpu.with_memory_space_constraint(a, pltpu.HBM)
        for a in (electric, magnetic, retention, coupling, spectrum_real, spectrum_imag, tab_y, tab_w, tab_t, tab_g)
    ]
    held = pl.pallas_call(
        step_kernel,
        out_shape=shapes[:4] + [jax.ShapeDtypeStruct((8, 16, 128), F32)],
        in_specs=[hbm] * 11,
        out_specs=[in_vmem] * 5,
        scratch_shapes=[
            vmem(electric.shape, F32), vmem(magnetic.shape, F32), vmem(retention.shape, F32), vmem(coupling.shape, F32),
            vmem(spectrum_real.shape, F32), vmem(spectrum_imag.shape, F32),
            vmem(tab_y.shape, BF16), vmem(tab_w.shape, BF16), vmem(tab_t.shape, F32), vmem(tab_g.shape, BF16),
            vmem((2, 16, 128), F32), vmem((2, 16, 128), F32), vmem((2, 16, 128), F32), vmem((2, 16, 128), F32),
            vmem((2, 128, 128), F32), vmem((2, 128, 128), F32), vmem((8, 128), F32),
            vmem((8, 128), F32), vmem((3, 4, 8, 128), F32),
            vmem((4, 32, 128), F32), vmem((4, 32, 128), F32), vmem((2, 4, 4, 16, 128), F32),
            vmem((32, 8, 128), F32), vmem((2, 16, 8, 128), F32), vmem((32, 4, 128), F32), vmem((4, 8, 4, 128), F32),
            vmem((2, 128, 128), F32), vmem((15, 16, 128), F32), vmem((8, 128), F32), pltpu.SMEM((4,), F32),
            dma((22,)), dma((4,)), dma((3, 4)), dma((3, 4)), dma((2, 4)), dma((2, 4)), dma((4,)), dma((4,)), dma((6,)),
            dma((32,)), dma((2, 16)), dma((32,)), dma((4, 8)), dma,
        ],
        compiler_params=pltpu.CompilerParams(collective_id=0, has_side_effects=True, vmem_limit_bytes=40 * 2**20),
    )(*fixed[:6], pltpu.with_memory_space_constraint(phases, pltpu.HBM), *fixed[6:])
    return pl.pallas_call(
        flush_kernel,
        out_shape=shapes,
        in_specs=[in_vmem] * 5,
        out_specs=[hbm] * 5,
        scratch_shapes=[vmem((16, 16, 128), F32), vmem((2, 4, 4, 8, 64), F32), dma((27,))],
        compiler_params=pltpu.CompilerParams(vmem_limit_bytes=16 * 2**20),
    )(*held)


def solution(mesh):
    placed = (
        P(None, "gx", "gy", None),
        P(None, "gx", "gy", None),
        P("gx", "gy", None),
        P("gx", "gy", None),
        P(None, None, "gx", "gy"),
        P(None, None, "gx", "gy"),
        P(),
    )
    return jax.shard_map(
        per_device,
        mesh=mesh,
        in_specs=placed,
        out_specs=(
            P(None, "gx", "gy", None),
            P(None, "gx", "gy", None),
            P(None, None, "gx", "gy"),
            P(None, None, "gx", "gy"),
            P(None, None, None, "gx", "gy"),
        ),
        check_vma=False,
    )
```

```python
import functools
import itertools
import math

import jax
import jax.numpy as jnp
import numpy as np
from jax import lax
from jax.experimental import pallas as pl
from jax.experimental.pallas import tpu as pltpu
from jax.sharding import PartitionSpec as P

MESH = pl.DeviceIdType.MESH
WAVES = 256
PLANE = 111
GX, GY = 32, 4
F32, BF16 = jnp.float32, jnp.bfloat16


def split_np(table):
    high = table.astype(np.float32).astype(jnp.bfloat16)
    low = (table - high.astype(np.float64)).astype(np.float32).astype(jnp.bfloat16)
    return np.stack([high, low])


def angle_np(wave, place):
    return (np.multiply.outer(wave, place) % 1024) * (math.pi / 512)


@functools.cache
def tables():
    wave = 2 * np.arange(WAVES) - 255
    ang = angle_np(wave, np.arange(512)).reshape(256, 4, 128).transpose(1, 0, 2)
    tab_y = split_np(np.concatenate([np.cos(ang), np.sin(ang)], axis=2))
    ang = angle_np(2 * np.arange(32) - 255, 16 * np.arange(32))
    eye = np.eye(8)
    ang = ang.reshape(32, 4, 2, 4).transpose(2, 0, 1, 3).reshape(2, 32, 16)
    tab_w = np.stack([np.concatenate([np.kron(np.cos(a), eye), np.kron(np.sin(a), eye)], axis=1) for a in ang])
    tab_w = split_np(tab_w)
    ang = np.repeat(angle_np(2 * np.arange(32) - 255, np.arange(16)), 8, axis=0)
    cos, sin = np.tile(np.cos(ang), (1, 8)), np.tile(np.sin(ang), (1, 8))
    sin[:, 64:] *= -1
    tab_t = np.stack([cos, sin]).astype(np.float32)
    ang = 2 * math.pi * (np.multiply.outer(np.arange(8), np.arange(16)) % 16) / 16
    eye = np.eye(4)
    blocks = [np.einsum("ai,fg->afgi", t, eye).reshape(32, 64) for t in (np.cos(ang), np.sin(ang))]
    tab_g = split_np(np.concatenate(blocks, axis=1) / 512.0)
    return tab_y, tab_w, tab_t, tab_g


def hops(o):
    return min(o[0], 4 - o[0]) + 2 * o[1] + min(o[2], 4 - o[2])


def split(value):
    high = value.astype(BF16)
    return high, (value - high.astype(F32)).astype(BF16)


def dot_nt(a, b):
    return lax.dot_general(a, b, (((1,), (1,)), ((), ())), preferred_element_type=F32)


def dot_nn(a, b):
    return lax.dot_general(a, b, (((1,), (0,)), ((), ())), preferred_element_type=F32)


def plane_of(value, at):
    wide = jnp.broadcast_to(value[:, at : at + 1], (128, 128))
    rows = lax.broadcasted_iota(jnp.int32, (128, 128), 0)
    lanes = lax.broadcasted_iota(jnp.int32, (128, 128), 1)
    return jnp.sum(jnp.where(rows == lanes, wide, 0.0), axis=0, keepdims=True)


def step_kernel(
    e_hbm, h_hbm, r_hbm, c_hbm, sr_hbm, si_hbm, ph_hbm, ty_hbm, tw_hbm, tt_hbm, tg_hbm,
    eo, ho, nr, ni, rel,
    eb, hb, rb, cb, srv, siv, ty, tw, tt, tg,
    ye_s, yh_s, ye_l, yh_l, xe_l, xh_l, ce_l, pk_s, pk_l, t_s, t_l, al,
    bs, bl, cs, cl, xh_s, pp, wv, ph_ref, gm, gt,
    ld_sem, yh_sem, pk_ss, pk_rs, a_ss, a_rs, t_ss, t_rs, x_sem, b_ss, b_rs, c_ss, c_rs, ph_sem,
):
    X = lax.axis_index("gx")
    Y = lax.axis_index("gy")
    xn, xp = lax.rem(X + 1, GX), lax.rem(X + GX - 1, GX)
    yn, yp = lax.rem(Y + 1, GY), lax.rem(Y + GY - 1, GY)
    has_xn, has_xp, has_yn, has_yp = X < GX - 1, X > 0, Y < GY - 1, Y > 0

    pending = []
    barrier = pltpu.get_barrier_semaphore()
    home, slot = X // 8, lax.rem(X, 8)
    offsets = sorted(itertools.product(range(4), range(2), range(4)), key=lambda o: (-hops(o), o))
    at_y = [((X // 8 + a) & 3) * 8 for a in range(4)]
    at_x = [((X // 4 + b) & 1) * 4 for b in range(2)]
    at_z = [(X + c) & 3 for c in range(4)]

    def block_at(o):
        return at_y[o[0]] + at_x[o[1]] + at_z[o[2]]

    def greet(x, y):
        pl.semaphore_signal(barrier, inc=1, device_id=(x, y), device_id_type=MESH)

    others = [lax.rem(Y + d, GY) for d in range(1, GY)]
    for o in offsets[:-1]:
        greet(block_at(o), Y)
    for x in (xp, xn, X):
        for y in others:
            greet(x, y)
    for o in sorted(itertools.product(range(2), range(4)), key=lambda o: (-hops((0,) + o), o)):
        for y in others:
            greet(8 * Y + at_x[o[0]] + at_z[o[1]], y)
    greeted = 3 * (GY - 1) + (GX - 1) + jnp.where(home != Y, GX, 0)

    loads = []

    def load(src, dst):
        copy = pltpu.make_async_copy(src, dst, ld_sem.at[len(loads)])
        copy.start()
        loads.append(copy)
        return copy

    phase = pltpu.make_async_copy(ph_hbm, ph_ref, ph_sem)
    phase.start()
    chunks = []
    for at in range(4):
        part = pl.ds(4 * at, 4)
        chunks.append(
            [
                load(e_hbm.at[:, part], eb.at[:, part]),
                load(h_hbm.at[:, part], hb.at[:, part]),
                load(c_hbm.at[part], cb.at[part]),
                load(r_hbm.at[part], rb.at[part]),
            ]
        )
    spec = [load(sr_hbm, srv), load(si_hbm, siv)]
    phase.wait()
    row8 = lax.broadcasted_iota(jnp.int32, (8, 128), 0)
    angle = jnp.zeros((8, 128), F32)
    for f in range(4):
        angle = jnp.where(lax.rem(row8, 4) == f, ph_ref[f], angle)
    wv[...] = jnp.where(row8 < 4, jnp.cos(angle), jnp.sin(angle))

    rows = lax.broadcasted_iota(jnp.int32, (128, 128), 0)
    lanes = lax.broadcasted_iota(jnp.int32, (128, 128), 1)
    row16 = lax.broadcasted_iota(jnp.int32, (16, 128), 0)
    lane16 = lax.broadcasted_iota(jnp.int32, (16, 128), 1)
    lane1 = lax.broadcasted_iota(jnp.int32, (1, 128), 1)

    def next_z(v, lane):
        return jnp.where(lane == 127, 0.0, pltpu.roll(v, 127, 1))

    def prev_z(v, lane):
        return jnp.where(lane == 0, 0.0, pltpu.roll(v, 1, 1))

    @pl.when(jnp.logical_not(has_xn))
    def _():
        xe_l[...] = jnp.zeros_like(xe_l)
        pk_l[2] = jnp.zeros_like(pk_l[2])

    @pl.when(jnp.logical_not(has_xp))
    def _():
        xh_l[...] = jnp.zeros_like(xh_l)
        pk_l[0] = jnp.zeros_like(pk_l[0])

    @pl.when(jnp.logical_not(has_yn))
    def _():
        ye_l[...] = jnp.zeros_like(ye_l)

    @pl.when(jnp.logical_not(has_yp))
    def _():
        yh_l[...] = jnp.zeros_like(yh_l)

    @pl.when(jnp.logical_not(jnp.logical_and(has_xn, has_yp)))
    def _():
        ce_l[...] = jnp.zeros_like(ce_l)

    fields = [(eb, 0), (eb, 1), (eb, 2), (hb, 0), (hb, 1), (hb, 2), (rb, None), (cb, None)]
    wanted = [(0, 0), (0, 1), (0, 2), (1, 0), (1, 1), (1, 2), (2, 0), (2, 1), (3, 0), (3, 1), (4, 0), (4, 1), (5, 1), (6, 1), (7, 1)]
    lane32 = lax.broadcasted_iota(jnp.int32, (32, 128), 1)
    window = jnp.logical_and(lane32 >= PLANE - 1, lane32 < PLANE + 3)

    for at in range(4):
        for copy in chunks[at]:
            copy.wait()

        def gather(block, carry, at=at):
            ys = pl.ds(pl.multiple_of(block * 32, 32), 32)
            total = None
            for which, (ref, comp) in enumerate(fields):
                for x in range(4):
                    v = ref[4 * at + x, ys, :] if comp is None else ref[comp, 4 * at + x, ys, :]
                    v = jnp.where(window, v, 0.0)
                    shift = (4 * (4 * which + x) - (PLANE - 1)) % 128
                    v = pltpu.roll(v, shift, 1) if shift else v
                    total = v if total is None else total + v
            gm[ys, :] = total
            return carry

        lax.fori_loop(0, 4, gather, 0)
        gt[...] = gm[...].T
        for to, (which, z) in enumerate(wanted):
            pp[to, 4 * at : 4 * at + 4, :] = gt[pl.ds(16 * which + z, 4, stride=4), :]
    tabs = [load(ty_hbm, ty), load(tw_hbm, tw), load(tt_hbm, tt), load(tg_hbm, tg)]

    ex0, ex1, ex2, ey0, ey1, ey2, ez0, ez1, hx0, hx1, hy0, hy1, hz1, r1, c1 = (pp[at] for at in range(15))

    def next_x(v):
        return jnp.where(row16 == 15, 0.0, pltpu.roll(v, 15, 0))

    def prev_x(v):
        return jnp.where(row16 == 0, 0.0, pltpu.roll(v, 1, 0))

    phx1 = hx1 - 0.5 * ((next_z(ez1, lane16) - ez1) - (ey2 - ey1))
    phx0 = hx0 - 0.5 * ((next_z(ez0, lane16) - ez0) - (ey1 - ey0))
    phy1 = hy1 - 0.5 * ((ex2 - ex1) - (next_x(ez1) - ez1))
    phy0 = hy0 - 0.5 * ((ex1 - ex0) - (next_x(ez0) - ez0))
    phz1 = hz1 - 0.5 * ((next_x(ey1) - ey1) - (next_z(ex1, lane16) - ex1))
    t_s[0, 0:16] = r1 * ex1 + c1 * ((phz1 - prev_z(phz1, lane16)) - (phy1 - phy0))
    t_s[1, 0:16] = r1 * ey1 + c1 * ((phx1 - phx0) - (phz1 - prev_x(phz1)))
    t_s[2, 0:16] = phx1
    t_s[3, 0:16] = phy1
    cols = jnp.zeros((16, 128), F32)
    for at, (v, y) in enumerate(((ex1, 0), (ez1, 0), (ez0, 0), (c1, 0), (phz1, 127), (c1, 127))):
        cols = jnp.where(lane16 == at, v[:, y : y + 1], cols)
    for g in range(GY):
        t_s[g, 16:32] = cols
    pk_s[0:1] = ey1[0:1]
    pk_s[1:2] = ez1[0:1]
    pk_s[2:3] = ez0[0:1]
    pk_s[3:4] = phz1[15:16]
    pk_s[4:5] = c1[0:1]
    pk_s[5:6] = c1[15:16]
    pk_s[6:7] = ex1[15:16]
    pk_s[7:8] = jnp.zeros((1, 128), F32)

    ye_s[0] = eb[0, :, 0, :]
    ye_s[1] = eb[2, :, 0, :]
    ex, ey, ez = eb[0, :, 127, :], eb[1, :, 127, :], eb[2, :, 127, :]
    yh_s[0] = hb[0, :, 127, :] - 0.5 * (-ez - (next_z(ey, lane16) - ey))
    ey_up = jnp.where(row16 == 15, 0.0, pltpu.roll(ey, 15, 0))
    yh_s[1] = hb[2, :, 127, :] - 0.5 * (ey_up - ey + ex)

    pk_l[1, Y] = pk_s[...]
    for copy in spec:
        copy.wait()
    al[0, Y] = srv[Y]
    al[1, Y] = siv[Y]
    t_l[Y] = t_s[Y]

    pl.semaphore_wait(barrier, greeted)

    def remote(src, dst, ss, rs, x, y):
        return pltpu.make_async_remote_copy(
            src_ref=src, dst_ref=dst, send_sem=ss, recv_sem=rs, device_id=(x, y), device_id_type=MESH
        )

    def pack(dx, d):
        return remote(
            pk_s, pk_l.at[2 - dx, Y], pk_ss.at[dx, d], pk_rs.at[2 - dx, Y], (xp, X, xn)[dx], lax.rem(Y + d, GY)
        )

    for dx, ok in ((0, has_xp), (2, has_xn)):
        for d in range(GY):
            pl.when(ok)(pack(dx, d).start)
    for d in range(1, GY):
        pack(1, d).start()

    def packs_sent():
        for dx, ok in ((0, has_xp), (2, has_xn)):
            for d in range(GY):
                pl.when(ok)(pack(dx, d).wait_send)
        for d in range(1, GY):
            pack(1, d).wait_send()

    pending.append(packs_sent)

    def tangent(d):
        g = lax.rem(Y + d, GY)
        return remote(t_s.at[g], t_l.at[Y], t_ss.at[d], t_rs.at[Y], X, g)

    for d in range(1, GY):
        tangent(d).start()
        pending.append(tangent(d).wait_send)

    def spectrum(part, d):
        g = lax.rem(Y + d, GY)
        return remote((srv, siv)[part].at[g], al.at[part, Y], a_ss.at[part, d], a_rs.at[part, Y], X, g)

    for d in range(1, GY):
        for part in range(2):
            spectrum(part, d).start()
            pending.append(spectrum(part, d).wait_send)

    ye = remote(ye_s, ye_l, yh_sem.at[0], yh_sem.at[1], X, yp)
    yh = remote(yh_s, yh_l, yh_sem.at[2], yh_sem.at[3], X, yn)
    pl.when(has_yp)(ye.start)
    pl.when(has_yn)(yh.start)
    pending.append(lambda: pl.when(has_yp)(ye.wait_send))
    pending.append(lambda: pl.when(has_yn)(yh.wait_send))

    corner = remote(eb.at[1, 0, pl.ds(120, 8)], ce_l, x_sem.at[0], x_sem.at[1], xp, yn)
    pl.when(jnp.logical_and(has_xp, has_yn))(corner.start)
    pending.append(lambda: pl.when(jnp.logical_and(has_xp, has_yn))(corner.wait_send))
    xe = remote(eb.at[pl.ds(1, 2), 0], xe_l, x_sem.at[2], x_sem.at[3], xp, Y)
    pl.when(has_xp)(xe.start)
    pending.append(lambda: pl.when(has_xp)(xe.wait_send))

    pl.when(has_yn)(ye.wait_recv)
    pl.when(has_yp)(yh.wait_recv)
    yh_l[0] = jnp.where(has_yp, yh_l[0] - 0.5 * ye_s[1], 0.0)
    yh_l[1] = jnp.where(has_yp, yh_l[1] + 0.5 * ye_s[0], 0.0)

    ex, ey, ez = eb[0, 15], eb[1, 15], eb[2, 15]
    exn = jnp.where(rows == 127, ye_l[0, 15:16, :], pltpu.roll(ex, 127, 0))
    xh_s[0] = hb[1, 15] - 0.5 * ((next_z(ex, lanes) - ex) + ez)
    xh_s[1] = hb[2, 15] - 0.5 * (-ey - (exn - ex))
    xh = remote(xh_s, xh_l, x_sem.at[4], x_sem.at[5], xn, Y)
    pl.when(has_xn)(xh.start)
    pending.append(lambda: pl.when(has_xn)(xh.wait_send))

    def from_gy(make, d):
        make(d).wait_recv()

    for d in range(1, GY):
        s = lax.rem(Y + d, GY)
        for part in range(2):
            remote(srv.at[0], al.at[part, s], a_ss.at[part, d], a_rs.at[part, s], X, s).wait_recv()
        remote(t_s.at[0], t_l.at[s], t_ss.at[d], t_rs.at[s], X, s).wait_recv()
    for copy in tabs:
        copy.wait()

    wave_cos, wave_sin = [wv[f : f + 1] for f in range(4)], [wv[f : f + 1] for f in range(4, 8)]
    total = None
    for s in range(GY):
        t, mine = t_l[s, 0:16], t_l[s, 16:32]
        if s < GY - 1:
            after = t_l[s + 1, 16:32]
            exn, ez1n, ez0n, c127 = after[:, 0:1], after[:, 1:2], after[:, 2:3], mine[:, 5:6]
            exn_p = prev_x(after)[:, 0:1]
            edge = jnp.where(
                Y == 0,
                0.5 * c127 * exn,
                jnp.where(Y == 1, -0.5 * c127 * ((ez1n - ez0n) + (exn - exn_p)), jnp.where(Y == 2, -0.5 * ez1n, 0.0)),
            )
            t = t + jnp.where(lane16 == 127, edge, 0.0)
        if s > 0:
            hzp0 = t_l[s - 1, 16:32][:, 4:5] + 0.5 * mine[:, 0:1]
            t = t + jnp.where(lane16 == 0, jnp.where(Y == 0, -mine[:, 3:4] * hzp0, 0.0), 0.0)
        re = jnp.concatenate([al[0, s, f] + t * wave_cos[f] for f in range(4)], axis=0)
        im = jnp.concatenate([al[1, s, f] - t * wave_sin[f] for f in range(4)], axis=0)
        data = jnp.concatenate(
            [jnp.concatenate([re, im], axis=0), jnp.concatenate([im, -re], axis=0)], axis=1
        )
        high, low = split(data)
        part = dot_nt(ty[0, s], high) + dot_nt(ty[0, s], low) + dot_nt(ty[1, s], high)
        total = part if total is None else total + part
    bs[...] = total.reshape(GX, 8, 128)

    for d in range(1, GY):
        s = lax.rem(Y + d, GY)
        remote(pk_s, pk_l.at[1, s], pk_ss.at[1, d], pk_rs.at[1, s], X, s).wait_recv()
    for s in range(GY):
        pl.when(has_xn)(remote(pk_s, pk_l.at[2, s], pk_ss.at[2, s], pk_rs.at[2, s], xn, Y).wait_recv)
        pl.when(has_xp)(remote(pk_s, pk_l.at[0, s], pk_ss.at[0, s], pk_rs.at[0, s], xp, Y).wait_recv)
    added = None
    none = jnp.zeros((1, 128), F32)
    for s in range(GY):
        nxt, own, prv = pk_l[2, s], pk_l[1, s], pk_l[0, s]
        dhz = -0.5 * nxt[0:1]
        before = -0.5 * pk_l[2, s - 1][0:1, 127:128] if s else jnp.zeros((1, 1), F32)
        dhz_p = jnp.where(lane1 == 0, before, pltpu.roll(dhz, 1, 1))
        dhy = 0.5 * nxt[1:2]
        dhyd = dhy - 0.5 * nxt[2:3]
        after = 0.5 * pk_l[0, s + 1][6:7, 0:1] if s < GY - 1 else jnp.zeros((1, 1), F32)
        hzp = prv[3:4] - 0.5 * own[0:1] + jnp.where(lane1 == 127, after, 0.0)
        last = jnp.where(
            Y == 0, own[5:6] * (dhz - dhz_p - dhyd), jnp.where(Y == 1, -own[5:6] * dhz, jnp.where(Y == 3, dhy, 0.0))
        )
        head = jnp.where(jnp.logical_and(Y == 1, has_xp), own[4:5] * hzp, 0.0)
        pair = [
            jnp.where(row8 == 0, last, 0.0) + jnp.where(row8 == 1, head, 0.0),
            jnp.where(row8 == 2, last, 0.0) + jnp.where(row8 == 3, head, 0.0),
        ]
        high, low = split(jnp.concatenate(pair, axis=1))
        rhs = jnp.concatenate([high, low], axis=0)
        part = dot_nt(ty[0, s], rhs) + dot_nt(ty[1, s], rhs)
        added = part if added is None else added + part
    added = added[:, 0:8] + added[:, 8:16]
    wc, ws = none, none
    for f in range(4):
        wc = jnp.where((lane1 // 16) % 4 == f, wave_cos[f], wc)
        ws = jnp.where((lane1 // 16) % 4 == f, wave_sin[f], ws)
    by_cos, by_sin = jnp.where(lane1 < 64, wc, -ws), jnp.where(lane1 < 64, -ws, -wc)
    is_last, is_head = lane1 % 16 == 15, lane1 % 16 == 0
    extra = added[:, 0:1] * jnp.where(is_last, by_cos, 0.0) + added[:, 1:2] * jnp.where(is_head, by_cos, 0.0)
    extra = extra + added[:, 2:3] * jnp.where(is_last, by_sin, 0.0) + added[:, 3:4] * jnp.where(is_head, by_sin, 0.0)
    bs[...] = bs[...] + extra.reshape(GX, 8, 128)

    x_hi, row_in = (X // 4) & 1, (X // 8) * 4 + (X & 3)

    def column(at):
        to = block_at(offsets[at])
        return remote(bs.at[to], bl.at[x_hi, row_in], b_ss.at[at], b_rs.at[x_hi, row_in], to, Y)

    for at in range(GX - 1):
        column(at).start()
        pending.append(column(at).wait_send)
    bl[x_hi, row_in] = bs[X]

    def row(x, edge_first, edge_last):
        ex, ey, ez = eb[0, x], eb[1, x], eb[2, x]
        exn = jnp.where(rows == 127, ye_l[0, pl.ds(x, 1), :], pltpu.roll(ex, 127, 0))
        ezn = jnp.where(rows == 127, ye_l[1, pl.ds(x, 1), :], pltpu.roll(ez, 127, 0))
        if edge_last:
            ey_x, ez_x = -ey, -ez
        else:
            ey_x, ez_x = eb[1, x + 1] - ey, eb[2, x + 1] - ez
        hx = hb[0, x] - 0.5 * ((ezn - ez) - (next_z(ey, lanes) - ey))
        hy = hb[1, x] - 0.5 * ((next_z(ex, lanes) - ex) - ez_x)
        hz = hb[2, x] - 0.5 * (ey_x - (exn - ex))
        ho[0, x] = hx
        ho[1, x] = hy
        ho[2, x] = hz
        hxp = jnp.where(rows == 0, yh_l[0, pl.ds(x, 1), :], pltpu.roll(hx, 1, 0))
        hzp = jnp.where(rows == 0, yh_l[1, pl.ds(x, 1), :], pltpu.roll(hz, 1, 0))
        if edge_first:
            hy_x, hz_x = hy, hz
        else:
            hy_x, hz_x = hy - ho[1, x - 1], hz - ho[2, x - 1]
        r, c = rb[x], cb[x]
        nx = r * ex + c * ((hz - hzp) - (hy - prev_z(hy, lanes)))
        ny = r * ey + c * ((hx - prev_z(hx, lanes)) - hz_x)
        nz = r * ez + c * (hy_x - (hx - hxp))
        eo[0, x] = nx
        eo[1, x] = ny
        eo[2, x] = nz
    row(0, True, False)

    def inner(x, carry):
        row(x, False, False)
        return carry

    lax.fori_loop(1, 15, inner, 0)
    row(15, False, True)

    pl.when(has_xn)(xe.wait_recv)
    pl.when(has_xp)(xh.wait_recv)
    pl.when(jnp.logical_and(has_xn, has_yp))(corner.wait_recv)
    dhy, dhz = 0.5 * xe_l[1], -0.5 * xe_l[0]
    ho[1, 15] = ho[1, 15] + dhy
    ho[2, 15] = ho[2, 15] + dhz
    dhz_p = jnp.where(rows == 0, -0.5 * ce_l[7:8], pltpu.roll(dhz, 1, 0))
    c = cb[15]
    eo[0, 15] = eo[0, 15] + c * ((dhz - dhz_p) - (dhy - prev_z(dhy, lanes)))
    eo[1, 15] = eo[1, 15] - c * dhz
    eo[2, 15] = eo[2, 15] + c * dhy
    hyp = jnp.where(has_xp, xh_l[0] + 0.5 * eb[2, 0], 0.0)
    hzp = jnp.where(has_xp, xh_l[1] - 0.5 * eb[1, 0], 0.0)
    c = cb[0]
    eo[1, 0] = eo[1, 0] + c * hzp
    eo[2, 0] = eo[2, 0] - c * hyp
    def b_wait(o):
        src = block_at(o)
        at = ((src // 4) & 1, (src // 8) * 4 + (src & 3))
        remote(bs.at[src], bl.at[at], b_ss.at[0], b_rs.at[at], src, Y).wait_recv()

    sign = jnp.where(lax.broadcasted_iota(jnp.int32, (128, 128), 1) < 64, 1.0, -1.0)
    y = None
    for half in range(2):
        for o in offsets[:-1]:
            if o[1] == half:
                b_wait(o)
        which = (x_hi + half) & 1
        block = bl[which].reshape(128, 128)
        high, low = split(jnp.concatenate([block, pltpu.roll(block, 64, 1) * sign], axis=0))
        part = dot_nn(tw[0, which], high) + dot_nn(tw[0, which], low) + dot_nn(tw[1, which], high)
        y = part if y is None else y + part
    y = y * tt[0] + pltpu.roll(y, 64, 1) * tt[1]
    y_sw = pltpu.roll(y, 64, 1) * jnp.concatenate([sign, sign], axis=0)
    pieces = []
    for b in range(4):
        pieces += [y[64 * b : 64 * b + 64], y_sw[64 * b : 64 * b + 64]]
    high, low = split(jnp.concatenate(pieces, axis=0))
    out = dot_nt(tg[0], high) + dot_nt(tg[0], low) + dot_nt(tg[1], high)
    for a in range(8):
        for b in range(4):
            cs[4 * a + b] = out[4 * a : 4 * a + 4, 128 * b : 128 * b + 128]

    def finished(at):
        to = block_at(offsets[at])
        return remote(cs.at[to], cl.at[Y, slot], c_ss.at[at], c_rs.at[Y, slot], to, home)

    for at in range(GX - 1):
        finished(at).start()
        pending.append(finished(at).wait_send)
    pl.when(home != Y)(finished(GX - 1).start)
    pending.append(lambda: pl.when(home != Y)(finished(GX - 1).wait_send))

    @pl.when(home == Y)
    def _():
        cl[Y, slot] = cs[X]

    def own_plane(x, carry):
        for at, v in enumerate((eo[0, x], eo[1, x], ho[0, x], ho[1, x])):
            pp[at, pl.ds(x, 1), :] = plane_of(v, PLANE)
        return carry

    lax.fori_loop(0, 16, own_plane, 0)
    for at in range(4):
        t = pp[at]
        for f in range(4):
            nr[at, f] = srv[at, f] + t * wave_cos[f]
            ni[at, f] = siv[at, f] - t * wave_sin[f]

    def c_wait(i, carry):
        g, q = i // 8, lax.rem(i, 8)
        src = 8 * Y + q

        @pl.when(jnp.logical_or(g != Y, src != X))
        def _():
            remote(cs.at[0], cl.at[g, q], c_ss.at[0], c_rs.at[g, q], src, g).wait_recv()

        return carry

    lax.fori_loop(0, 32, c_wait, 0)

    for q in range(8):
        for g in range(4):
            rel[q, 4 * g : 4 * g + 4, :] = cl[g, q]
    for wait in pending:
        wait()


def flush_kernel(eo, ho, nr, ni, rel, e_out, h_out, r_out, i_out, f_out, zz, fv, sem):
    copies = []
    for i in range(3):
        for x in range(0, 16, 4):
            part = (i, pl.ds(x, 4))
            copies += [(eo.at[part], e_out.at[part]), (ho.at[part], h_out.at[part])]
    copies += [(nr, r_out), (ni, i_out)]
    copies = [pltpu.make_async_copy(src, dst, sem.at[at]) for at, (src, dst) in enumerate(copies)]
    for copy in copies:
        copy.start()
    lane16 = lax.broadcasted_iota(jnp.int32, (16, 128), 1)
    turned = [pltpu.roll(rel[q], 8 * q, 1) if q else rel[q] for q in range(8)]
    group = lane16 // 8
    for s in range(16):
        acc = turned[0]
        for q in range(1, 8):
            acc = jnp.where(group == (q + s) % 16, turned[q], acc)
        if s:
            acc = pltpu.roll(acc, 128 - 8 * s, 1)
        zz[:, s, :] = acc
    for g in range(4):
        for f in range(4):
            fv[0, g, f] = zz[4 * g + f, 0:8, 0:64]
            fv[1, g, f] = zz[4 * g + f, 8:16, 0:64]
    copies.append(pltpu.make_async_copy(fv, f_out, sem.at[26]))
    copies[-1].start()
    for copy in copies:
        copy.wait()


def per_device(electric, magnetic, retention, coupling, spectrum_real, spectrum_imag, phases):
    tab_y, tab_w, tab_t, tab_g = (jnp.asarray(t) for t in tables())
    vmem, dma = pltpu.VMEM, pltpu.SemaphoreType.DMA
    hbm = pl.BlockSpec(memory_space=pltpu.HBM)
    in_vmem = pl.BlockSpec(memory_space=pltpu.VMEM)
    shapes = [
        jax.ShapeDtypeStruct(electric.shape, F32),
        jax.ShapeDtypeStruct(magnetic.shape, F32),
        jax.ShapeDtypeStruct(spectrum_real.shape, F32),
        jax.ShapeDtypeStruct(spectrum_imag.shape, F32),
        jax.ShapeDtypeStruct((2, 4, 4, 8, 64), F32),
    ]
    fixed = [
        pltpu.with_memory_space_constraint(a, pltpu.HBM)
        for a in (electric, magnetic, retention, coupling, spectrum_real, spectrum_imag, tab_y, tab_w, tab_t, tab_g)
    ]
    held = pl.pallas_call(
        step_kernel,
        out_shape=shapes[:4] + [jax.ShapeDtypeStruct((8, 16, 128), F32)],
        in_specs=[hbm] * 11,
        out_specs=[in_vmem] * 5,
        scratch_shapes=[
            vmem(electric.shape, F32), vmem(magnetic.shape, F32), vmem(retention.shape, F32), vmem(coupling.shape, F32),
            vmem(spectrum_real.shape, F32), vmem(spectrum_imag.shape, F32),
            vmem(tab_y.shape, BF16), vmem(tab_w.shape, BF16), vmem(tab_t.shape, F32), vmem(tab_g.shape, BF16),
            vmem((2, 16, 128), F32), vmem((2, 16, 128), F32), vmem((2, 16, 128), F32), vmem((2, 16, 128), F32),
            vmem((2, 128, 128), F32), vmem((2, 128, 128), F32), vmem((8, 128), F32),
            vmem((8, 128), F32), vmem((3, 4, 8, 128), F32),
            vmem((4, 32, 128), F32), vmem((4, 32, 128), F32), vmem((2, 4, 4, 16, 128), F32),
            vmem((32, 8, 128), F32), vmem((2, 16, 8, 128), F32), vmem((32, 4, 128), F32), vmem((4, 8, 4, 128), F32),
            vmem((2, 128, 128), F32), vmem((15, 16, 128), F32), vmem((8, 128), F32), pltpu.SMEM((4,), F32),
            vmem((128, 128), F32), vmem((128, 128), F32),
            dma((22,)), dma((4,)), dma((3, 4)), dma((3, 4)), dma((2, 4)), dma((2, 4)), dma((4,)), dma((4,)), dma((6,)),
            dma((32,)), dma((2, 16)), dma((32,)), dma((4, 8)), dma,
        ],
        compiler_params=pltpu.CompilerParams(collective_id=0, has_side_effects=True, vmem_limit_bytes=40 * 2**20),
    )(*fixed[:6], pltpu.with_memory_space_constraint(phases, pltpu.HBM), *fixed[6:])
    return pl.pallas_call(
        flush_kernel,
        out_shape=shapes,
        in_specs=[in_vmem] * 5,
        out_specs=[hbm] * 5,
        scratch_shapes=[vmem((16, 16, 128), F32), vmem((2, 4, 4, 8, 64), F32), dma((27,))],
        compiler_params=pltpu.CompilerParams(vmem_limit_bytes=16 * 2**20),
    )(*held)


def solution(mesh):
    placed = (
        P(None, "gx", "gy", None),
        P(None, "gx", "gy", None),
        P("gx", "gy", None),
        P("gx", "gy", None),
        P(None, None, "gx", "gy"),
        P(None, None, "gx", "gy"),
        P(),
    )
    return jax.shard_map(
        per_device,
        mesh=mesh,
        in_specs=placed,
        out_specs=(
            P(None, "gx", "gy", None),
            P(None, "gx", "gy", None),
            P(None, None, "gx", "gy"),
            P(None, None, "gx", "gy"),
            P(None, None, None, "gx", "gy"),
        ),
        check_vma=False,
    )
```

```python
import functools
import itertools
import math

import jax
import jax.numpy as jnp
import numpy as np
from jax import lax
from jax.experimental import pallas as pl
from jax.experimental.pallas import tpu as pltpu
from jax.sharding import PartitionSpec as P

MESH = pl.DeviceIdType.MESH
WAVES = 256
PLANE = 111
GX, GY = 32, 4
F32, BF16 = jnp.float32, jnp.bfloat16


def split_np(table):
    high = table.astype(np.float32).astype(jnp.bfloat16)
    low = (table - high.astype(np.float64)).astype(np.float32).astype(jnp.bfloat16)
    return np.stack([high, low])


def angle_np(wave, place):
    return (np.multiply.outer(wave, place) % 1024) * (math.pi / 512)


@functools.cache
def tables():
    wave = 2 * np.arange(WAVES) - 255
    ang = angle_np(wave, np.arange(512)).reshape(256, 4, 128).transpose(1, 0, 2)
    tab_y = split_np(np.concatenate([np.cos(ang), np.sin(ang)], axis=2))
    ang = angle_np(2 * np.arange(32) - 255, 16 * np.arange(32))
    eye = np.eye(8)
    ang = ang.reshape(32, 4, 2, 4).transpose(2, 0, 1, 3).reshape(2, 32, 16)
    tab_w = np.stack([np.concatenate([np.kron(np.cos(a), eye), np.kron(np.sin(a), eye)], axis=1) for a in ang])
    tab_w = split_np(tab_w)
    ang = np.repeat(angle_np(2 * np.arange(32) - 255, np.arange(16)), 8, axis=0)
    cos, sin = np.tile(np.cos(ang), (1, 8)), np.tile(np.sin(ang), (1, 8))
    sin[:, 64:] *= -1
    tab_t = np.stack([cos, sin]).astype(np.float32)
    ang = 2 * math.pi * (np.multiply.outer(np.arange(8), np.arange(16)) % 16) / 16
    eye = np.eye(4)
    blocks = [np.einsum("ai,fg->afgi", t, eye).reshape(32, 64) for t in (np.cos(ang), np.sin(ang))]
    tab_g = split_np(np.concatenate(blocks, axis=1) / 512.0)
    return tab_y, tab_w, tab_t, tab_g


def hops(o):
    return min(o[0], 4 - o[0]) + 2 * o[1] + min(o[2], 4 - o[2])


def split(value):
    high = value.astype(BF16)
    return high, (value - high.astype(F32)).astype(BF16)


def dot_nt(a, b):
    return lax.dot_general(a, b, (((1,), (1,)), ((), ())), preferred_element_type=F32)


def dot_nn(a, b):
    return lax.dot_general(a, b, (((1,), (0,)), ((), ())), preferred_element_type=F32)


def plane_of(value, at):
    wide = jnp.broadcast_to(value[:, at : at + 1], (128, 128))
    rows = lax.broadcasted_iota(jnp.int32, (128, 128), 0)
    lanes = lax.broadcasted_iota(jnp.int32, (128, 128), 1)
    return jnp.sum(jnp.where(rows == lanes, wide, 0.0), axis=0, keepdims=True)


def step_kernel(
    e_hbm, h_hbm, r_hbm, c_hbm, sr_hbm, si_hbm, ph_hbm, ty_hbm, tw_hbm, tt_hbm, tg_hbm,
    eo, ho, nr, ni, rel,
    eb, hb, rb, cb, srv, siv, ty, tw, tt, tg,
    ye_s, yh_s, ye_l, yh_l, xe_l, xh_l, ce_l, pk_s, pk_l, t_s, t_l, al,
    bs, bl, cs, cl, xh_s, pp, wv, ph_ref, gm, gt,
    ld_sem, yh_sem, pk_ss, pk_rs, a_ss, a_rs, t_ss, t_rs, x_sem, b_ss, b_rs, c_ss, c_rs, ph_sem,
):
    X = lax.axis_index("gx")
    Y = lax.axis_index("gy")
    xn, xp = lax.rem(X + 1, GX), lax.rem(X + GX - 1, GX)
    yn, yp = lax.rem(Y + 1, GY), lax.rem(Y + GY - 1, GY)
    has_xn, has_xp, has_yn, has_yp = X < GX - 1, X > 0, Y < GY - 1, Y > 0

    pending = []
    barrier = pltpu.get_barrier_semaphore()
    home, slot = X // 8, lax.rem(X, 8)
    offsets = sorted(itertools.product(range(4), range(2), range(4)), key=lambda o: (-hops(o), o))
    at_y = [((X // 8 + a) & 3) * 8 for a in range(4)]
    at_x = [((X // 4 + b) & 1) * 4 for b in range(2)]
    at_z = [(X + c) & 3 for c in range(4)]

    def block_at(o):
        return at_y[o[0]] + at_x[o[1]] + at_z[o[2]]

    def greet(x, y):
        pl.semaphore_signal(barrier, inc=1, device_id=(x, y), device_id_type=MESH)

    others = [lax.rem(Y + d, GY) for d in range(1, GY)]
    for o in offsets[:-1]:
        greet(block_at(o), Y)
    for x in (xp, xn, X):
        for y in others:
            greet(x, y)
    for o in sorted(itertools.product(range(2), range(4)), key=lambda o: (-hops((0,) + o), o)):
        for y in others:
            greet(8 * Y + at_x[o[0]] + at_z[o[1]], y)
    greeted = 3 * (GY - 1) + (GX - 1) + jnp.where(home != Y, GX, 0)

    def load(src, dst, sem):
        copy = pltpu.make_async_copy(src, dst, sem)
        copy.start()
        return copy

    phase = pltpu.make_async_copy(ph_hbm, ph_ref, ph_sem)
    phase.start()
    for at in range(4):
        part = pl.ds(4 * at, 4)
        load(e_hbm.at[:, part], eb.at[:, part], ld_sem.at[at])
        load(h_hbm.at[:, part], hb.at[:, part], ld_sem.at[at])
        load(c_hbm.at[part], cb.at[part], ld_sem.at[at])
        load(r_hbm.at[part], rb.at[part], ld_sem.at[at])
    load(sr_hbm, srv, ld_sem.at[4])
    load(si_hbm, siv, ld_sem.at[4])
    phase.wait()
    row8 = lax.broadcasted_iota(jnp.int32, (8, 128), 0)
    angle = jnp.zeros((8, 128), F32)
    for f in range(4):
        angle = jnp.where(lax.rem(row8, 4) == f, ph_ref[f], angle)
    wv[...] = jnp.where(row8 < 4, jnp.cos(angle), jnp.sin(angle))

    rows = lax.broadcasted_iota(jnp.int32, (128, 128), 0)
    lanes = lax.broadcasted_iota(jnp.int32, (128, 128), 1)
    row16 = lax.broadcasted_iota(jnp.int32, (16, 128), 0)
    lane16 = lax.broadcasted_iota(jnp.int32, (16, 128), 1)
    lane1 = lax.broadcasted_iota(jnp.int32, (1, 128), 1)

    def next_z(v, lane):
        return jnp.where(lane == 127, 0.0, pltpu.roll(v, 127, 1))

    def prev_z(v, lane):
        return jnp.where(lane == 0, 0.0, pltpu.roll(v, 1, 1))

    @pl.when(jnp.logical_not(has_xn))
    def _():
        xe_l[...] = jnp.zeros_like(xe_l)
        pk_l[2] = jnp.zeros_like(pk_l[2])

    @pl.when(jnp.logical_not(has_xp))
    def _():
        xh_l[...] = jnp.zeros_like(xh_l)
        pk_l[0] = jnp.zeros_like(pk_l[0])

    @pl.when(jnp.logical_not(has_yn))
    def _():
        ye_l[...] = jnp.zeros_like(ye_l)

    @pl.when(jnp.logical_not(has_yp))
    def _():
        yh_l[...] = jnp.zeros_like(yh_l)

    @pl.when(jnp.logical_not(jnp.logical_and(has_xn, has_yp)))
    def _():
        ce_l[...] = jnp.zeros_like(ce_l)

    fields = [(eb, 0), (eb, 1), (eb, 2), (hb, 0), (hb, 1), (hb, 2), (rb, None), (cb, None)]
    wanted = [(0, 0), (0, 1), (0, 2), (1, 0), (1, 1), (1, 2), (2, 0), (2, 1), (3, 0), (3, 1), (4, 0), (4, 1), (5, 1), (6, 1), (7, 1)]
    lane32 = lax.broadcasted_iota(jnp.int32, (32, 128), 1)
    window = jnp.logical_and(lane32 >= PLANE - 1, lane32 < PLANE + 3)

    for at in range(4):
        pltpu.make_async_copy(e_hbm.at[0:2], eb.at[0:2], ld_sem.at[at]).wait()

        def gather(block, carry, at=at):
            ys = pl.ds(pl.multiple_of(block * 32, 32), 32)
            total = None
            for which, (ref, comp) in enumerate(fields):
                for x in range(4):
                    v = ref[4 * at + x, ys, :] if comp is None else ref[comp, 4 * at + x, ys, :]
                    v = jnp.where(window, v, 0.0)
                    shift = (4 * (4 * which + x) - (PLANE - 1)) % 128
                    v = pltpu.roll(v, shift, 1) if shift else v
                    total = v if total is None else total + v
            gm[ys, :] = total
            return carry

        lax.fori_loop(0, 4, gather, 0)
        gt[...] = gm[...].T
        for to, (which, z) in enumerate(wanted):
            pp[to, 4 * at : 4 * at + 4, :] = gt[pl.ds(16 * which + z, 4, stride=4), :]
    pairs = ((ty_hbm, ty), (tw_hbm, tw), (tt_hbm, tt), (tg_hbm, tg))
    tabs = [load(src, dst, ld_sem.at[5 + at]) for at, (src, dst) in enumerate(pairs)]

    ex0, ex1, ex2, ey0, ey1, ey2, ez0, ez1, hx0, hx1, hy0, hy1, hz1, r1, c1 = (pp[at] for at in range(15))

    def next_x(v):
        return jnp.where(row16 == 15, 0.0, pltpu.roll(v, 15, 0))

    def prev_x(v):
        return jnp.where(row16 == 0, 0.0, pltpu.roll(v, 1, 0))

    phx1 = hx1 - 0.5 * ((next_z(ez1, lane16) - ez1) - (ey2 - ey1))
    phx0 = hx0 - 0.5 * ((next_z(ez0, lane16) - ez0) - (ey1 - ey0))
    phy1 = hy1 - 0.5 * ((ex2 - ex1) - (next_x(ez1) - ez1))
    phy0 = hy0 - 0.5 * ((ex1 - ex0) - (next_x(ez0) - ez0))
    phz1 = hz1 - 0.5 * ((next_x(ey1) - ey1) - (next_z(ex1, lane16) - ex1))
    t_s[0, 0:16] = r1 * ex1 + c1 * ((phz1 - prev_z(phz1, lane16)) - (phy1 - phy0))
    t_s[1, 0:16] = r1 * ey1 + c1 * ((phx1 - phx0) - (phz1 - prev_x(phz1)))
    t_s[2, 0:16] = phx1
    t_s[3, 0:16] = phy1
    cols = jnp.zeros((16, 128), F32)
    for at, (v, y) in enumerate(((ex1, 0), (ez1, 0), (ez0, 0), (c1, 0), (phz1, 127), (c1, 127))):
        cols = jnp.where(lane16 == at, v[:, y : y + 1], cols)
    for g in range(GY):
        t_s[g, 16:32] = cols
    pk_s[0:1] = ey1[0:1]
    pk_s[1:2] = ez1[0:1]
    pk_s[2:3] = ez0[0:1]
    pk_s[3:4] = phz1[15:16]
    pk_s[4:5] = c1[0:1]
    pk_s[5:6] = c1[15:16]
    pk_s[6:7] = ex1[15:16]
    pk_s[7:8] = jnp.zeros((1, 128), F32)

    ye_s[0] = eb[0, :, 0, :]
    ye_s[1] = eb[2, :, 0, :]
    ex, ey, ez = eb[0, :, 127, :], eb[1, :, 127, :], eb[2, :, 127, :]
    yh_s[0] = hb[0, :, 127, :] - 0.5 * (-ez - (next_z(ey, lane16) - ey))
    ey_up = jnp.where(row16 == 15, 0.0, pltpu.roll(ey, 15, 0))
    yh_s[1] = hb[2, :, 127, :] - 0.5 * (ey_up - ey + ex)

    pk_l[1, Y] = pk_s[...]
    pltpu.make_async_copy(c_hbm.at[0:4], cb.at[0:4], ld_sem.at[4]).wait()
    al[0, Y] = srv[Y]
    al[1, Y] = siv[Y]
    t_l[Y] = t_s[Y]

    pl.semaphore_wait(barrier, greeted)

    def remote(src, dst, ss, rs, x, y):
        return pltpu.make_async_remote_copy(
            src_ref=src, dst_ref=dst, send_sem=ss, recv_sem=rs, device_id=(x, y), device_id_type=MESH
        )

    def pack(dx, d):
        return remote(
            pk_s, pk_l.at[2 - dx, Y], pk_ss.at[dx], pk_rs.at[2 - dx], (xp, X, xn)[dx], lax.rem(Y + d, GY)
        )

    for dx, ok in ((0, has_xp), (2, has_xn)):
        for d in range(GY):
            pl.when(ok)(pack(dx, d).start)
    for d in range(1, GY):
        pack(1, d).start()

    def all_of(ref, ss, rs):
        return remote(ref, ref, ss, rs, xp, Y)

    def packs_sent():
        for dx, ok in ((0, has_xp), (2, has_xn)):
            pl.when(ok)(all_of(pk_l.at[0], pk_ss.at[dx], pk_rs.at[dx]).wait_send)
        all_of(pk_l.at[0, 0:3], pk_ss.at[1], pk_rs.at[1]).wait_send()

    pending.append(packs_sent)

    def tangent(d):
        g = lax.rem(Y + d, GY)
        return remote(t_s.at[g], t_l.at[Y], t_ss, t_rs, X, g)

    for d in range(1, GY):
        tangent(d).start()
    pending.append(lambda: all_of(t_s.at[0:3], t_ss, t_rs).wait_send())

    def spectrum(part, d):
        g = lax.rem(Y + d, GY)
        return remote((srv, siv)[part].at[g], al.at[part, Y], a_ss, a_rs, X, g)

    for d in range(1, GY):
        for part in range(2):
            spectrum(part, d).start()
    pending.append(lambda: all_of(al.at[:, 0:3], a_ss, a_rs).wait_send())

    ye = remote(ye_s, ye_l, yh_sem.at[0], yh_sem.at[1], X, yp)
    yh = remote(yh_s, yh_l, yh_sem.at[2], yh_sem.at[3], X, yn)
    pl.when(has_yp)(ye.start)
    pl.when(has_yn)(yh.start)
    pending.append(lambda: pl.when(has_yp)(ye.wait_send))
    pending.append(lambda: pl.when(has_yn)(yh.wait_send))

    corner = remote(eb.at[1, 0, pl.ds(120, 8)], ce_l, x_sem.at[0], x_sem.at[1], xp, yn)
    pl.when(jnp.logical_and(has_xp, has_yn))(corner.start)
    pending.append(lambda: pl.when(jnp.logical_and(has_xp, has_yn))(corner.wait_send))
    xe = remote(eb.at[pl.ds(1, 2), 0], xe_l, x_sem.at[2], x_sem.at[3], xp, Y)
    pl.when(has_xp)(xe.start)
    pending.append(lambda: pl.when(has_xp)(xe.wait_send))

    pl.when(has_yn)(ye.wait_recv)
    pl.when(has_yp)(yh.wait_recv)
    yh_l[0] = jnp.where(has_yp, yh_l[0] - 0.5 * ye_s[1], 0.0)
    yh_l[1] = jnp.where(has_yp, yh_l[1] + 0.5 * ye_s[0], 0.0)

    ex, ey, ez = eb[0, 15], eb[1, 15], eb[2, 15]
    exn = jnp.where(rows == 127, ye_l[0, 15:16, :], pltpu.roll(ex, 127, 0))
    xh_s[0] = hb[1, 15] - 0.5 * ((next_z(ex, lanes) - ex) + ez)
    xh_s[1] = hb[2, 15] - 0.5 * (-ey - (exn - ex))
    xh = remote(xh_s, xh_l, x_sem.at[4], x_sem.at[5], xn, Y)
    pl.when(has_xn)(xh.start)
    pending.append(lambda: pl.when(has_xn)(xh.wait_send))

    def from_gy(make, d):
        make(d).wait_recv()

    all_of(al.at[:, 0:3], a_ss, a_rs).wait_recv()
    all_of(t_l.at[0:3], t_ss, t_rs).wait_recv()
    for copy in tabs:
        copy.wait()

    wave_cos, wave_sin = [wv[f : f + 1] for f in range(4)], [wv[f : f + 1] for f in range(4, 8)]
    total = None
    for s in range(GY):
        t, mine = t_l[s, 0:16], t_l[s, 16:32]
        if s < GY - 1:
            after = t_l[s + 1, 16:32]
            exn, ez1n, ez0n, c127 = after[:, 0:1], after[:, 1:2], after[:, 2:3], mine[:, 5:6]
            exn_p = prev_x(after)[:, 0:1]
            edge = jnp.where(
                Y == 0,
                0.5 * c127 * exn,
                jnp.where(Y == 1, -0.5 * c127 * ((ez1n - ez0n) + (exn - exn_p)), jnp.where(Y == 2, -0.5 * ez1n, 0.0)),
            )
            t = t + jnp.where(lane16 == 127, edge, 0.0)
        if s > 0:
            hzp0 = t_l[s - 1, 16:32][:, 4:5] + 0.5 * mine[:, 0:1]
            t = t + jnp.where(lane16 == 0, jnp.where(Y == 0, -mine[:, 3:4] * hzp0, 0.0), 0.0)
        re = jnp.concatenate([al[0, s, f] + t * wave_cos[f] for f in range(4)], axis=0)
        im = jnp.concatenate([al[1, s, f] - t * wave_sin[f] for f in range(4)], axis=0)
        data = jnp.concatenate(
            [jnp.concatenate([re, im], axis=0), jnp.concatenate([im, -re], axis=0)], axis=1
        )
        high, low = split(data)
        part = dot_nt(ty[0, s], high) + dot_nt(ty[0, s], low) + dot_nt(ty[1, s], high)
        total = part if total is None else total + part
    bs[...] = total.reshape(GX, 8, 128)

    all_of(pk_l.at[1, 0:3], pk_ss.at[1], pk_rs.at[1]).wait_recv()
    pl.when(has_xn)(all_of(pk_l.at[2], pk_ss.at[2], pk_rs.at[2]).wait_recv)
    pl.when(has_xp)(all_of(pk_l.at[0], pk_ss.at[0], pk_rs.at[0]).wait_recv)
    added = None
    none = jnp.zeros((1, 128), F32)
    for s in range(GY):
        nxt, own, prv = pk_l[2, s], pk_l[1, s], pk_l[0, s]
        dhz = -0.5 * nxt[0:1]
        before = -0.5 * pk_l[2, s - 1][0:1, 127:128] if s else jnp.zeros((1, 1), F32)
        dhz_p = jnp.where(lane1 == 0, before, pltpu.roll(dhz, 1, 1))
        dhy = 0.5 * nxt[1:2]
        dhyd = dhy - 0.5 * nxt[2:3]
        after = 0.5 * pk_l[0, s + 1][6:7, 0:1] if s < GY - 1 else jnp.zeros((1, 1), F32)
        hzp = prv[3:4] - 0.5 * own[0:1] + jnp.where(lane1 == 127, after, 0.0)
        last = jnp.where(
            Y == 0, own[5:6] * (dhz - dhz_p - dhyd), jnp.where(Y == 1, -own[5:6] * dhz, jnp.where(Y == 3, dhy, 0.0))
        )
        head = jnp.where(jnp.logical_and(Y == 1, has_xp), own[4:5] * hzp, 0.0)
        pair = [
            jnp.where(row8 == 0, last, 0.0) + jnp.where(row8 == 1, head, 0.0),
            jnp.where(row8 == 2, last, 0.0) + jnp.where(row8 == 3, head, 0.0),
        ]
        high, low = split(jnp.concatenate(pair, axis=1))
        rhs = jnp.concatenate([high, low], axis=0)
        part = dot_nt(ty[0, s], rhs) + dot_nt(ty[1, s], rhs)
        added = part if added is None else added + part
    added = added[:, 0:8] + added[:, 8:16]
    wc, ws = none, none
    for f in range(4):
        wc = jnp.where((lane1 // 16) % 4 == f, wave_cos[f], wc)
        ws = jnp.where((lane1 // 16) % 4 == f, wave_sin[f], ws)
    by_cos, by_sin = jnp.where(lane1 < 64, wc, -ws), jnp.where(lane1 < 64, -ws, -wc)
    is_last, is_head = lane1 % 16 == 15, lane1 % 16 == 0
    extra = added[:, 0:1] * jnp.where(is_last, by_cos, 0.0) + added[:, 1:2] * jnp.where(is_head, by_cos, 0.0)
    extra = extra + added[:, 2:3] * jnp.where(is_last, by_sin, 0.0) + added[:, 3:4] * jnp.where(is_head, by_sin, 0.0)
    bs[...] = bs[...] + extra.reshape(GX, 8, 128)

    x_hi, row_in = (X // 4) & 1, (X // 8) * 4 + (X & 3)

    def column(at):
        to = block_at(offsets[at])
        return remote(bs.at[to], bl.at[x_hi, row_in], b_ss, b_rs.at[offsets[at][1]], to, Y)

    for at in range(GX - 1):
        column(at).start()
    pending.append(lambda: all_of(bs.at[0:31], b_ss, b_rs.at[0]).wait_send())
    bl[x_hi, row_in] = bs[X]

    def row(x, edge_first, edge_last):
        ex, ey, ez = eb[0, x], eb[1, x], eb[2, x]
        exn = jnp.where(rows == 127, ye_l[0, pl.ds(x, 1), :], pltpu.roll(ex, 127, 0))
        ezn = jnp.where(rows == 127, ye_l[1, pl.ds(x, 1), :], pltpu.roll(ez, 127, 0))
        if edge_last:
            ey_x, ez_x = -ey, -ez
        else:
            ey_x, ez_x = eb[1, x + 1] - ey, eb[2, x + 1] - ez
        hx = hb[0, x] - 0.5 * ((ezn - ez) - (next_z(ey, lanes) - ey))
        hy = hb[1, x] - 0.5 * ((next_z(ex, lanes) - ex) - ez_x)
        hz = hb[2, x] - 0.5 * (ey_x - (exn - ex))
        ho[0, x] = hx
        ho[1, x] = hy
        ho[2, x] = hz
        hxp = jnp.where(rows == 0, yh_l[0, pl.ds(x, 1), :], pltpu.roll(hx, 1, 0))
        hzp = jnp.where(rows == 0, yh_l[1, pl.ds(x, 1), :], pltpu.roll(hz, 1, 0))
        if edge_first:
            hy_x, hz_x = hy, hz
        else:
            hy_x, hz_x = hy - ho[1, x - 1], hz - ho[2, x - 1]
        r, c = rb[x], cb[x]
        nx = r * ex + c * ((hz - hzp) - (hy - prev_z(hy, lanes)))
        ny = r * ey + c * ((hx - prev_z(hx, lanes)) - hz_x)
        nz = r * ez + c * (hy_x - (hx - hxp))
        eo[0, x] = nx
        eo[1, x] = ny
        eo[2, x] = nz
    row(0, True, False)

    def inner(x, carry):
        row(x, False, False)
        return carry

    lax.fori_loop(1, 15, inner, 0)
    row(15, False, True)

    sign = jnp.where(lax.broadcasted_iota(jnp.int32, (128, 128), 1) < 64, 1.0, -1.0)
    y = None
    for half in range(2):
        all_of(bs.at[0 : 15 + half], b_ss, b_rs.at[half]).wait_recv()
        which = (x_hi + half) & 1
        block = bl[which].reshape(128, 128)
        high, low = split(jnp.concatenate([block, pltpu.roll(block, 64, 1) * sign], axis=0))
        part = dot_nn(tw[0, which], high) + dot_nn(tw[0, which], low) + dot_nn(tw[1, which], high)
        y = part if y is None else y + part
    y = y * tt[0] + pltpu.roll(y, 64, 1) * tt[1]
    y_sw = pltpu.roll(y, 64, 1) * jnp.concatenate([sign, sign], axis=0)
    pieces = []
    for b in range(4):
        pieces += [y[64 * b : 64 * b + 64], y_sw[64 * b : 64 * b + 64]]
    high, low = split(jnp.concatenate(pieces, axis=0))
    out = dot_nt(tg[0], high) + dot_nt(tg[0], low) + dot_nt(tg[1], high)
    for a in range(8):
        for b in range(4):
            cs[4 * a + b] = out[4 * a : 4 * a + 4, 128 * b : 128 * b + 128]

    def finished(at):
        to = block_at(offsets[at])
        return remote(cs.at[to], cl.at[Y, slot], c_ss, c_rs, to, home)

    for at in range(GX - 1):
        finished(at).start()
    pl.when(home != Y)(finished(GX - 1).start)

    def blocks(wait):
        pl.when(home != Y)(lambda: wait(all_of(cs, c_ss, c_rs)))
        pl.when(home == Y)(lambda: wait(all_of(cs.at[0:31], c_ss, c_rs)))

    pending.append(lambda: blocks(lambda copy: copy.wait_send()))

    @pl.when(home == Y)
    def _():
        cl[Y, slot] = cs[X]

    pl.when(has_xn)(xe.wait_recv)
    pl.when(has_xp)(xh.wait_recv)
    pl.when(jnp.logical_and(has_xn, has_yp))(corner.wait_recv)
    dhy, dhz = 0.5 * xe_l[1], -0.5 * xe_l[0]
    ho[1, 15] = ho[1, 15] + dhy
    ho[2, 15] = ho[2, 15] + dhz
    dhz_p = jnp.where(rows == 0, -0.5 * ce_l[7:8], pltpu.roll(dhz, 1, 0))
    c = cb[15]
    eo[0, 15] = eo[0, 15] + c * ((dhz - dhz_p) - (dhy - prev_z(dhy, lanes)))
    eo[1, 15] = eo[1, 15] - c * dhz
    eo[2, 15] = eo[2, 15] + c * dhy
    hyp = jnp.where(has_xp, xh_l[0] + 0.5 * eb[2, 0], 0.0)
    hzp = jnp.where(has_xp, xh_l[1] - 0.5 * eb[1, 0], 0.0)
    c = cb[0]
    eo[1, 0] = eo[1, 0] + c * hzp
    eo[2, 0] = eo[2, 0] - c * hyp

    def own_plane(x, carry):
        for at, v in enumerate((eo[0, x], eo[1, x], ho[0, x], ho[1, x])):
            pp[at, pl.ds(x, 1), :] = plane_of(v, PLANE)
        return carry

    lax.fori_loop(0, 16, own_plane, 0)
    for at in range(4):
        t = pp[at]
        for f in range(4):
            nr[at, f] = srv[at, f] + t * wave_cos[f]
            ni[at, f] = siv[at, f] - t * wave_sin[f]

    blocks(lambda copy: copy.wait_recv())

    for q in range(8):
        for g in range(4):
            rel[q, 4 * g : 4 * g + 4, :] = cl[g, q]
    for wait in pending:
        wait()


def flush_kernel(eo, ho, nr, ni, rel, e_out, h_out, r_out, i_out, f_out, zz, fv, sem):
    for which, (src, dst) in enumerate(((eo, e_out), (ho, h_out))):
        for i in range(3):
            for x in range(0, 16, 8):
                part = (i, pl.ds(x, 8))
                pltpu.make_async_copy(src.at[part], dst.at[part], sem.at[which]).start()
    whole = [pltpu.make_async_copy(src, dst, sem.at[at]) for at, (src, dst) in enumerate(((eo, e_out), (ho, h_out)))]
    copies = [pltpu.make_async_copy(nr, r_out, sem.at[2]), pltpu.make_async_copy(ni, i_out, sem.at[3])]
    for copy in copies:
        copy.start()
    lane16 = lax.broadcasted_iota(jnp.int32, (16, 128), 1)
    turned = [pltpu.roll(rel[q], 8 * q, 1) if q else rel[q] for q in range(8)]
    group = lane16 // 8
    for s in range(16):
        acc = turned[0]
        for q in range(1, 8):
            acc = jnp.where(group == (q + s) % 16, turned[q], acc)
        if s:
            acc = pltpu.roll(acc, 128 - 8 * s, 1)
        zz[:, s, :] = acc
    for g in range(4):
        for f in range(4):
            fv[0, g, f] = zz[4 * g + f, 0:8, 0:64]
            fv[1, g, f] = zz[4 * g + f, 8:16, 0:64]
    copies.append(pltpu.make_async_copy(fv, f_out, sem.at[4]))
    copies[-1].start()
    for copy in copies + whole:
        copy.wait()


def per_device(electric, magnetic, retention, coupling, spectrum_real, spectrum_imag, phases):
    tab_y, tab_w, tab_t, tab_g = (jnp.asarray(t) for t in tables())
    vmem, dma = pltpu.VMEM, pltpu.SemaphoreType.DMA
    hbm = pl.BlockSpec(memory_space=pltpu.HBM)
    in_vmem = pl.BlockSpec(memory_space=pltpu.VMEM)
    shapes = [
        jax.ShapeDtypeStruct(electric.shape, F32),
        jax.ShapeDtypeStruct(magnetic.shape, F32),
        jax.ShapeDtypeStruct(spectrum_real.shape, F32),
        jax.ShapeDtypeStruct(spectrum_imag.shape, F32),
        jax.ShapeDtypeStruct((2, 4, 4, 8, 64), F32),
    ]
    fixed = [
        pltpu.with_memory_space_constraint(a, pltpu.HBM)
        for a in (electric, magnetic, retention, coupling, spectrum_real, spectrum_imag, tab_y, tab_w, tab_t, tab_g)
    ]
    held = pl.pallas_call(
        step_kernel,
        out_shape=shapes[:4] + [jax.ShapeDtypeStruct((8, 16, 128), F32)],
        in_specs=[hbm] * 11,
        out_specs=[in_vmem] * 5,
        scratch_shapes=[
            vmem(electric.shape, F32), vmem(magnetic.shape, F32), vmem(retention.shape, F32), vmem(coupling.shape, F32),
            vmem(spectrum_real.shape, F32), vmem(spectrum_imag.shape, F32),
            vmem(tab_y.shape, BF16), vmem(tab_w.shape, BF16), vmem(tab_t.shape, F32), vmem(tab_g.shape, BF16),
            vmem((2, 16, 128), F32), vmem((2, 16, 128), F32), vmem((2, 16, 128), F32), vmem((2, 16, 128), F32),
            vmem((2, 128, 128), F32), vmem((2, 128, 128), F32), vmem((8, 128), F32),
            vmem((8, 128), F32), vmem((3, 4, 8, 128), F32),
            vmem((4, 32, 128), F32), vmem((4, 32, 128), F32), vmem((2, 4, 4, 16, 128), F32),
            vmem((32, 8, 128), F32), vmem((2, 16, 8, 128), F32), vmem((32, 4, 128), F32), vmem((4, 8, 4, 128), F32),
            vmem((2, 128, 128), F32), vmem((15, 16, 128), F32), vmem((8, 128), F32), pltpu.SMEM((4,), F32),
            vmem((128, 128), F32), vmem((128, 128), F32),
            dma((9,)), dma((4,)), dma((3,)), dma((3,)), dma, dma, dma, dma, dma((6,)), dma, dma((2,)), dma, dma, dma,
        ],
        compiler_params=pltpu.CompilerParams(collective_id=0, has_side_effects=True, vmem_limit_bytes=40 * 2**20),
    )(*fixed[:6], pltpu.with_memory_space_constraint(phases, pltpu.HBM), *fixed[6:])
    return pl.pallas_call(
        flush_kernel,
        out_shape=shapes,
        in_specs=[in_vmem] * 5,
        out_specs=[hbm] * 5,
        scratch_shapes=[vmem((16, 16, 128), F32), vmem((2, 4, 4, 8, 64), F32), dma((5,))],
        compiler_params=pltpu.CompilerParams(vmem_limit_bytes=16 * 2**20),
    )(*held)


def solution(mesh):
    placed = (
        P(None, "gx", "gy", None),
        P(None, "gx", "gy", None),
        P("gx", "gy", None),
        P("gx", "gy", None),
        P(None, None, "gx", "gy"),
        P(None, None, "gx", "gy"),
        P(),
    )
    return jax.shard_map(
        per_device,
        mesh=mesh,
        in_specs=placed,
        out_specs=(
            P(None, "gx", "gy", None),
            P(None, "gx", "gy", None),
            P(None, None, "gx", "gy"),
            P(None, None, "gx", "gy"),
            P(None, None, None, "gx", "gy"),
        ),
        check_vma=False,
    )
```

```python
import functools
import itertools
import math

import jax
import jax.numpy as jnp
import numpy as np
from jax import lax
from jax.experimental import pallas as pl
from jax.experimental.pallas import tpu as pltpu
from jax.sharding import PartitionSpec as P

MESH = pl.DeviceIdType.MESH
WAVES = 256
PLANE = 111
GX, GY = 32, 4
F32, BF16 = jnp.float32, jnp.bfloat16


def split_np(table):
    high = table.astype(np.float32).astype(jnp.bfloat16)
    low = (table - high.astype(np.float64)).astype(np.float32).astype(jnp.bfloat16)
    return np.stack([high, low])


def angle_np(wave, place):
    return (np.multiply.outer(wave, place) % 1024) * (math.pi / 512)


@functools.cache
def tables():
    wave = 2 * np.arange(WAVES) - 255
    ang = angle_np(wave, np.arange(512)).reshape(256, 4, 128).transpose(1, 0, 2)
    tab_y = split_np(np.concatenate([np.cos(ang), np.sin(ang)], axis=2))
    ang = angle_np(2 * np.arange(32) - 255, 16 * np.arange(32))
    eye = np.eye(8)
    ang = ang.reshape(32, 4, 2, 4).transpose(2, 0, 1, 3).reshape(2, 32, 16)
    tab_w = np.stack([np.concatenate([np.kron(np.cos(a), eye), np.kron(np.sin(a), eye)], axis=1) for a in ang])
    tab_w = split_np(tab_w)
    ang = np.repeat(angle_np(2 * np.arange(32) - 255, np.arange(16)), 8, axis=0)
    cos, sin = np.tile(np.cos(ang), (1, 8)), np.tile(np.sin(ang), (1, 8))
    sin[:, 64:] *= -1
    tab_t = np.stack([cos, sin]).astype(np.float32)
    ang = 2 * math.pi * (np.multiply.outer(np.arange(8), np.arange(16)) % 16) / 16
    eye = np.eye(4)
    blocks = [np.einsum("ai,fg->afgi", t, eye).reshape(32, 64) for t in (np.cos(ang), np.sin(ang))]
    tab_g = split_np(np.concatenate(blocks, axis=1) / 512.0)
    return tab_y, tab_w, tab_t, tab_g


def hops(o):
    return min(o[0], 4 - o[0]) + 2 * o[1] + min(o[2], 4 - o[2])


def split(value):
    high = value.astype(BF16)
    return high, (value - high.astype(F32)).astype(BF16)


def dot_nt(a, b):
    return lax.dot_general(a, b, (((1,), (1,)), ((), ())), preferred_element_type=F32)


def dot_nn(a, b):
    return lax.dot_general(a, b, (((1,), (0,)), ((), ())), preferred_element_type=F32)


def plane_of(value, at):
    wide = jnp.broadcast_to(value[:, at : at + 1], (128, 128))
    rows = lax.broadcasted_iota(jnp.int32, (128, 128), 0)
    lanes = lax.broadcasted_iota(jnp.int32, (128, 128), 1)
    return jnp.sum(jnp.where(rows == lanes, wide, 0.0), axis=0, keepdims=True)


def step_kernel(
    e_hbm, h_hbm, r_hbm, c_hbm, sr_hbm, si_hbm, ph_hbm, ty_hbm, tw_hbm, tt_hbm, tg_hbm,
    eo, ho, nr, ni, rel,
    eb, hb, rb, cb, srv, siv, ty, tw, tt, tg,
    ye_s, yh_s, ye_l, yh_l, xe_l, xh_l, ce_l, pk_s, pk_l, t_s, t_l, al,
    bs, bl, cs, cl, xh_s, pp, wv, ph_ref, gm, gt,
    ld_sem, yh_sem, pk_ss, pk_rs, a_ss, a_rs, t_ss, t_rs, x_sem, b_ss, b_rs, c_ss, c_rs, ph_sem,
):
    X = lax.axis_index("gx")
    Y = lax.axis_index("gy")
    xn, xp = lax.rem(X + 1, GX), lax.rem(X + GX - 1, GX)
    yn, yp = lax.rem(Y + 1, GY), lax.rem(Y + GY - 1, GY)
    has_xn, has_xp, has_yn, has_yp = X < GX - 1, X > 0, Y < GY - 1, Y > 0

    pending = []
    barrier = pltpu.get_barrier_semaphore()
    home, slot = X // 8, lax.rem(X, 8)
    offsets = sorted(itertools.product(range(4), range(2), range(4)), key=lambda o: (-hops(o), o))
    at_y = [((X // 8 + a) & 3) * 8 for a in range(4)]
    at_x = [((X // 4 + b) & 1) * 4 for b in range(2)]
    at_z = [(X + c) & 3 for c in range(4)]

    def block_at(o):
        return at_y[o[0]] + at_x[o[1]] + at_z[o[2]]

    def greet(x, y):
        pl.semaphore_signal(barrier, inc=1, device_id=(x, y), device_id_type=MESH)

    others = [lax.rem(Y + d, GY) for d in range(1, GY)]
    for o in offsets[:-1]:
        greet(block_at(o), Y)
    for x in (xp, xn, X):
        for y in others:
            greet(x, y)
    for o in sorted(itertools.product(range(2), range(4)), key=lambda o: (-hops((0,) + o), o)):
        for y in others:
            greet(8 * Y + at_x[o[0]] + at_z[o[1]], y)
    greeted = 3 * (GY - 1) + (GX - 1) + jnp.where(home != Y, GX, 0)

    def load(src, dst, sem):
        copy = pltpu.make_async_copy(src, dst, sem)
        copy.start()
        return copy

    phase = pltpu.make_async_copy(ph_hbm, ph_ref, ph_sem)
    phase.start()
    for at in range(4):
        part = pl.ds(4 * at, 4)
        load(e_hbm.at[:, part], eb.at[:, part], ld_sem.at[at])
        load(h_hbm.at[:, part], hb.at[:, part], ld_sem.at[at])
        load(c_hbm.at[part], cb.at[part], ld_sem.at[at])
        load(r_hbm.at[part], rb.at[part], ld_sem.at[at])
    load(sr_hbm, srv, ld_sem.at[4])
    load(si_hbm, siv, ld_sem.at[4])
    phase.wait()
    row8 = lax.broadcasted_iota(jnp.int32, (8, 128), 0)
    angle = jnp.zeros((8, 128), F32)
    for f in range(4):
        angle = jnp.where(lax.rem(row8, 4) == f, ph_ref[f], angle)
    wv[...] = jnp.where(row8 < 4, jnp.cos(angle), jnp.sin(angle))

    rows = lax.broadcasted_iota(jnp.int32, (128, 128), 0)
    lanes = lax.broadcasted_iota(jnp.int32, (128, 128), 1)
    row16 = lax.broadcasted_iota(jnp.int32, (16, 128), 0)
    lane16 = lax.broadcasted_iota(jnp.int32, (16, 128), 1)
    lane1 = lax.broadcasted_iota(jnp.int32, (1, 128), 1)

    def next_z(v, lane):
        return jnp.where(lane == 127, 0.0, pltpu.roll(v, 127, 1))

    def prev_z(v, lane):
        return jnp.where(lane == 0, 0.0, pltpu.roll(v, 1, 1))

    @pl.when(jnp.logical_not(has_xn))
    def _():
        xe_l[...] = jnp.zeros_like(xe_l)
        pk_l[2] = jnp.zeros_like(pk_l[2])

    @pl.when(jnp.logical_not(has_xp))
    def _():
        xh_l[...] = jnp.zeros_like(xh_l)
        pk_l[0] = jnp.zeros_like(pk_l[0])

    @pl.when(jnp.logical_not(has_yn))
    def _():
        ye_l[...] = jnp.zeros_like(ye_l)

    @pl.when(jnp.logical_not(has_yp))
    def _():
        yh_l[...] = jnp.zeros_like(yh_l)

    @pl.when(jnp.logical_not(jnp.logical_and(has_xn, has_yp)))
    def _():
        ce_l[...] = jnp.zeros_like(ce_l)

    fields = [(eb, 0), (eb, 1), (eb, 2), (hb, 0), (hb, 1), (hb, 2), (rb, None), (cb, None)]
    wanted = [(0, 0), (0, 1), (0, 2), (1, 0), (1, 1), (1, 2), (2, 0), (2, 1), (3, 0), (3, 1), (4, 0), (4, 1), (5, 1), (6, 1), (7, 1)]
    lane32 = lax.broadcasted_iota(jnp.int32, (32, 128), 1)
    window = jnp.logical_and(lane32 >= PLANE - 1, lane32 < PLANE + 3)

    for at in range(4):
        pltpu.make_async_copy(e_hbm.at[0:2], eb.at[0:2], ld_sem.at[at]).wait()

        def gather(block, carry, at=at):
            ys = pl.ds(pl.multiple_of(block * 32, 32), 32)
            total = None
            for which, (ref, comp) in enumerate(fields):
                for x in range(4):
                    v = ref[4 * at + x, ys, :] if comp is None else ref[comp, 4 * at + x, ys, :]
                    v = jnp.where(window, v, 0.0)
                    shift = (4 * (4 * which + x) - (PLANE - 1)) % 128
                    v = pltpu.roll(v, shift, 1) if shift else v
                    total = v if total is None else total + v
            gm[ys, :] = total
            return carry

        lax.fori_loop(0, 4, gather, 0)
        gt[...] = gm[...].T
        for to, (which, z) in enumerate(wanted):
            pp[to, 4 * at : 4 * at + 4, :] = gt[pl.ds(16 * which + z, 4, stride=4), :]
    pairs = ((ty_hbm, ty), (tw_hbm, tw), (tt_hbm, tt), (tg_hbm, tg))
    tabs = [load(src, dst, ld_sem.at[5 + at]) for at, (src, dst) in enumerate(pairs)]

    ex0, ex1, ex2, ey0, ey1, ey2, ez0, ez1, hx0, hx1, hy0, hy1, hz1, r1, c1 = (pp[at] for at in range(15))

    def next_x(v):
        return jnp.where(row16 == 15, 0.0, pltpu.roll(v, 15, 0))

    def prev_x(v):
        return jnp.where(row16 == 0, 0.0, pltpu.roll(v, 1, 0))

    phx1 = hx1 - 0.5 * ((next_z(ez1, lane16) - ez1) - (ey2 - ey1))
    phx0 = hx0 - 0.5 * ((next_z(ez0, lane16) - ez0) - (ey1 - ey0))
    phy1 = hy1 - 0.5 * ((ex2 - ex1) - (next_x(ez1) - ez1))
    phy0 = hy0 - 0.5 * ((ex1 - ex0) - (next_x(ez0) - ez0))
    phz1 = hz1 - 0.5 * ((next_x(ey1) - ey1) - (next_z(ex1, lane16) - ex1))
    t_s[0, 0:16] = r1 * ex1 + c1 * ((phz1 - prev_z(phz1, lane16)) - (phy1 - phy0))
    t_s[1, 0:16] = r1 * ey1 + c1 * ((phx1 - phx0) - (phz1 - prev_x(phz1)))
    t_s[2, 0:16] = phx1
    t_s[3, 0:16] = phy1
    cols = jnp.zeros((16, 128), F32)
    for at, (v, y) in enumerate(((ex1, 0), (ez1, 0), (ez0, 0), (c1, 0), (phz1, 127), (c1, 127))):
        cols = jnp.where(lane16 == at, v[:, y : y + 1], cols)
    for g in range(GY):
        t_s[g, 16:32] = cols
    pk_s[0:1] = ey1[0:1]
    pk_s[1:2] = ez1[0:1]
    pk_s[2:3] = ez0[0:1]
    pk_s[3:4] = phz1[15:16]
    pk_s[4:5] = c1[0:1]
    pk_s[5:6] = c1[15:16]
    pk_s[6:7] = ex1[15:16]
    pk_s[7:8] = jnp.zeros((1, 128), F32)

    ye_s[0] = eb[0, :, 0, :]
    ye_s[1] = eb[2, :, 0, :]
    ex, ey, ez = eb[0, :, 127, :], eb[1, :, 127, :], eb[2, :, 127, :]
    yh_s[0] = hb[0, :, 127, :] - 0.5 * (-ez - (next_z(ey, lane16) - ey))
    ey_up = jnp.where(row16 == 15, 0.0, pltpu.roll(ey, 15, 0))
    yh_s[1] = hb[2, :, 127, :] - 0.5 * (ey_up - ey + ex)

    pk_l[1, Y] = pk_s[...]
    pltpu.make_async_copy(c_hbm.at[0:4], cb.at[0:4], ld_sem.at[4]).wait()
    al[0, Y] = srv[Y]
    al[1, Y] = siv[Y]
    t_l[Y] = t_s[Y]

    pl.semaphore_wait(barrier, greeted)

    def remote(src, dst, ss, rs, x, y):
        return pltpu.make_async_remote_copy(
            src_ref=src, dst_ref=dst, send_sem=ss, recv_sem=rs, device_id=(x, y), device_id_type=MESH
        )

    def pack(dx, d):
        return remote(
            pk_s, pk_l.at[2 - dx, Y], pk_ss.at[dx], pk_rs.at[2 - dx], (xp, X, xn)[dx], lax.rem(Y + d, GY)
        )

    for dx, ok in ((0, has_xp), (2, has_xn)):
        for d in range(GY):
            pl.when(ok)(pack(dx, d).start)
    for d in range(1, GY):
        pack(1, d).start()

    def all_of(ref, ss, rs):
        return remote(ref, ref, ss, rs, xp, Y)

    def packs_sent():
        for dx, ok in ((0, has_xp), (2, has_xn)):
            pl.when(ok)(all_of(pk_l.at[0], pk_ss.at[dx], pk_rs.at[dx]).wait_send)
        all_of(pk_l.at[0, 0:3], pk_ss.at[1], pk_rs.at[1]).wait_send()

    pending.append(packs_sent)

    def tangent(d):
        g = lax.rem(Y + d, GY)
        return remote(t_s.at[g], t_l.at[Y], t_ss, t_rs, X, g)

    for d in range(1, GY):
        tangent(d).start()
    pending.append(lambda: all_of(t_s.at[0:3], t_ss, t_rs).wait_send())

    def spectrum(part, d):
        g = lax.rem(Y + d, GY)
        return remote((srv, siv)[part].at[g], al.at[part, Y], a_ss, a_rs, X, g)

    for d in range(1, GY):
        for part in range(2):
            spectrum(part, d).start()
    pending.append(lambda: all_of(al.at[:, 0:3], a_ss, a_rs).wait_send())

    ye = remote(ye_s, ye_l, yh_sem.at[0], yh_sem.at[1], X, yp)
    yh = remote(yh_s, yh_l, yh_sem.at[2], yh_sem.at[3], X, yn)
    pl.when(has_yp)(ye.start)
    pl.when(has_yn)(yh.start)
    pending.append(lambda: pl.when(has_yp)(ye.wait_send))
    pending.append(lambda: pl.when(has_yn)(yh.wait_send))

    corner = remote(eb.at[1, 0, pl.ds(120, 8)], ce_l, x_sem.at[0], x_sem.at[1], xp, yn)
    pl.when(jnp.logical_and(has_xp, has_yn))(corner.start)
    pending.append(lambda: pl.when(jnp.logical_and(has_xp, has_yn))(corner.wait_send))
    xe = remote(eb.at[pl.ds(1, 2), 0], xe_l, x_sem.at[2], x_sem.at[3], xp, Y)
    pl.when(has_xp)(xe.start)
    pending.append(lambda: pl.when(has_xp)(xe.wait_send))

    pl.when(has_yn)(ye.wait_recv)
    pl.when(has_yp)(yh.wait_recv)
    yh_l[0] = jnp.where(has_yp, yh_l[0] - 0.5 * ye_s[1], 0.0)
    yh_l[1] = jnp.where(has_yp, yh_l[1] + 0.5 * ye_s[0], 0.0)

    ex, ey, ez = eb[0, 15], eb[1, 15], eb[2, 15]
    exn = jnp.where(rows == 127, ye_l[0, 15:16, :], pltpu.roll(ex, 127, 0))
    xh_s[0] = hb[1, 15] - 0.5 * ((next_z(ex, lanes) - ex) + ez)
    xh_s[1] = hb[2, 15] - 0.5 * (-ey - (exn - ex))
    xh = remote(xh_s, xh_l, x_sem.at[4], x_sem.at[5], xn, Y)
    pl.when(has_xn)(xh.start)
    pending.append(lambda: pl.when(has_xn)(xh.wait_send))

    def from_gy(make, d):
        make(d).wait_recv()

    all_of(al.at[:, 0:3], a_ss, a_rs).wait_recv()
    all_of(t_l.at[0:3], t_ss, t_rs).wait_recv()
    for copy in tabs:
        copy.wait()

    wave_cos, wave_sin = [wv[f : f + 1] for f in range(4)], [wv[f : f + 1] for f in range(4, 8)]
    total = None
    for s in range(GY):
        t, mine = t_l[s, 0:16], t_l[s, 16:32]
        if s < GY - 1:
            after = t_l[s + 1, 16:32]
            exn, ez1n, ez0n, c127 = after[:, 0:1], after[:, 1:2], after[:, 2:3], mine[:, 5:6]
            exn_p = prev_x(after)[:, 0:1]
            edge = jnp.where(
                Y == 0,
                0.5 * c127 * exn,
                jnp.where(Y == 1, -0.5 * c127 * ((ez1n - ez0n) + (exn - exn_p)), jnp.where(Y == 2, -0.5 * ez1n, 0.0)),
            )
            t = t + jnp.where(lane16 == 127, edge, 0.0)
        if s > 0:
            hzp0 = t_l[s - 1, 16:32][:, 4:5] + 0.5 * mine[:, 0:1]
            t = t + jnp.where(lane16 == 0, jnp.where(Y == 0, -mine[:, 3:4] * hzp0, 0.0), 0.0)
        re = jnp.concatenate([al[0, s, f] + t * wave_cos[f] for f in range(4)], axis=0)
        im = jnp.concatenate([al[1, s, f] - t * wave_sin[f] for f in range(4)], axis=0)
        data = jnp.concatenate(
            [jnp.concatenate([re, im], axis=0), jnp.concatenate([im, -re], axis=0)], axis=1
        )
        high, low = split(data)
        part = dot_nt(ty[0, s], high) + dot_nt(ty[0, s], low) + dot_nt(ty[1, s], high)
        total = part if total is None else total + part
    bs[...] = total.reshape(GX, 8, 128)

    none = jnp.zeros((1, 128), F32)
    wc, ws = none, none
    for f in range(4):
        wc = jnp.where((lane1 // 16) % 4 == f, wave_cos[f], wc)
        ws = jnp.where((lane1 // 16) % 4 == f, wave_sin[f], ws)
    by_cos, by_sin = jnp.where(lane1 < 64, wc, -ws), jnp.where(lane1 < 64, -ws, -wc)
    is_last, is_head = lane1 % 16 == 15, lane1 % 16 == 0
    cos_last, cos_head = jnp.where(is_last, by_cos, 0.0), jnp.where(is_head, by_cos, 0.0)
    sin_last, sin_head = jnp.where(is_last, by_sin, 0.0), jnp.where(is_head, by_sin, 0.0)
    all_of(pk_l.at[1, 0:3], pk_ss.at[1], pk_rs.at[1]).wait_recv()
    pl.when(has_xn)(all_of(pk_l.at[2], pk_ss.at[2], pk_rs.at[2]).wait_recv)
    pl.when(has_xp)(all_of(pk_l.at[0], pk_ss.at[0], pk_rs.at[0]).wait_recv)
    added = None
    for s in range(GY):
        nxt, own, prv = pk_l[2, s], pk_l[1, s], pk_l[0, s]
        dhz = -0.5 * nxt[0:1]
        before = -0.5 * pk_l[2, s - 1][0:1, 127:128] if s else jnp.zeros((1, 1), F32)
        dhz_p = jnp.where(lane1 == 0, before, pltpu.roll(dhz, 1, 1))
        dhy = 0.5 * nxt[1:2]
        dhyd = dhy - 0.5 * nxt[2:3]
        after = 0.5 * pk_l[0, s + 1][6:7, 0:1] if s < GY - 1 else jnp.zeros((1, 1), F32)
        hzp = prv[3:4] - 0.5 * own[0:1] + jnp.where(lane1 == 127, after, 0.0)
        last = jnp.where(
            Y == 0, own[5:6] * (dhz - dhz_p - dhyd), jnp.where(Y == 1, -own[5:6] * dhz, jnp.where(Y == 3, dhy, 0.0))
        )
        head = jnp.where(jnp.logical_and(Y == 1, has_xp), own[4:5] * hzp, 0.0)
        pair = [
            jnp.where(row8 == 0, last, 0.0) + jnp.where(row8 == 1, head, 0.0),
            jnp.where(row8 == 2, last, 0.0) + jnp.where(row8 == 3, head, 0.0),
        ]
        high, low = split(jnp.concatenate(pair, axis=1))
        rhs = jnp.concatenate([high, low], axis=0)
        part = dot_nt(ty[0, s], rhs) + dot_nt(ty[1, s], rhs)
        added = part if added is None else added + part
    added = added[:, 0:8] + added[:, 8:16]
    extra = added[:, 0:1] * cos_last + added[:, 1:2] * cos_head + added[:, 2:3] * sin_last + added[:, 3:4] * sin_head
    bs[...] = bs[...] + extra.reshape(GX, 8, 128)

    x_hi, row_in = (X // 4) & 1, (X // 8) * 4 + (X & 3)

    def column(at):
        to = block_at(offsets[at])
        return remote(bs.at[to], bl.at[x_hi, row_in], b_ss, b_rs.at[offsets[at][1]], to, Y)

    for at in range(GX - 1):
        column(at).start()
    pending.append(lambda: all_of(bs.at[0:31], b_ss, b_rs.at[0]).wait_send())
    bl[x_hi, row_in] = bs[X]

    def row(x, edge_first, edge_last):
        ex, ey, ez = eb[0, x], eb[1, x], eb[2, x]
        exn = jnp.where(rows == 127, ye_l[0, pl.ds(x, 1), :], pltpu.roll(ex, 127, 0))
        ezn = jnp.where(rows == 127, ye_l[1, pl.ds(x, 1), :], pltpu.roll(ez, 127, 0))
        if edge_last:
            ey_x, ez_x = -ey, -ez
        else:
            ey_x, ez_x = eb[1, x + 1] - ey, eb[2, x + 1] - ez
        hx = hb[0, x] - 0.5 * ((ezn - ez) - (next_z(ey, lanes) - ey))
        hy = hb[1, x] - 0.5 * ((next_z(ex, lanes) - ex) - ez_x)
        hz = hb[2, x] - 0.5 * (ey_x - (exn - ex))
        ho[0, x] = hx
        ho[1, x] = hy
        ho[2, x] = hz
        hxp = jnp.where(rows == 0, yh_l[0, pl.ds(x, 1), :], pltpu.roll(hx, 1, 0))
        hzp = jnp.where(rows == 0, yh_l[1, pl.ds(x, 1), :], pltpu.roll(hz, 1, 0))
        if edge_first:
            hy_x, hz_x = hy, hz
        else:
            hy_x, hz_x = hy - ho[1, x - 1], hz - ho[2, x - 1]
        r, c = rb[x], cb[x]
        nx = r * ex + c * ((hz - hzp) - (hy - prev_z(hy, lanes)))
        ny = r * ey + c * ((hx - prev_z(hx, lanes)) - hz_x)
        nz = r * ez + c * (hy_x - (hx - hxp))
        eo[0, x] = nx
        eo[1, x] = ny
        eo[2, x] = nz
    row(0, True, False)

    def inner(x, carry):
        row(x, False, False)
        return carry

    lax.fori_loop(1, 15, inner, 0)
    row(15, False, True)

    sign = jnp.where(lax.broadcasted_iota(jnp.int32, (128, 128), 1) < 64, 1.0, -1.0)
    y = None
    for half in range(2):
        all_of(bs.at[0 : 15 + half], b_ss, b_rs.at[half]).wait_recv()
        which = (x_hi + half) & 1
        block = bl[which].reshape(128, 128)
        high, low = split(jnp.concatenate([block, pltpu.roll(block, 64, 1) * sign], axis=0))
        part = dot_nn(tw[0, which], high) + dot_nn(tw[0, which], low) + dot_nn(tw[1, which], high)
        y = part if y is None else y + part
    y = y * tt[0] + pltpu.roll(y, 64, 1) * tt[1]
    y_sw = pltpu.roll(y, 64, 1) * jnp.concatenate([sign, sign], axis=0)
    pieces = []
    for b in range(4):
        pieces += [y[64 * b : 64 * b + 64], y_sw[64 * b : 64 * b + 64]]
    high, low = split(jnp.concatenate(pieces, axis=0))
    out = dot_nt(tg[0], high) + dot_nt(tg[0], low) + dot_nt(tg[1], high)
    for a in range(8):
        for b in range(4):
            cs[4 * a + b] = out[4 * a : 4 * a + 4, 128 * b : 128 * b + 128]

    def finished(at):
        to = block_at(offsets[at])
        return remote(cs.at[to], cl.at[Y, slot], c_ss, c_rs, to, home)

    for at in range(GX - 1):
        finished(at).start()
    pl.when(home != Y)(finished(GX - 1).start)

    def blocks(wait):
        pl.when(home != Y)(lambda: wait(all_of(cs, c_ss, c_rs)))
        pl.when(home == Y)(lambda: wait(all_of(cs.at[0:31], c_ss, c_rs)))

    pending.append(lambda: blocks(lambda copy: copy.wait_send()))

    @pl.when(home == Y)
    def _():
        cl[Y, slot] = cs[X]

    pl.when(has_xn)(xe.wait_recv)
    pl.when(has_xp)(xh.wait_recv)
    pl.when(jnp.logical_and(has_xn, has_yp))(corner.wait_recv)
    dhy, dhz = 0.5 * xe_l[1], -0.5 * xe_l[0]
    ho[1, 15] = ho[1, 15] + dhy
    ho[2, 15] = ho[2, 15] + dhz
    dhz_p = jnp.where(rows == 0, -0.5 * ce_l[7:8], pltpu.roll(dhz, 1, 0))
    c = cb[15]
    eo[0, 15] = eo[0, 15] + c * ((dhz - dhz_p) - (dhy - prev_z(dhy, lanes)))
    eo[1, 15] = eo[1, 15] - c * dhz
    eo[2, 15] = eo[2, 15] + c * dhy
    hyp = jnp.where(has_xp, xh_l[0] + 0.5 * eb[2, 0], 0.0)
    hzp = jnp.where(has_xp, xh_l[1] - 0.5 * eb[1, 0], 0.0)
    c = cb[0]
    eo[1, 0] = eo[1, 0] + c * hzp
    eo[2, 0] = eo[2, 0] - c * hyp

    def own_plane(x, carry):
        for at, v in enumerate((eo[0, x], eo[1, x], ho[0, x], ho[1, x])):
            pp[at, pl.ds(x, 1), :] = plane_of(v, PLANE)
        return carry

    lax.fori_loop(0, 16, own_plane, 0)
    for at in range(4):
        t = pp[at]
        for f in range(4):
            nr[at, f] = srv[at, f] + t * wave_cos[f]
            ni[at, f] = siv[at, f] - t * wave_sin[f]

    blocks(lambda copy: copy.wait_recv())

    for q in range(8):
        for g in range(4):
            rel[q, 4 * g : 4 * g + 4, :] = cl[g, q]
    for wait in pending:
        wait()


def flush_kernel(eo, ho, nr, ni, rel, e_out, h_out, r_out, i_out, f_out, zz, fv, sem):
    for which, (src, dst) in enumerate(((eo, e_out), (ho, h_out))):
        for i in range(3):
            for x in range(0, 16, 8):
                part = (i, pl.ds(x, 8))
                pltpu.make_async_copy(src.at[part], dst.at[part], sem.at[which]).start()
    whole = [pltpu.make_async_copy(src, dst, sem.at[at]) for at, (src, dst) in enumerate(((eo, e_out), (ho, h_out)))]
    copies = [pltpu.make_async_copy(nr, r_out, sem.at[2]), pltpu.make_async_copy(ni, i_out, sem.at[3])]
    for copy in copies:
        copy.start()
    lane16 = lax.broadcasted_iota(jnp.int32, (16, 128), 1)
    turned = [pltpu.roll(rel[q], 8 * q, 1) if q else rel[q] for q in range(8)]
    group = lane16 // 8
    for s in range(16):
        acc = turned[0]
        for q in range(1, 8):
            acc = jnp.where(group == (q + s) % 16, turned[q], acc)
        if s:
            acc = pltpu.roll(acc, 128 - 8 * s, 1)
        zz[:, s, :] = acc
    for g in range(4):
        for f in range(4):
            fv[0, g, f] = zz[4 * g + f, 0:8, 0:64]
            fv[1, g, f] = zz[4 * g + f, 8:16, 0:64]
    copies.append(pltpu.make_async_copy(fv, f_out, sem.at[4]))
    copies[-1].start()
    for copy in copies + whole:
        copy.wait()


def per_device(electric, magnetic, retention, coupling, spectrum_real, spectrum_imag, phases):
    tab_y, tab_w, tab_t, tab_g = (jnp.asarray(t) for t in tables())
    vmem, dma = pltpu.VMEM, pltpu.SemaphoreType.DMA
    hbm = pl.BlockSpec(memory_space=pltpu.HBM)
    in_vmem = pl.BlockSpec(memory_space=pltpu.VMEM)
    shapes = [
        jax.ShapeDtypeStruct(electric.shape, F32),
        jax.ShapeDtypeStruct(magnetic.shape, F32),
        jax.ShapeDtypeStruct(spectrum_real.shape, F32),
        jax.ShapeDtypeStruct(spectrum_imag.shape, F32),
        jax.ShapeDtypeStruct((2, 4, 4, 8, 64), F32),
    ]
    fixed = [
        pltpu.with_memory_space_constraint(a, pltpu.HBM)
        for a in (electric, magnetic, retention, coupling, spectrum_real, spectrum_imag, tab_y, tab_w, tab_t, tab_g)
    ]
    held = pl.pallas_call(
        step_kernel,
        out_shape=shapes[:4] + [jax.ShapeDtypeStruct((8, 16, 128), F32)],
        in_specs=[hbm] * 11,
        out_specs=[in_vmem] * 5,
        scratch_shapes=[
            vmem(electric.shape, F32), vmem(magnetic.shape, F32), vmem(retention.shape, F32), vmem(coupling.shape, F32),
            vmem(spectrum_real.shape, F32), vmem(spectrum_imag.shape, F32),
            vmem(tab_y.shape, BF16), vmem(tab_w.shape, BF16), vmem(tab_t.shape, F32), vmem(tab_g.shape, BF16),
            vmem((2, 16, 128), F32), vmem((2, 16, 128), F32), vmem((2, 16, 128), F32), vmem((2, 16, 128), F32),
            vmem((2, 128, 128), F32), vmem((2, 128, 128), F32), vmem((8, 128), F32),
            vmem((8, 128), F32), vmem((3, 4, 8, 128), F32),
            vmem((4, 32, 128), F32), vmem((4, 32, 128), F32), vmem((2, 4, 4, 16, 128), F32),
            vmem((32, 8, 128), F32), vmem((2, 16, 8, 128), F32), vmem((32, 4, 128), F32), vmem((4, 8, 4, 128), F32),
            vmem((2, 128, 128), F32), vmem((15, 16, 128), F32), vmem((8, 128), F32), pltpu.SMEM((4,), F32),
            vmem((128, 128), F32), vmem((128, 128), F32),
            dma((9,)), dma((4,)), dma((3,)), dma((3,)), dma, dma, dma, dma, dma((6,)), dma, dma((2,)), dma, dma, dma,
        ],
        compiler_params=pltpu.CompilerParams(collective_id=0, has_side_effects=True, vmem_limit_bytes=40 * 2**20),
    )(*fixed[:6], pltpu.with_memory_space_constraint(phases, pltpu.HBM), *fixed[6:])
    return pl.pallas_call(
        flush_kernel,
        out_shape=shapes,
        in_specs=[in_vmem] * 5,
        out_specs=[hbm] * 5,
        scratch_shapes=[vmem((16, 16, 128), F32), vmem((2, 4, 4, 8, 64), F32), dma((5,))],
        compiler_params=pltpu.CompilerParams(vmem_limit_bytes=16 * 2**20),
    )(*held)


def solution(mesh):
    placed = (
        P(None, "gx", "gy", None),
        P(None, "gx", "gy", None),
        P("gx", "gy", None),
        P("gx", "gy", None),
        P(None, None, "gx", "gy"),
        P(None, None, "gx", "gy"),
        P(),
    )
    return jax.shard_map(
        per_device,
        mesh=mesh,
        in_specs=placed,
        out_specs=(
            P(None, "gx", "gy", None),
            P(None, "gx", "gy", None),
            P(None, None, "gx", "gy"),
            P(None, None, "gx", "gy"),
            P(None, None, None, "gx", "gy"),
        ),
        check_vma=False,
    )
```
